512 devices in a mesh: grp: 4 (over y), dev: 128 (over z, x, core).
Axes of the slice: x: 4, y: 4, z: 16, core: 2. Of those that a mesh axis runs over, the one named last changes fastest.
Arguments:
- spectrum: float32 [1152, 128, 128], P(None, 'dev'), may hold values from 0.05 to 2
- sea_mask: int32 [128, 128], P('dev'), may hold values 0 or 1
- wind: float32 [2, 128, 128], P(None, 'dev'), may hold values from -24 to 24
- currents: float32 [4, 2, 65536], P('grp', None, 'dev'), may hold values from -6 to 6
- coupling: int32 [4, 65536], P('grp', 'dev'), may hold values from 0 to 16383, as said below
Outputs:
- updated: float32 [1152, 128, 128], P(None, 'dev')
- cell_drift: float32 [4, 2, 65536], P('grp', None, 'dev')
The draws below stay inside these ranges and needn't reach their ends.
Inputs may be any that keep to these rules, and one draw needn't show every extreme that they name: `coupling`: an ocean cell's entry names the wave point i * 128 + j that it is averaged into and reads its drift from; cell c lies in grid column i with i equal to c // 512 - 1, c // 512 or c // 512 + 1, periodic over 128 columns. `sea_mask`: 1 marks a sea point.
All inputs are finite; a program needn't handle non-finite values. No bound on the sum of `sea_mask` on one device may be relied on, other than what follows from the above.
Results may differ from the reference program's by a relative error of at most 0.00014.
Values sent between devices are 32-bit elements; how exact they have to be, the bound alone decides.
A program may use at most 64 MiB of HBM per device.

```python
import math
import jax
import jax.numpy as jnp
from jax import lax

NDIR = 32
CELL_DEV = 512
NB = 1152
NX = 128
NY = 128
CELLS = 65536
N_GRP = 4
N_DEV = 128


def draw_coupling(key, part):
    first_key, second_key = jax.random.split(jax.random.fold_in(key, 11))
    owner = (jnp.arange(CELL_DEV * N_DEV, dtype=jnp.int32) // CELL_DEV)[None, :]
    offset = jax.random.randint(first_key, (N_GRP, CELL_DEV * N_DEV), -1, 2, dtype=jnp.int32)
    target_col = (owner + offset + NX) % NX
    target_row = jax.random.randint(second_key, (N_GRP, CELL_DEV * N_DEV), 0, NY, dtype=jnp.int32)
    return (target_col * NY + target_row).astype(jnp.int32)


def plant(drawn, key, least, largest):
    place = [jax.random.randint(jax.random.fold_in(key, axis), (), 0, length) for axis, length in enumerate(drawn.shape)]
    widest = drawn.shape.index(max(drawn.shape))
    next_to = place[:widest] + [(place[widest] + 1) % drawn.shape[widest]] + place[widest + 1:]
    return drawn.at[tuple(place)].set(least).at[tuple(next_to)].set(largest)


def block_levels(stream_key, dims, cuts, least, top_value):
    def one(position, blocks):
        heights = jax.random.uniform(jax.random.fold_in(jax.random.fold_in(stream_key, 6), position), (blocks,), jnp.float32, least / len(cuts), top_value / len(cuts))
        return jnp.repeat(jnp.exp(heights), dims[position] // blocks).reshape((-1,) + (1,) * (len(dims) - position - 1))

    gain = one(*cuts[0])
    for cut in cuts[1:]:
        gain = gain * one(*cut)
    return gain


def scatter_about(rng, extent, scale, most, pieces=(), kind=jnp.bfloat16):
    array = scale * jax.random.normal(rng, extent, jnp.float32)
    if pieces:
        array = array * block_levels(rng, extent, pieces, -0.22, 0.18)
    return jnp.clip(array, -most, most).astype(kind)


def setup_inputs(seed: int = 0) -> dict:
    key_of = jax.random.split(jax.random.key(seed), 6)
    spectrum = jnp.clip(jnp.exp(math.log(2.0) - 3.6888794 * jax.random.uniform(key_of[0], (NB, NX, NY), jnp.float32) ** block_levels(key_of[0], (NB, NX, NY), ((1, 128),), -0.2, 0.2)), 0.05, 2.0)
    sea_mask = plant((jax.random.randint(key_of[1], (NX, NY), 0, 4) < 3).astype(jnp.int32), jax.random.fold_in(key_of[1], 1), 0, 1)
    wind = scatter_about(key_of[2], (2, NX, NY), 8.0, 24.0, ((1, 128),), jnp.float32)
    currents = scatter_about(key_of[3], (N_GRP, 2, CELLS), 1.5, 6.0, ((0, 4), (2, 128)), jnp.float32)
    coupling = draw_coupling(jax.random.fold_in(key_of[5], 71), 0)
    return {"spectrum": spectrum, "sea_mask": sea_mask, "wind": wind, "currents": currents, "coupling": coupling}


FIRST_FREQ = 0.04
GROWTH = 1.1
SPEED_TOP = 0.45
CURRENT_TOP = 0.2
WIND_GAIN = 0.03
WHITECAP = 0.3
STEEP_SCALE = 0.4
STOKES_GAIN = 3.0


def bin_tables(bin_index):
    freq_level = (bin_index // NDIR).astype(jnp.float32)
    heading = (bin_index % NDIR).astype(jnp.float32) * (2.0 * math.pi / NDIR)
    frequency = FIRST_FREQ * GROWTH ** freq_level
    group_speed = SPEED_TOP * FIRST_FREQ / frequency
    return frequency, jnp.cos(heading), jnp.sin(heading), group_speed


def column(values):
    return values[:, None, None]


def sources(energy, sea_frac, wind, mean_current, frequency, cosine_dir, sine_dir):
    energy = energy * sea_frac
    spacing = 0.1 * frequency
    total_energy = jnp.sum(energy * column(spacing), axis=0)
    moment = jnp.sum(energy * column(spacing * frequency), axis=0)
    is_sea = sea_frac > 0.5
    safe_total = jnp.where(is_sea, total_energy, 1.0)
    mean_freq = jnp.where(is_sea, moment / safe_total, 1.0)
    steepness = STEEP_SCALE * total_energy * mean_freq ** 4
    damping = WHITECAP * (column(frequency) / mean_freq) ** 2 * steepness ** 2
    along_wind = column(cosine_dir) * (wind[0] - mean_current[0]) + column(sine_dir) * (wind[1] - mean_current[1])
    growth = WIND_GAIN * jnp.maximum(0.64 * column(frequency) * along_wind - 1.0, 0.0)
    return energy * (1.0 + growth) / (1.0 + damping)


def transport(west_energy, centre, east_energy, west_flow, centre_flow, east_flow, group_speed, cosine_dir, sine_dir, sea_frac):
    speed_x = column(group_speed * cosine_dir)
    speed_y = column(group_speed * sine_dir)
    face_east = 0.5 * ((speed_x + centre_flow[0]) + (speed_x + east_flow[0]))
    face_west = 0.5 * ((speed_x + west_flow[0]) + (speed_x + centre_flow[0]))
    flux_east = jnp.maximum(face_east, 0.0) * centre + jnp.minimum(face_east, 0.0) * east_energy
    flux_west = jnp.maximum(face_west, 0.0) * west_energy + jnp.minimum(face_west, 0.0) * centre
    speed_north = speed_y + centre_flow[1]
    face_north = 0.5 * (speed_north[:, :, :-1] + speed_north[:, :, 1:])
    flux_north = jnp.maximum(face_north, 0.0) * centre[:, :, :-1] + jnp.minimum(face_north, 0.0) * centre[:, :, 1:]
    flux_north = jnp.pad(flux_north, ((0, 0), (0, 0), (1, 1)))
    return sea_frac * (centre - (flux_east - flux_west) - (flux_north[:, :, 1:] - flux_north[:, :, :-1]))


def stokes_table(frequency, cosine_dir, sine_dir):
    weight = STOKES_GAIN * 0.1 * frequency ** 4
    return jnp.stack([weight * cosine_dir, weight * sine_dir])


def reference(spectrum, sea_mask, wind, currents, coupling):
    bin_count, width_x, width_y = spectrum.shape
    groups = currents.shape[0]
    frequency, cosine_dir, sine_dir, group_speed = bin_tables(jnp.arange(bin_count, dtype=jnp.int32))
    sea_frac = sea_mask.astype(jnp.float32)
    ocean_values = jnp.concatenate([currents[1:], jnp.ones_like(currents[1:, :1])], axis=1)
    ocean_values = jnp.transpose(ocean_values, (0, 2, 1)).reshape(-1, 3)
    targets = coupling[1:].reshape(-1)
    cell_sums = jax.ops.segment_sum(ocean_values, targets, num_segments=width_x * width_y).T.reshape(3, width_x, width_y)
    mean_current = cell_sums[:2] / jnp.maximum(cell_sums[2], 1.0)
    transport_flow = CURRENT_TOP * jnp.tanh(mean_current)
    forced = sources(spectrum, sea_frac, wind, mean_current, frequency, cosine_dir, sine_dir)
    updated = transport(jnp.roll(forced, 1, axis=1), forced, jnp.roll(forced, -1, axis=1),
                        jnp.roll(transport_flow, 1, axis=1), transport_flow, jnp.roll(transport_flow, -1, axis=1),
                        group_speed, cosine_dir, sine_dir, sea_frac)
    stokes_drift = jnp.dot(stokes_table(frequency, cosine_dir, sine_dir), updated.reshape(bin_count, -1),
                           precision=lax.Precision.HIGHEST)
    picked = jnp.transpose(stokes_drift[:, coupling], (1, 0, 2))
    ocean_group = (jnp.arange(groups) > 0).astype(jnp.float32)[:, None, None]
    return updated, picked * ocean_group
```

```python
import functools
import math

import jax
import jax.numpy as jnp
import numpy as np
from jax import lax
from jax.experimental import pallas as pl
from jax.experimental.pallas import tpu as pltpu
from jax.sharding import PartitionSpec as P

MESH = pl.DeviceIdType.MESH
F32 = jnp.float32
BF16 = jnp.bfloat16

NDIR = 32
FIRST_FREQ = 0.04
GROWTH = 1.1
SPEED_TOP = 0.45
CURRENT_TOP = 0.2
WIND_GAIN = 0.03
WHITECAP = 0.3
STEEP_SCALE = 0.4
STOKES_GAIN = 3.0
LANES = 128
SUB = 8
GROWTH_F = WIND_GAIN * 0.64


def bin_tables(levels):
    padded = -(-levels // SUB) * SUB
    heading = np.arange(NDIR) * (2.0 * math.pi / NDIR)
    freq = FIRST_FREQ * GROWTH ** np.arange(padded)
    rows = np.concatenate(
        [
            np.cos(heading),
            np.sin(heading),
            GROWTH_F * freq,
            freq**2,
            SPEED_TOP * FIRST_FREQ / freq,
            STOKES_GAIN * 0.1 * freq**4,
        ]
    )
    table = np.broadcast_to(rows[:, None], (rows.shape[0], LANES))
    return jnp.asarray(table.astype(np.float32)), padded


def split3(x):
    hi = x.astype(BF16)
    rest = x - hi.astype(F32)
    mid = rest.astype(BF16)
    low = (rest - mid.astype(F32)).astype(BF16)
    return jnp.concatenate([hi, mid, low], axis=0)


def sum3(x):
    n = x.shape[0] // 3
    return x[:n] + x[n : 2 * n] + x[2 * n :]


def kernel(
    n_grp,
    n_dev,
    levels,
    padded,
    chunks,
    head_chunks,
    spec_hbm,
    mask_ref,
    wind_ref,
    cur_ref,
    coup_ref,
    tab_ref,
    upd_ref,
    cell_ref,
    ctr,
    west,
    east,
    base,
    part,
    nbr,
    info,
    drift,
    rtab,
    dtab,
    load_sem,
    halo_send,
    halo_recv,
    part_send,
    part_recv,
    nbr_send,
    nbr_recv,
    info_send,
    info_recv,
    drift_send,
    drift_recv,
):
    g = lax.axis_index("grp")
    d = lax.axis_index("dev")
    bins = levels * NDIR
    per = levels // chunks
    rows = per * NDIR
    quads = NDIR // SUB
    COS, SIN, FG = 0, NDIR, 2 * NDIR
    F2, GS, WT = FG + padded, FG + 2 * padded, FG + 3 * padded

    def at(step):
        return {"grp": g, "dev": lax.rem(d + step + n_dev, n_dev)}

    def group(step):
        return {"grp": lax.rem(g + step, n_grp), "dev": d}

    barrier = pltpu.get_barrier_semaphore()
    for k in range(1, n_grp):
        pl.semaphore_signal(barrier, inc=1, device_id=group(k), device_id_type=MESH)
    for k in (-2, -1, 1, 2):
        pl.semaphore_signal(barrier, inc=1, device_id=at(k), device_id_type=MESH)

    load = pltpu.make_async_copy(spec_hbm, ctr, load_sem)
    load.start()

    coup = coup_ref[...]
    slot = ((coup >> 7) - d + n_dev + 1) & (n_dev - 1)
    row = coup & (LANES - 1)
    cells = coup.shape[1]
    one_hot = jnp.where(
        lax.broadcasted_iota(jnp.int32, (LANES, cells), 0) == row, 1.0, 0.0
    ).astype(BF16)
    kind = lax.broadcasted_iota(jnp.int32, (2 * SUB, cells), 0)
    comp = kind & 3
    value = jnp.where(
        comp == 0, cur_ref[0:1, :], jnp.where(comp == 1, cur_ref[1:2, :], jnp.where(comp == 2, 1.0, 0.0))
    )
    value = jnp.where(jnp.logical_and((kind >> 2) == slot, g > 0), value, 0.0)
    sums = lax.dot_general(
        split3(value), one_hot, (((1,), (1,)), ((), ())), preferred_element_type=F32
    )
    part[g] = sum3(sums)

    load.wait()

    def add_level(l, acc):
        r = pl.multiple_of(l * NDIR, NDIR)
        e = ctr[pl.ds(r, SUB), :]
        for m in range(1, quads):
            e = e + ctr[pl.ds(r + m * SUB, SUB), :]
        return (
            acc[0] + e * tab_ref[pl.ds(FG + l, 1), :],
            acc[1] + e * tab_ref[pl.ds(F2 + l, 1), :],
        )

    zero = jnp.zeros((SUB, LANES), F32)
    total, moment = lax.fori_loop(0, levels, add_level, (zero, zero), unroll=4)
    sea = mask_ref[...].astype(F32)
    total = jnp.sum(total, axis=0, keepdims=True) * (0.1 / GROWTH_F) * sea
    moment = jnp.sum(moment, axis=0, keepdims=True) * 0.1 * sea
    is_sea = sea > 0.5
    mean_freq = jnp.where(is_sea, moment / jnp.where(is_sea, total, 1.0), 1.0)
    steepness = STEEP_SCALE * total * mean_freq**4
    damp = WHITECAP * (steepness / mean_freq) ** 2
    which = lax.broadcasted_iota(jnp.int32, (SUB, LANES), 0)
    info[1] = jnp.where(
        which == 0,
        sea,
        jnp.where(
            which == 1,
            damp,
            jnp.where(which == 2, wind_ref[0:1, :], jnp.where(which == 3, wind_ref[1:2, :], 0.0)),
        ),
    )

    pl.semaphore_wait(barrier, n_grp - 1 + 4)

    part_copies = []
    for k in range(1, n_grp):
        copy = pltpu.make_async_remote_copy(
            src_ref=part.at[g],
            dst_ref=part.at[g],
            send_sem=part_send.at[k],
            recv_sem=part_recv.at[g],
            device_id=group(k),
            device_id_type=MESH,
        )
        copy.start()
        part_copies.append(copy)
    info_copies = []
    for i, step in enumerate((1, -1)):
        copy = pltpu.make_async_remote_copy(
            src_ref=info.at[1],
            dst_ref=info.at[1 - step],
            send_sem=info_send.at[i],
            recv_sem=info_recv.at[i],
            device_id=at(step),
            device_id_type=MESH,
        )
        copy.start()
        info_copies.append(copy)

    halo_copies = []

    def send_chunk(k):
        for i, (step, there) in enumerate(((1, west), (-1, east))):
            copy = pltpu.make_async_remote_copy(
                src_ref=ctr.at[pl.ds(k * rows, rows), :],
                dst_ref=there.at[pl.ds(k * rows, rows), :],
                send_sem=halo_send.at[i, k],
                recv_sem=halo_recv.at[i, k],
                device_id=at(step),
                device_id_type=MESH,
            )
            copy.start()
            halo_copies.append(copy)

    for k in range(head_chunks):
        send_chunk(k)

    for k in range(1, n_grp):
        src = lax.rem(g - k + n_grp, n_grp)
        pltpu.make_async_remote_copy(
            src_ref=part.at[src],
            dst_ref=part.at[src],
            send_sem=part_send.at[k],
            recv_sem=part_recv.at[src],
            device_id=group(k),
            device_id_type=MESH,
        ).wait_recv()
    both = part[1]
    for k in range(2, n_grp):
        both = both + part[k]
    nbr[2] = both
    nbr_copies = []
    for i, step in enumerate((-2, -1, 1, 2)):
        copy = pltpu.make_async_remote_copy(
            src_ref=nbr.at[2],
            dst_ref=nbr.at[2 - step],
            send_sem=nbr_send.at[i],
            recv_sem=nbr_recv.at[i],
            device_id=at(step),
            device_id_type=MESH,
        )
        copy.start()
        nbr_copies.append(copy)
    for k in range(head_chunks, chunks):
        send_chunk(k)

    for copy in info_copies:
        copy.wait_recv()
    for copy in nbr_copies:
        copy.wait_recv()

    cos = [tab_ref[pl.ds(COS + m * SUB, SUB), :] for m in range(quads)]
    sin = [tab_ref[pl.ds(SIN + m * SUB, SUB), :] for m in range(quads)]
    flows = []
    for c in range(3):
        s4 = nbr[c + 1, 4:8, :] + nbr[c, 8:12, :] + nbr[c + 2, 0:4, :]
        count = jnp.maximum(s4[2:3], 1.0)
        mean_x = s4[0:1] / count
        mean_y = s4[1:2] / count
        flows.append((CURRENT_TOP * jnp.tanh(mean_x), CURRENT_TOP * jnp.tanh(mean_y)))
        sea_c = info[c, 0:1, :]
        damp_c = info[c, 1:2, :]
        wx = info[c, 2:3, :] - mean_x
        wy = info[c, 3:4, :] - mean_y
        for m in range(quads):
            dtab[c, pl.ds(m * SUB, SUB), :] = cos[m] * wx + sin[m] * wy
        for q in range(padded // SUB):
            f2 = tab_ref[pl.ds(F2 + q * SUB, SUB), :]
            rtab[c, pl.ds(q * SUB, SUB), :] = sea_c / (1.0 + f2 * damp_c)
    wide = (SUB, LANES)
    face_w = jnp.broadcast_to(0.5 * (flows[0][0] + flows[1][0]), wide)
    face_e = jnp.broadcast_to(0.5 * (flows[1][0] + flows[2][0]), wide)
    flow_y = jnp.broadcast_to(flows[1][1], wide)
    face_n = 0.5 * (flow_y + pltpu.roll(flow_y, LANES - 1, 1))
    sea_w = jnp.broadcast_to(sea, wide)
    inner = lax.broadcasted_iota(jnp.int32, wide, 1) < LANES - 1
    gain = [[dtab[c, pl.ds(m * SUB, SUB), :] for m in range(quads)] for c in range(3)]

    def forced(energy, c, m, fg, rec):
        return energy * (jnp.maximum(gain[c][m] * fg + (1.0 - WIND_GAIN), 1.0) * rec)

    def own_level(l, carry):
        fg = tab_ref[pl.ds(FG + l, 1), :]
        gs = tab_ref[pl.ds(GS + l, 1), :]
        rec = rtab[1, pl.ds(l, 1), :]
        for m in range(quads):
            r = pl.ds(pl.multiple_of(l * NDIR + m * SUB, SUB), SUB)
            e = forced(ctr[r, :], 1, m, fg, rec)
            a = jnp.where(inner, gs * sin[m] + face_n, 0.0)
            flux = a * jnp.where(a > 0.0, e, pltpu.roll(e, LANES - 1, 1))
            own = (e - flux) + pltpu.roll(flux, 1, 1)
            base[0, r, :] = e
            base[1, r, :] = own
        return carry

    lax.fori_loop(0, levels, own_level, 0, unroll=2)

    def edge_level(l, acc):
        fg = tab_ref[pl.ds(FG + l, 1), :]
        gs = tab_ref[pl.ds(GS + l, 1), :]
        wt = tab_ref[pl.ds(WT + l, 1), :]
        rec_w = rtab[0, pl.ds(l, 1), :]
        rec_e = rtab[2, pl.ds(l, 1), :]
        out = []
        for m in range(quads):
            r = pl.ds(pl.multiple_of(l * NDIR + m * SUB, SUB), SUB)
            e = base[0, r, :]
            ew = forced(west[r, :], 0, m, fg, rec_w)
            ee = forced(east[r, :], 2, m, fg, rec_e)
            speed = gs * cos[m]
            a = speed + face_e
            b = speed + face_w
            flux_e = a * jnp.where(a > 0.0, e, ee)
            flux_w = b * jnp.where(b > 0.0, ew, e)
            u = sea_w * (base[1, r, :] - flux_e + flux_w)
            upd_ref[r, :] = u
            out.append(acc[m] + wt * u)
        return tuple(out)

    acc = (zero,) * quads
    for k in range(chunks):
        for copy in halo_copies[2 * k : 2 * k + 2]:
            copy.wait_recv()
        acc = lax.fori_loop(k * per, (k + 1) * per, edge_level, acc, unroll=2)

    dx = acc[0] * cos[0]
    dy = acc[0] * sin[0]
    for m in range(1, quads):
        dx = dx + acc[m] * cos[m]
        dy = dy + acc[m] * sin[m]
    drift[1] = jnp.where(
        which == 0,
        jnp.sum(dx, axis=0, keepdims=True),
        jnp.where(which == 1, jnp.sum(dy, axis=0, keepdims=True), 0.0),
    )
    drift_copies = []
    for i, step in enumerate((1, -1)):
        copy = pltpu.make_async_remote_copy(
            src_ref=drift.at[1],
            dst_ref=drift.at[1 - step],
            send_sem=drift_send.at[i],
            recv_sem=drift_recv.at[i],
            device_id=at(step),
            device_id_type=MESH,
        )
        copy.start()
        drift_copies.append(copy)
    for copy in part_copies + info_copies + nbr_copies + halo_copies:
        copy.wait_send()
    for copy in drift_copies:
        copy.wait()

    band = jnp.zeros((2 * SUB, LANES), F32)
    place = lax.broadcasted_iota(jnp.int32, (2 * SUB, LANES), 0)
    for c in range(3):
        for v in range(2):
            band = jnp.where(place == 4 * c + v, drift[c, v : v + 1, :], band)
    picked = sum3(jnp.dot(split3(band), one_hot, preferred_element_type=F32))
    for v in range(2):
        out = jnp.where(
            slot == 0,
            picked[v : v + 1],
            jnp.where(slot == 1, picked[4 + v : 5 + v], picked[8 + v : 9 + v]),
        )
        cell_ref[v : v + 1, :] = jnp.where(g > 0, out, 0.0)


def body(n_grp, n_dev, spectrum, sea_mask, wind, currents, coupling):
    bins, _, width = spectrum.shape
    levels = bins // NDIR
    cells = currents.shape[2]
    table, padded = bin_tables(levels)
    chunks, head_chunks = 6, 2
    vmem = pl.BlockSpec(memory_space=pltpu.VMEM)
    hbm = pl.BlockSpec(memory_space=pl.ANY)
    dma = pltpu.SemaphoreType.DMA
    updated, cell_drift = pl.pallas_call(
        functools.partial(kernel, n_grp, n_dev, levels, padded, chunks, head_chunks),
        out_shape=(
            jax.ShapeDtypeStruct((bins, width), F32),
            jax.ShapeDtypeStruct((2, cells), F32),
        ),
        in_specs=[hbm, vmem, vmem, vmem, vmem, vmem],
        out_specs=(vmem, vmem),
        scratch_shapes=[
            pltpu.VMEM((bins, width), F32),
            pltpu.VMEM((bins, width), F32),
            pltpu.VMEM((bins, width), F32),
            pltpu.VMEM((2, bins, width), F32),
            pltpu.VMEM((n_grp, 2 * SUB, width), F32),
            pltpu.VMEM((5, 2 * SUB, width), F32),
            pltpu.VMEM((3, SUB, width), F32),
            pltpu.VMEM((3, SUB, width), F32),
            pltpu.VMEM((3, padded, width), F32),
            pltpu.VMEM((3, NDIR, width), F32),
            dma(()),
            dma((2, chunks)),
            dma((2, chunks)),
            dma((n_grp,)),
            dma((n_grp,)),
            dma((4,)),
            dma((4,)),
            dma((2,)),
            dma((2,)),
            dma((2,)),
            dma((2,)),
        ],
        compiler_params=pltpu.CompilerParams(
            collective_id=0, has_side_effects=True, vmem_limit_bytes=32 * 1024 * 1024
        ),
        name="wave_step",
    )(
        spectrum.reshape(bins, width),
        sea_mask,
        wind.reshape(2, width),
        currents.reshape(2, cells),
        coupling,
        table,
    )
    return updated.reshape(bins, 1, width), cell_drift.reshape(1, 2, cells)


def solution(mesh):
    return jax.shard_map(
        functools.partial(body, mesh.shape["grp"], mesh.shape["dev"]),
        mesh=mesh,
        in_specs=(
            P(None, "dev", None),
            P("dev", None),
            P(None, "dev", None),
            P("grp", None, "dev"),
            P("grp", "dev"),
        ),
        out_specs=(P(None, "dev", None), P("grp", None, "dev")),
        check_vma=False,
    )
```

```python
import functools
import math

import jax
import jax.numpy as jnp
import numpy as np
from jax import lax
from jax.experimental import pallas as pl
from jax.experimental.pallas import tpu as pltpu
from jax.sharding import PartitionSpec as P

MESH = pl.DeviceIdType.MESH
F32 = jnp.float32
BF16 = jnp.bfloat16

NDIR = 32
FIRST_FREQ = 0.04
GROWTH = 1.1
SPEED_TOP = 0.45
CURRENT_TOP = 0.2
WIND_GAIN = 0.03
WHITECAP = 0.3
STEEP_SCALE = 0.4
STOKES_GAIN = 3.0
LANES = 128
SUB = 8
GROWTH_F = WIND_GAIN * 0.64


def bin_tables(levels):
    padded = -(-levels // SUB) * SUB
    heading = np.arange(NDIR) * (2.0 * math.pi / NDIR)
    freq = FIRST_FREQ * GROWTH ** np.arange(padded)
    rows = np.concatenate(
        [
            np.cos(heading),
            np.sin(heading),
            GROWTH_F * freq,
            freq**2,
            SPEED_TOP * FIRST_FREQ / freq,
            STOKES_GAIN * 0.1 * freq**4,
        ]
    )
    table = np.broadcast_to(rows[:, None], (rows.shape[0], LANES))
    return jnp.asarray(table.astype(np.float32)), padded


def split3(x):
    hi = x.astype(BF16)
    rest = x - hi.astype(F32)
    mid = rest.astype(BF16)
    low = (rest - mid.astype(F32)).astype(BF16)
    return jnp.concatenate([hi, mid, low], axis=0)


def sum3(x):
    n = x.shape[0] // 3
    return x[:n] + x[n : 2 * n] + x[2 * n :]


def kernel(
    n_grp,
    n_dev,
    levels,
    padded,
    chunks,
    head_chunks,
    spec_hbm,
    mask_hbm,
    wind_hbm,
    cur_hbm,
    coup_hbm,
    tab_hbm,
    upd_ref,
    drift,
    coup_ref,
    ctr,
    mask_ref,
    wind_ref,
    cur_ref,
    tab_ref,
    west,
    east,
    base,
    part,
    nbr,
    info,
    rtab,
    dtab,
    load_sem,
    halo_send,
    halo_recv,
    part_send,
    part_recv,
    nbr_send,
    nbr_recv,
    info_send,
    info_recv,
    drift_send,
    drift_recv,
):
    g = lax.axis_index("grp")
    d = lax.axis_index("dev")
    bins = levels * NDIR
    per = levels // chunks
    rows = per * NDIR
    quads = NDIR // SUB
    COS, SIN, FG = 0, NDIR, 2 * NDIR
    F2, GS, WT = FG + padded, FG + 2 * padded, FG + 3 * padded

    def at(step):
        return {"grp": g, "dev": lax.rem(d + step + n_dev, n_dev)}

    def group(step):
        return {"grp": lax.rem(g + step, n_grp), "dev": d}

    loads = [
        pltpu.make_async_copy(src, dst, load_sem.at[i])
        for i, (src, dst) in enumerate(
            (
                (coup_hbm, coup_ref),
                (cur_hbm, cur_ref),
                (spec_hbm, ctr),
                (tab_hbm, tab_ref),
                (mask_hbm, mask_ref),
                (wind_hbm, wind_ref),
            )
        )
    ]
    for load in loads:
        load.start()
    barrier = pltpu.get_barrier_semaphore()
    for k in range(1, n_grp):
        pl.semaphore_signal(barrier, inc=1, device_id=group(k), device_id_type=MESH)
    for k in (-2, -1, 1, 2):
        pl.semaphore_signal(barrier, inc=1, device_id=at(k), device_id_type=MESH)

    loads[0].wait()
    loads[1].wait()
    coup = coup_ref[...]
    slot = ((coup >> 7) - d + n_dev + 1) & (n_dev - 1)
    row = coup & (LANES - 1)
    cells = coup.shape[1]
    one_hot = jnp.where(
        lax.broadcasted_iota(jnp.int32, (LANES, cells), 0) == row, 1.0, 0.0
    ).astype(BF16)
    kind = lax.broadcasted_iota(jnp.int32, (2 * SUB, cells), 0)
    comp = kind & 3
    value = jnp.where(
        comp == 0, cur_ref[0:1, :], jnp.where(comp == 1, cur_ref[1:2, :], jnp.where(comp == 2, 1.0, 0.0))
    )
    value = jnp.where(jnp.logical_and((kind >> 2) == slot, g > 0), value, 0.0)
    sums = lax.dot_general(
        split3(value), one_hot, (((1,), (1,)), ((), ())), preferred_element_type=F32
    )
    part[g] = sum3(sums)

    for load in loads[2:]:
        load.wait()

    def add_level(l, acc):
        r = pl.multiple_of(l * NDIR, NDIR)
        e = ctr[pl.ds(r, SUB), :]
        for m in range(1, quads):
            e = e + ctr[pl.ds(r + m * SUB, SUB), :]
        return (
            acc[0] + e * tab_ref[pl.ds(FG + l, 1), :],
            acc[1] + e * tab_ref[pl.ds(F2 + l, 1), :],
        )

    zero = jnp.zeros((SUB, LANES), F32)
    total, moment = lax.fori_loop(0, levels, add_level, (zero, zero), unroll=4)
    sea = mask_ref[...].astype(F32)
    total = jnp.sum(total, axis=0, keepdims=True) * (0.1 / GROWTH_F) * sea
    moment = jnp.sum(moment, axis=0, keepdims=True) * 0.1 * sea
    is_sea = sea > 0.5
    mean_freq = jnp.where(is_sea, moment / jnp.where(is_sea, total, 1.0), 1.0)
    steepness = STEEP_SCALE * total * mean_freq**4
    damp = WHITECAP * (steepness / mean_freq) ** 2
    which = lax.broadcasted_iota(jnp.int32, (SUB, LANES), 0)
    info[1] = jnp.where(
        which == 0,
        sea,
        jnp.where(
            which == 1,
            damp,
            jnp.where(which == 2, wind_ref[0:1, :], jnp.where(which == 3, wind_ref[1:2, :], 0.0)),
        ),
    )

    pl.semaphore_wait(barrier, n_grp - 1 + 4)

    part_copies = []
    for k in range(1, n_grp):
        copy = pltpu.make_async_remote_copy(
            src_ref=part.at[g],
            dst_ref=part.at[g],
            send_sem=part_send.at[k],
            recv_sem=part_recv.at[g],
            device_id=group(k),
            device_id_type=MESH,
        )
        copy.start()
        part_copies.append(copy)
    info_copies = []
    for i, step in enumerate((1, -1)):
        copy = pltpu.make_async_remote_copy(
            src_ref=info.at[1],
            dst_ref=info.at[1 - step],
            send_sem=info_send.at[i],
            recv_sem=info_recv.at[i],
            device_id=at(step),
            device_id_type=MESH,
        )
        copy.start()
        info_copies.append(copy)

    halo_copies = []

    def send_chunk(k):
        for i, (step, there) in enumerate(((1, west), (-1, east))):
            copy = pltpu.make_async_remote_copy(
                src_ref=ctr.at[pl.ds(k * rows, rows), :],
                dst_ref=there.at[pl.ds(k * rows, rows), :],
                send_sem=halo_send.at[i, k],
                recv_sem=halo_recv.at[i, k],
                device_id=at(step),
                device_id_type=MESH,
            )
            copy.start()
            halo_copies.append(copy)

    for k in range(head_chunks):
        send_chunk(k)

    for k in range(1, n_grp):
        src = lax.rem(g - k + n_grp, n_grp)
        pltpu.make_async_remote_copy(
            src_ref=part.at[src],
            dst_ref=part.at[src],
            send_sem=part_send.at[k],
            recv_sem=part_recv.at[src],
            device_id=group(k),
            device_id_type=MESH,
        ).wait_recv()
    both = part[1]
    for k in range(2, n_grp):
        both = both + part[k]
    nbr[2] = both
    nbr_copies = []
    for i, step in enumerate((-2, -1, 1, 2)):
        copy = pltpu.make_async_remote_copy(
            src_ref=nbr.at[2],
            dst_ref=nbr.at[2 - step],
            send_sem=nbr_send.at[i],
            recv_sem=nbr_recv.at[i],
            device_id=at(step),
            device_id_type=MESH,
        )
        copy.start()
        nbr_copies.append(copy)
    for k in range(head_chunks, chunks):
        send_chunk(k)

    for copy in info_copies:
        copy.wait_recv()
    for copy in nbr_copies:
        copy.wait_recv()

    cos = [tab_ref[pl.ds(COS + m * SUB, SUB), :] for m in range(quads)]
    sin = [tab_ref[pl.ds(SIN + m * SUB, SUB), :] for m in range(quads)]
    flows = []
    for c in range(3):
        s4 = nbr[c + 1, 4:8, :] + nbr[c, 8:12, :] + nbr[c + 2, 0:4, :]
        count = jnp.maximum(s4[2:3], 1.0)
        mean_x = s4[0:1] / count
        mean_y = s4[1:2] / count
        flows.append((CURRENT_TOP * jnp.tanh(mean_x), CURRENT_TOP * jnp.tanh(mean_y)))
        sea_c = info[c, 0:1, :]
        damp_c = info[c, 1:2, :]
        wx = info[c, 2:3, :] - mean_x
        wy = info[c, 3:4, :] - mean_y
        for m in range(quads):
            dtab[c, pl.ds(m * SUB, SUB), :] = cos[m] * wx + sin[m] * wy
        for q in range(padded // SUB):
            f2 = tab_ref[pl.ds(F2 + q * SUB, SUB), :]
            rtab[c, pl.ds(q * SUB, SUB), :] = sea_c / (1.0 + f2 * damp_c)
    wide = (SUB, LANES)
    face_w = jnp.broadcast_to(0.5 * (flows[0][0] + flows[1][0]), wide)
    face_e = jnp.broadcast_to(0.5 * (flows[1][0] + flows[2][0]), wide)
    flow_y = jnp.broadcast_to(flows[1][1], wide)
    face_n = 0.5 * (flow_y + pltpu.roll(flow_y, LANES - 1, 1))
    sea_w = jnp.broadcast_to(sea, wide)
    inner = lax.broadcasted_iota(jnp.int32, wide, 1) < LANES - 1
    gain = [[dtab[c, pl.ds(m * SUB, SUB), :] for m in range(quads)] for c in range(3)]

    def forced(energy, c, m, fg, rec):
        return energy * (jnp.maximum(gain[c][m] * fg + (1.0 - WIND_GAIN), 1.0) * rec)

    def own_level(l, carry):
        fg = tab_ref[pl.ds(FG + l, 1), :]
        gs = tab_ref[pl.ds(GS + l, 1), :]
        rec = rtab[1, pl.ds(l, 1), :]
        for m in range(quads):
            r = pl.ds(pl.multiple_of(l * NDIR + m * SUB, SUB), SUB)
            e = forced(ctr[r, :], 1, m, fg, rec)
            a = jnp.where(inner, gs * sin[m] + face_n, 0.0)
            flux = a * jnp.where(a > 0.0, e, pltpu.roll(e, LANES - 1, 1))
            own = (e - flux) + pltpu.roll(flux, 1, 1)
            base[0, r, :] = e
            base[1, r, :] = own
        return carry

    lax.fori_loop(0, levels, own_level, 0, unroll=2)

    def edge_level(l, acc):
        fg = tab_ref[pl.ds(FG + l, 1), :]
        gs = tab_ref[pl.ds(GS + l, 1), :]
        wt = tab_ref[pl.ds(WT + l, 1), :]
        rec_w = rtab[0, pl.ds(l, 1), :]
        rec_e = rtab[2, pl.ds(l, 1), :]
        out = []
        for m in range(quads):
            r = pl.ds(pl.multiple_of(l * NDIR + m * SUB, SUB), SUB)
            e = base[0, r, :]
            ew = forced(west[r, :], 0, m, fg, rec_w)
            ee = forced(east[r, :], 2, m, fg, rec_e)
            speed = gs * cos[m]
            a = speed + face_e
            b = speed + face_w
            flux_e = a * jnp.where(a > 0.0, e, ee)
            flux_w = b * jnp.where(b > 0.0, ew, e)
            u = sea_w * (base[1, r, :] - flux_e + flux_w)
            upd_ref[r, :] = u
            out.append(acc[m] + wt * u)
        return tuple(out)

    acc = (zero,) * quads
    for k in range(chunks):
        for copy in halo_copies[2 * k : 2 * k + 2]:
            copy.wait_recv()
        acc = lax.fori_loop(k * per, (k + 1) * per, edge_level, acc, unroll=2)

    dx = acc[0] * cos[0]
    dy = acc[0] * sin[0]
    for m in range(1, quads):
        dx = dx + acc[m] * cos[m]
        dy = dy + acc[m] * sin[m]
    drift[1] = jnp.where(
        which == 0,
        jnp.sum(dx, axis=0, keepdims=True),
        jnp.where(which == 1, jnp.sum(dy, axis=0, keepdims=True), 0.0),
    )
    drift_copies = []
    for i, step in enumerate((1, -1)):
        copy = pltpu.make_async_remote_copy(
            src_ref=drift.at[1],
            dst_ref=drift.at[1 - step],
            send_sem=drift_send.at[i],
            recv_sem=drift_recv.at[i],
            device_id=at(step),
            device_id_type=MESH,
        )
        copy.start()
        drift_copies.append(copy)
    for copy in part_copies + info_copies + nbr_copies + halo_copies:
        copy.wait_send()
    for copy in drift_copies:
        copy.wait()


def finish(upd_ref, drift, coup_ref, upd_hbm, cell_hbm, cell_ref, sem):
    g = lax.axis_index("grp")
    d = lax.axis_index("dev")
    n_dev = lax.axis_size("dev")
    store = pltpu.make_async_copy(upd_ref, upd_hbm, sem.at[0])
    store.start()
    coup = coup_ref[...]
    cells = coup.shape[1]
    slot = ((coup >> 7) - d + n_dev + 1) & (n_dev - 1)
    row = coup & (LANES - 1)
    one_hot = jnp.where(
        lax.broadcasted_iota(jnp.int32, (LANES, cells), 0) == row, 1.0, 0.0
    ).astype(BF16)
    band = jnp.zeros((2 * SUB, LANES), F32)
    place = lax.broadcasted_iota(jnp.int32, (2 * SUB, LANES), 0)
    for c in range(3):
        for v in range(2):
            band = jnp.where(place == 4 * c + v, drift[c, v : v + 1, :], band)
    picked = sum3(jnp.dot(split3(band), one_hot, preferred_element_type=F32))
    for v in range(2):
        out = jnp.where(
            slot == 0,
            picked[v : v + 1],
            jnp.where(slot == 1, picked[4 + v : 5 + v], picked[8 + v : 9 + v]),
        )
        cell_ref[v : v + 1, :] = jnp.where(g > 0, out, 0.0)
    cell_store = pltpu.make_async_copy(cell_ref, cell_hbm, sem.at[1])
    cell_store.start()
    cell_store.wait()
    store.wait()


def body(n_grp, n_dev, spectrum, sea_mask, wind, currents, coupling):
    bins, _, width = spectrum.shape
    levels = bins // NDIR
    cells = currents.shape[2]
    table, padded = bin_tables(levels)
    chunks, head_chunks = 6, 2
    vmem = pl.BlockSpec(memory_space=pltpu.VMEM)
    hbm = pl.BlockSpec(memory_space=pltpu.HBM)
    dma = pltpu.SemaphoreType.DMA
    updated, drift, coup = pl.pallas_call(
        functools.partial(kernel, n_grp, n_dev, levels, padded, chunks, head_chunks),
        out_shape=(
            jax.ShapeDtypeStruct((bins, width), F32),
            jax.ShapeDtypeStruct((3, SUB, width), F32),
            jax.ShapeDtypeStruct((1, cells), jnp.int32),
        ),
        in_specs=[hbm] * 6,
        out_specs=(vmem, vmem, vmem),
        scratch_shapes=[
            pltpu.VMEM((bins, width), F32),
            pltpu.VMEM((1, width), jnp.int32),
            pltpu.VMEM((2, width), F32),
            pltpu.VMEM((2, cells), F32),
            pltpu.VMEM(table.shape, F32),
            pltpu.VMEM((bins, width), F32),
            pltpu.VMEM((bins, width), F32),
            pltpu.VMEM((2, bins, width), F32),
            pltpu.VMEM((n_grp, 2 * SUB, width), F32),
            pltpu.VMEM((5, 2 * SUB, width), F32),
            pltpu.VMEM((3, SUB, width), F32),
            pltpu.VMEM((3, padded, width), F32),
            pltpu.VMEM((3, NDIR, width), F32),
            dma((6,)),
            dma((2, chunks)),
            dma((2, chunks)),
            dma((n_grp,)),
            dma((n_grp,)),
            dma((4,)),
            dma((4,)),
            dma((2,)),
            dma((2,)),
            dma((2,)),
            dma((2,)),
        ],
        compiler_params=pltpu.CompilerParams(
            collective_id=0, has_side_effects=True, vmem_limit_bytes=32 * 1024 * 1024
        ),
        name="wave_step",
    )(
        *[
            pltpu.with_memory_space_constraint(x, pltpu.HBM)
            for x in (
                spectrum.reshape(bins, width),
                sea_mask,
                wind.reshape(2, width),
                currents.reshape(2, cells),
                coupling,
                table,
            )
        ]
    )
    updated, cell_drift = pl.pallas_call(
        finish,
        out_shape=(
            jax.ShapeDtypeStruct((bins, width), F32),
            jax.ShapeDtypeStruct((2, cells), F32),
        ),
        in_specs=[vmem, vmem, vmem],
        out_specs=(hbm, hbm),
        scratch_shapes=[pltpu.VMEM((2, cells), F32), dma((2,))],
        compiler_params=pltpu.CompilerParams(vmem_limit_bytes=16 * 1024 * 1024),
        name="finish",
    )(updated, drift, coup)
    return updated.reshape(bins, 1, width), cell_drift.reshape(1, 2, cells)


def solution(mesh):
    return jax.shard_map(
        functools.partial(body, mesh.shape["grp"], mesh.shape["dev"]),
        mesh=mesh,
        in_specs=(
            P(None, "dev", None),
            P("dev", None),
            P(None, "dev", None),
            P("grp", None, "dev"),
            P("grp", "dev"),
        ),
        out_specs=(P(None, "dev", None), P("grp", None, "dev")),
        check_vma=False,
    )
```

```python
import functools
import math

import jax
import jax.numpy as jnp
import numpy as np
from jax import lax
from jax.experimental import pallas as pl
from jax.experimental.pallas import tpu as pltpu
from jax.sharding import PartitionSpec as P

MESH = pl.DeviceIdType.MESH
F32 = jnp.float32
BF16 = jnp.bfloat16

NDIR = 32
FIRST_FREQ = 0.04
GROWTH = 1.1
SPEED_TOP = 0.45
CURRENT_TOP = 0.2
WIND_GAIN = 0.03
WHITECAP = 0.3
STEEP_SCALE = 0.4
STOKES_GAIN = 3.0
LANES = 128
SUB = 8
GROWTH_F = WIND_GAIN * 0.64


def bin_tables(levels):
    padded = -(-levels // SUB) * SUB
    heading = np.arange(NDIR) * (2.0 * math.pi / NDIR)
    freq = FIRST_FREQ * GROWTH ** np.arange(padded)
    rows = np.concatenate(
        [
            np.cos(heading),
            np.sin(heading),
            GROWTH_F * freq,
            freq**2,
            SPEED_TOP * FIRST_FREQ / freq,
            STOKES_GAIN * 0.1 * freq**4,
        ]
    )
    table = np.broadcast_to(rows[:, None], (rows.shape[0], LANES))
    return jnp.asarray(table.astype(np.float32)), padded


def split3(x):
    hi = x.astype(BF16)
    rest = x - hi.astype(F32)
    mid = rest.astype(BF16)
    low = (rest - mid.astype(F32)).astype(BF16)
    return jnp.concatenate([hi, mid, low], axis=0)


def sum3(x):
    n = x.shape[0] // 3
    return x[:n] + x[n : 2 * n] + x[2 * n :]


def kernel(
    n_grp,
    n_dev,
    levels,
    padded,
    chunks,
    head_chunks,
    spec_hbm,
    mask_hbm,
    wind_hbm,
    cur_hbm,
    coup_hbm,
    tab_hbm,
    upd_ref,
    drift,
    where_ref,
    ctr,
    coup_ref,
    mask_ref,
    wind_ref,
    cur_ref,
    tab_ref,
    west,
    east,
    base,
    part,
    nbr,
    info,
    rtab,
    dtab,
    load_sem,
    halo_send,
    halo_recv,
    part_send,
    part_recv,
    nbr_send,
    nbr_recv,
    info_send,
    info_recv,
    drift_send,
    drift_recv,
):
    g = lax.axis_index("grp")
    d = lax.axis_index("dev")
    bins = levels * NDIR
    per = levels // chunks
    rows = per * NDIR
    quads = NDIR // SUB
    COS, SIN, FG = 0, NDIR, 2 * NDIR
    F2, GS, WT = FG + padded, FG + 2 * padded, FG + 3 * padded

    def at(step):
        return {"grp": g, "dev": lax.rem(d + step + n_dev, n_dev)}

    def group(step):
        return {"grp": lax.rem(g + step, n_grp), "dev": d}

    loads = [
        pltpu.make_async_copy(src, dst, load_sem.at[i])
        for i, (src, dst) in enumerate(
            (
                (coup_hbm, coup_ref),
                (cur_hbm, cur_ref),
                (spec_hbm, ctr),
                (tab_hbm, tab_ref),
                (mask_hbm, mask_ref),
                (wind_hbm, wind_ref),
            )
        )
    ]
    for load in loads:
        load.start()
    barrier = pltpu.get_barrier_semaphore()
    for k in range(1, n_grp):
        pl.semaphore_signal(barrier, inc=1, device_id=group(k), device_id_type=MESH)
    for k in (-2, -1, 1, 2):
        pl.semaphore_signal(barrier, inc=1, device_id=at(k), device_id_type=MESH)

    loads[0].wait()
    loads[1].wait()
    coup = coup_ref[...]
    slot = ((coup >> 7) - d + n_dev + 1) & (n_dev - 1)
    row = coup & (LANES - 1)
    cells = coup.shape[1]
    one_hot = jnp.where(
        lax.broadcasted_iota(jnp.int32, (LANES, cells), 0) == row, 1.0, 0.0
    ).astype(BF16)
    kind = lax.broadcasted_iota(jnp.int32, (2 * SUB, cells), 0)
    comp = kind & 3
    value = jnp.where(
        comp == 0, cur_ref[0:1, :], jnp.where(comp == 1, cur_ref[1:2, :], jnp.where(comp == 2, 1.0, 0.0))
    )
    value = jnp.where(jnp.logical_and((kind >> 2) == slot, g > 0), value, 0.0)
    sums = lax.dot_general(
        split3(value), one_hot, (((1,), (1,)), ((), ())), preferred_element_type=F32
    )
    part[g] = sum3(sums)
    where_ref[0:1, :] = jnp.where(g > 0, slot, 3)
    where_ref[1:2, :] = row

    for load in loads[2:]:
        load.wait()

    def add_level(l, acc):
        r = pl.multiple_of(l * NDIR, NDIR)
        e = ctr[pl.ds(r, SUB), :]
        for m in range(1, quads):
            e = e + ctr[pl.ds(r + m * SUB, SUB), :]
        return (
            acc[0] + e * tab_ref[pl.ds(FG + l, 1), :],
            acc[1] + e * tab_ref[pl.ds(F2 + l, 1), :],
        )

    zero = jnp.zeros((SUB, LANES), F32)
    total, moment = lax.fori_loop(0, levels, add_level, (zero, zero), unroll=4)
    sea = mask_ref[...].astype(F32)
    total = jnp.sum(total, axis=0, keepdims=True) * (0.1 / GROWTH_F) * sea
    moment = jnp.sum(moment, axis=0, keepdims=True) * 0.1 * sea
    is_sea = sea > 0.5
    mean_freq = jnp.where(is_sea, moment / jnp.where(is_sea, total, 1.0), 1.0)
    steepness = STEEP_SCALE * total * mean_freq**4
    damp = WHITECAP * (steepness / mean_freq) ** 2
    which = lax.broadcasted_iota(jnp.int32, (SUB, LANES), 0)
    info[1] = jnp.where(
        which == 0,
        sea,
        jnp.where(
            which == 1,
            damp,
            jnp.where(which == 2, wind_ref[0:1, :], jnp.where(which == 3, wind_ref[1:2, :], 0.0)),
        ),
    )

    pl.semaphore_wait(barrier, n_grp - 1 + 4)

    part_copies = []
    for k in range(1, n_grp):
        copy = pltpu.make_async_remote_copy(
            src_ref=part.at[g],
            dst_ref=part.at[g],
            send_sem=part_send.at[k],
            recv_sem=part_recv.at[g],
            device_id=group(k),
            device_id_type=MESH,
        )
        copy.start()
        part_copies.append(copy)
    info_copies = []
    for i, step in enumerate((1, -1)):
        copy = pltpu.make_async_remote_copy(
            src_ref=info.at[1],
            dst_ref=info.at[1 - step],
            send_sem=info_send.at[i],
            recv_sem=info_recv.at[i],
            device_id=at(step),
            device_id_type=MESH,
        )
        copy.start()
        info_copies.append(copy)

    halo_copies = []

    def send_chunk(k):
        for i, (step, there) in enumerate(((1, west), (-1, east))):
            copy = pltpu.make_async_remote_copy(
                src_ref=ctr.at[pl.ds(k * rows, rows), :],
                dst_ref=there.at[pl.ds(k * rows, rows), :],
                send_sem=halo_send.at[i, k],
                recv_sem=halo_recv.at[i, k],
                device_id=at(step),
                device_id_type=MESH,
            )
            copy.start()
            halo_copies.append(copy)

    for k in range(head_chunks):
        send_chunk(k)

    for k in range(1, n_grp):
        src = lax.rem(g - k + n_grp, n_grp)
        pltpu.make_async_remote_copy(
            src_ref=part.at[src],
            dst_ref=part.at[src],
            send_sem=part_send.at[k],
            recv_sem=part_recv.at[src],
            device_id=group(k),
            device_id_type=MESH,
        ).wait_recv()
    both = part[1]
    for k in range(2, n_grp):
        both = both + part[k]
    nbr[2] = both
    nbr_copies = []
    for i, step in enumerate((-2, -1, 1, 2)):
        copy = pltpu.make_async_remote_copy(
            src_ref=nbr.at[2],
            dst_ref=nbr.at[2 - step],
            send_sem=nbr_send.at[i],
            recv_sem=nbr_recv.at[i],
            device_id=at(step),
            device_id_type=MESH,
        )
        copy.start()
        nbr_copies.append(copy)
    for k in range(head_chunks, chunks):
        send_chunk(k)

    for copy in info_copies:
        copy.wait_recv()
    for copy in nbr_copies:
        copy.wait_recv()

    cos = [tab_ref[pl.ds(COS + m * SUB, SUB), :] for m in range(quads)]
    sin = [tab_ref[pl.ds(SIN + m * SUB, SUB), :] for m in range(quads)]
    flows = []
    for c in range(3):
        s4 = nbr[c + 1, 4:8, :] + nbr[c, 8:12, :] + nbr[c + 2, 0:4, :]
        count = jnp.maximum(s4[2:3], 1.0)
        mean_x = s4[0:1] / count
        mean_y = s4[1:2] / count
        flows.append((CURRENT_TOP * jnp.tanh(mean_x), CURRENT_TOP * jnp.tanh(mean_y)))
        sea_c = info[c, 0:1, :]
        damp_c = info[c, 1:2, :]
        wx = info[c, 2:3, :] - mean_x
        wy = info[c, 3:4, :] - mean_y
        for m in range(quads):
            dtab[c, pl.ds(m * SUB, SUB), :] = cos[m] * wx + sin[m] * wy
        for q in range(padded // SUB):
            f2 = tab_ref[pl.ds(F2 + q * SUB, SUB), :]
            rtab[c, pl.ds(q * SUB, SUB), :] = sea_c / (1.0 + f2 * damp_c)
    wide = (SUB, LANES)
    face_w = jnp.broadcast_to(0.5 * (flows[0][0] + flows[1][0]), wide)
    face_e = jnp.broadcast_to(0.5 * (flows[1][0] + flows[2][0]), wide)
    flow_y = jnp.broadcast_to(flows[1][1], wide)
    face_n = 0.5 * (flow_y + pltpu.roll(flow_y, LANES - 1, 1))
    face_s = 0.5 * (flow_y + pltpu.roll(flow_y, 1, 1))
    sea_w = jnp.broadcast_to(sea, wide)
    lane = lax.broadcasted_iota(jnp.int32, wide, 1)
    has_n = lane < LANES - 1
    has_s = lane > 0
    gain = [[dtab[c, pl.ds(m * SUB, SUB), :] for m in range(quads)] for c in range(3)]

    def forced(energy, c, m, fg, rec):
        return energy * (jnp.maximum(gain[c][m] * fg + (1.0 - WIND_GAIN), 1.0) * rec)

    def own_level(l, carry):
        fg = tab_ref[pl.ds(FG + l, 1), :]
        gs = tab_ref[pl.ds(GS + l, 1), :]
        rec = rtab[1, pl.ds(l, 1), :]
        for m in range(quads):
            r = pl.ds(pl.multiple_of(l * NDIR + m * SUB, SUB), SUB)
            e = forced(ctr[r, :], 1, m, fg, rec)
            speed = gs * sin[m]
            a = jnp.where(has_n, speed + face_n, 0.0)
            b = jnp.where(has_s, speed + face_s, 0.0)
            flux_n = a * jnp.where(a > 0.0, e, pltpu.roll(e, LANES - 1, 1))
            flux_s = b * jnp.where(b > 0.0, pltpu.roll(e, 1, 1), e)
            base[0, r, :] = e
            base[1, r, :] = e - flux_n + flux_s
        return carry

    lax.fori_loop(0, levels, own_level, 0, unroll=per)

    def edge_level(l, acc):
        fg = tab_ref[pl.ds(FG + l, 1), :]
        gs = tab_ref[pl.ds(GS + l, 1), :]
        wt = tab_ref[pl.ds(WT + l, 1), :]
        rec_w = rtab[0, pl.ds(l, 1), :]
        rec_e = rtab[2, pl.ds(l, 1), :]
        out = []
        for m in range(quads):
            r = pl.ds(pl.multiple_of(l * NDIR + m * SUB, SUB), SUB)
            e = base[0, r, :]
            ew = forced(west[r, :], 0, m, fg, rec_w)
            ee = forced(east[r, :], 2, m, fg, rec_e)
            speed = gs * cos[m]
            a = speed + face_e
            b = speed + face_w
            flux_e = a * jnp.where(a > 0.0, e, ee)
            flux_w = b * jnp.where(b > 0.0, ew, e)
            u = sea_w * (base[1, r, :] - flux_e + flux_w)
            upd_ref[r, :] = u
            out.append(acc[m] + wt * u)
        return tuple(out)

    acc = (zero,) * quads
    for k in range(chunks):
        for copy in halo_copies[2 * k : 2 * k + 2]:
            copy.wait_recv()
        acc = lax.fori_loop(k * per, (k + 1) * per, edge_level, acc, unroll=per)

    dx = acc[0] * cos[0]
    dy = acc[0] * sin[0]
    for m in range(1, quads):
        dx = dx + acc[m] * cos[m]
        dy = dy + acc[m] * sin[m]
    drift[1] = jnp.where(
        which == 0,
        jnp.sum(dx, axis=0, keepdims=True),
        jnp.where(which == 1, jnp.sum(dy, axis=0, keepdims=True), 0.0),
    )
    drift_copies = []
    for i, step in enumerate((1, -1)):
        copy = pltpu.make_async_remote_copy(
            src_ref=drift.at[1],
            dst_ref=drift.at[1 - step],
            send_sem=drift_send.at[i],
            recv_sem=drift_recv.at[i],
            device_id=at(step),
            device_id_type=MESH,
        )
        copy.start()
        drift_copies.append(copy)
    for copy in part_copies + info_copies + nbr_copies + halo_copies:
        copy.wait_send()
    for copy in drift_copies:
        copy.wait()


def finish(upd_ref, drift, where_ref, upd_hbm, cell_hbm, cell_ref, sem):
    store = pltpu.make_async_copy(upd_ref, upd_hbm, sem.at[0])
    store.start()
    slot = where_ref[0:1, :]
    row = where_ref[1:2, :]
    cells = row.shape[1]
    one_hot = jnp.where(
        lax.broadcasted_iota(jnp.int32, (LANES, cells), 0) == row, 1.0, 0.0
    ).astype(BF16)
    band = jnp.zeros((2 * SUB, LANES), F32)
    place = lax.broadcasted_iota(jnp.int32, (2 * SUB, LANES), 0)
    for c in range(3):
        for v in range(2):
            band = jnp.where(place == 4 * c + v, drift[c, v : v + 1, :], band)
    picked = sum3(jnp.dot(split3(band), one_hot, preferred_element_type=F32))
    for v in range(2):
        out = jnp.where(slot == 2, picked[8 + v : 9 + v], 0.0)
        out = jnp.where(slot == 1, picked[4 + v : 5 + v], out)
        cell_ref[v : v + 1, :] = jnp.where(slot == 0, picked[v : v + 1], out)
    cell_store = pltpu.make_async_copy(cell_ref, cell_hbm, sem.at[1])
    cell_store.start()
    cell_store.wait()
    store.wait()


def body(n_grp, n_dev, spectrum, sea_mask, wind, currents, coupling):
    bins, _, width = spectrum.shape
    levels = bins // NDIR
    cells = currents.shape[2]
    table, padded = bin_tables(levels)
    chunks, head_chunks = 6, 4
    vmem = pl.BlockSpec(memory_space=pltpu.VMEM)
    hbm = pl.BlockSpec(memory_space=pltpu.HBM)
    dma = pltpu.SemaphoreType.DMA
    updated, drift, where = pl.pallas_call(
        functools.partial(kernel, n_grp, n_dev, levels, padded, chunks, head_chunks),
        out_shape=(
            jax.ShapeDtypeStruct((bins, width), F32),
            jax.ShapeDtypeStruct((3, SUB, width), F32),
            jax.ShapeDtypeStruct((2, cells), jnp.int32),
        ),
        in_specs=[hbm] * 6,
        out_specs=(vmem, vmem, vmem),
        scratch_shapes=[
            pltpu.VMEM((bins, width), F32),
            pltpu.VMEM((1, cells), jnp.int32),
            pltpu.VMEM((1, width), jnp.int32),
            pltpu.VMEM((2, width), F32),
            pltpu.VMEM((2, cells), F32),
            pltpu.VMEM(table.shape, F32),
            pltpu.VMEM((bins, width), F32),
            pltpu.VMEM((bins, width), F32),
            pltpu.VMEM((2, bins, width), F32),
            pltpu.VMEM((n_grp, 2 * SUB, width), F32),
            pltpu.VMEM((5, 2 * SUB, width), F32),
            pltpu.VMEM((3, SUB, width), F32),
            pltpu.VMEM((3, padded, width), F32),
            pltpu.VMEM((3, NDIR, width), F32),
            dma((6,)),
            dma((2, chunks)),
            dma((2, chunks)),
            dma((n_grp,)),
            dma((n_grp,)),
            dma((4,)),
            dma((4,)),
            dma((2,)),
            dma((2,)),
            dma((2,)),
            dma((2,)),
        ],
        compiler_params=pltpu.CompilerParams(
            collective_id=0, has_side_effects=True, vmem_limit_bytes=32 * 1024 * 1024
        ),
        name="wave_step",
    )(
        *[
            pltpu.with_memory_space_constraint(x, pltpu.HBM)
            for x in (
                spectrum.reshape(bins, width),
                sea_mask,
                wind.reshape(2, width),
                currents.reshape(2, cells),
                coupling,
                table,
            )
        ]
    )
    updated, cell_drift = pl.pallas_call(
        finish,
        out_shape=(
            jax.ShapeDtypeStruct((bins, width), F32),
            jax.ShapeDtypeStruct((2, cells), F32),
        ),
        in_specs=[vmem, vmem, vmem],
        out_specs=(hbm, hbm),
        scratch_shapes=[pltpu.VMEM((2, cells), F32), dma((2,))],
        compiler_params=pltpu.CompilerParams(vmem_limit_bytes=16 * 1024 * 1024),
        name="finish",
    )(updated, drift, where)
    return updated.reshape(bins, 1, width), cell_drift.reshape(1, 2, cells)


def solution(mesh):
    return jax.shard_map(
        functools.partial(body, mesh.shape["grp"], mesh.shape["dev"]),
        mesh=mesh,
        in_specs=(
            P(None, "dev", None),
            P("dev", None),
            P(None, "dev", None),
            P("grp", None, "dev"),
            P("grp", "dev"),
        ),
        out_specs=(P(None, "dev", None), P("grp", None, "dev")),
        check_vma=False,
    )
```

```python
import functools
import math

import jax
import jax.numpy as jnp
import numpy as np
from jax import lax
from jax.experimental import pallas as pl
from jax.experimental.pallas import tpu as pltpu
from jax.sharding import PartitionSpec as P

MESH = pl.DeviceIdType.MESH
F32 = jnp.float32
BF16 = jnp.bfloat16

NDIR = 32
FIRST_FREQ = 0.04
GROWTH = 1.1
SPEED_TOP = 0.45
CURRENT_TOP = 0.2
WIND_GAIN = 0.03
WHITECAP = 0.3
STEEP_SCALE = 0.4
STOKES_GAIN = 3.0
LANES = 128
SUB = 8
GROWTH_F = WIND_GAIN * 0.64


def bin_tables(levels):
    padded = -(-levels // SUB) * SUB
    heading = np.arange(NDIR) * (2.0 * math.pi / NDIR)
    freq = FIRST_FREQ * GROWTH ** np.arange(padded)
    rows = np.concatenate(
        [
            np.cos(heading),
            np.sin(heading),
            GROWTH_F * freq,
            freq**2,
            SPEED_TOP * FIRST_FREQ / freq,
            STOKES_GAIN * 0.1 * freq**4,
        ]
    )
    table = np.broadcast_to(rows[:, None], (rows.shape[0], LANES))
    return jnp.asarray(table.astype(np.float32)), padded


def split3(x):
    hi = x.astype(BF16)
    rest = x - hi.astype(F32)
    mid = rest.astype(BF16)
    low = (rest - mid.astype(F32)).astype(BF16)
    return jnp.concatenate([hi, mid, low], axis=0)


def sum3(x):
    n = x.shape[0] // 3
    return x[:n] + x[n : 2 * n] + x[2 * n :]


def kernel(
    n_grp,
    n_dev,
    levels,
    padded,
    chunks,
    head_chunks,
    spec_hbm,
    mask_hbm,
    wind_hbm,
    cur_hbm,
    coup_hbm,
    tab_hbm,
    upd_ref,
    drift_ref,
    where_ref,
    ctr,
    coup_ref,
    mask_ref,
    wind_ref,
    cur_ref,
    tab_ref,
    near,
    far,
    base,
    part,
    nbr,
    info,
    drift,
    last,
    rtab,
    dtab,
    load_sem,
    halo_send,
    halo_recv,
    part_send,
    part_recv,
    nbr_send,
    nbr_recv,
    info_send,
    info_recv,
    drift_send,
    drift_recv,
):
    g = lax.axis_index("grp")
    d = lax.axis_index("dev")
    side = 2 * lax.rem(d, 2) - 1

    bins = levels * NDIR
    per = levels // chunks
    rows = per * NDIR
    quads = NDIR // SUB
    COS, SIN, FG = 0, NDIR, 2 * NDIR
    F2, GS, WT = FG + padded, FG + 2 * padded, FG + 3 * padded

    def at(step):
        return {"grp": g, "dev": lax.rem(d + step + n_dev, n_dev)}

    def group(step):
        return {"grp": lax.rem(g + step, n_grp), "dev": d}

    loads = [
        pltpu.make_async_copy(src, dst, load_sem.at[i])
        for i, (src, dst) in enumerate(
            (
                (coup_hbm, coup_ref),
                (cur_hbm, cur_ref),
                (spec_hbm, ctr),
                (tab_hbm, tab_ref),
                (mask_hbm, mask_ref),
                (wind_hbm, wind_ref),
            )
        )
    ]
    for load in loads:
        load.start()
    barrier = pltpu.get_barrier_semaphore()
    for k in range(1, n_grp):
        pl.semaphore_signal(barrier, inc=1, device_id=group(k), device_id_type=MESH)
    for k in (-2, -1, 1, 2):
        pl.semaphore_signal(barrier, inc=1, device_id=at(k), device_id_type=MESH)

    loads[0].wait()
    loads[1].wait()
    coup = coup_ref[...]
    slot = ((coup >> 7) - d + n_dev + 1) & (n_dev - 1)
    row = coup & (LANES - 1)
    cells = coup.shape[1]
    one_hot = jnp.where(
        lax.broadcasted_iota(jnp.int32, (LANES, cells), 0) == row, 1.0, 0.0
    ).astype(BF16)
    kind = lax.broadcasted_iota(jnp.int32, (2 * SUB, cells), 0)
    comp = kind & 3
    value = jnp.where(
        comp == 0, cur_ref[0:1, :], jnp.where(comp == 1, cur_ref[1:2, :], jnp.where(comp == 2, 1.0, 0.0))
    )
    value = jnp.where(jnp.logical_and((kind >> 2) == slot, g > 0), value, 0.0)
    sums = lax.dot_general(
        split3(value), one_hot, (((1,), (1,)), ((), ())), preferred_element_type=F32
    )
    part[g] = sum3(sums)
    where_ref[0:1, :] = jnp.where(g > 0, 1 + (slot - 1) * side, 3)
    where_ref[1:2, :] = row

    for load in loads[2:]:
        load.wait()

    def add_level(l, acc):
        r = pl.multiple_of(l * NDIR, NDIR)
        e = ctr[pl.ds(r, SUB), :]
        for m in range(1, quads):
            e = e + ctr[pl.ds(r + m * SUB, SUB), :]
        return (
            acc[0] + e * tab_ref[pl.ds(FG + l, 1), :],
            acc[1] + e * tab_ref[pl.ds(F2 + l, 1), :],
        )

    zero = jnp.zeros((SUB, LANES), F32)
    total, moment = lax.fori_loop(0, levels, add_level, (zero, zero), unroll=4)
    sea = mask_ref[...].astype(F32)
    total = jnp.sum(total, axis=0, keepdims=True) * (0.1 / GROWTH_F) * sea
    moment = jnp.sum(moment, axis=0, keepdims=True) * 0.1 * sea
    is_sea = sea > 0.5
    mean_freq = jnp.where(is_sea, moment / jnp.where(is_sea, total, 1.0), 1.0)
    steepness = STEEP_SCALE * total * mean_freq**4
    damp = WHITECAP * (steepness / mean_freq) ** 2
    which = lax.broadcasted_iota(jnp.int32, (SUB, LANES), 0)
    info[1] = jnp.where(
        which == 0,
        sea,
        jnp.where(
            which == 1,
            damp,
            jnp.where(which == 2, wind_ref[0:1, :], jnp.where(which == 3, wind_ref[1:2, :], 0.0)),
        ),
    )

    pl.semaphore_wait(barrier, n_grp - 1 + 4)

    part_copies = []
    for k in range(1, n_grp):
        copy = pltpu.make_async_remote_copy(
            src_ref=part.at[g],
            dst_ref=part.at[g],
            send_sem=part_send.at[k],
            recv_sem=part_recv.at[g],
            device_id=group(k),
            device_id_type=MESH,
        )
        copy.start()
        part_copies.append(copy)
    info_copies = []
    for i, step in ((1, side), (0, -side)):
        copy = pltpu.make_async_remote_copy(
            src_ref=info.at[1],
            dst_ref=info.at[2 * i],
            send_sem=info_send.at[i],
            recv_sem=info_recv.at[i],
            device_id=at(step),
            device_id_type=MESH,
        )
        copy.start()
        info_copies.append(copy)

    far_copies = []

    def send_far(k):
        copy = pltpu.make_async_remote_copy(
            src_ref=ctr.at[pl.ds(k * rows, rows), :],
            dst_ref=far.at[pl.ds(k * rows, rows), :],
            send_sem=halo_send.at[k],
            recv_sem=halo_recv.at[k],
            device_id=at(side),
            device_id_type=MESH,
        )
        copy.start()
        far_copies.append(copy)

    send_far(0)
    near_copy = pltpu.make_async_remote_copy(
        src_ref=ctr,
        dst_ref=near,
        send_sem=halo_send.at[chunks],
        recv_sem=halo_recv.at[chunks],
        device_id=at(-side),
        device_id_type=MESH,
    )
    near_copy.start()
    for k in range(1, head_chunks):
        send_far(k)

    for k in range(1, n_grp):
        src = lax.rem(g - k + n_grp, n_grp)
        pltpu.make_async_remote_copy(
            src_ref=part.at[src],
            dst_ref=part.at[src],
            send_sem=part_send.at[k],
            recv_sem=part_recv.at[src],
            device_id=group(k),
            device_id_type=MESH,
        ).wait_recv()
    both = part[1]
    for k in range(2, n_grp):
        both = both + part[k]
    nbr[2] = both
    nbr_copies = []
    for i, step in enumerate((-2, -1, 1, 2)):
        copy = pltpu.make_async_remote_copy(
            src_ref=nbr.at[2],
            dst_ref=nbr.at[2 - step],
            send_sem=nbr_send.at[i],
            recv_sem=nbr_recv.at[i],
            device_id=at(step),
            device_id_type=MESH,
        )
        copy.start()
        nbr_copies.append(copy)
    for k in range(head_chunks, chunks):
        send_far(k)

    for copy in info_copies:
        copy.wait_recv()
    for copy in nbr_copies:
        copy.wait_recv()

    cos = [tab_ref[pl.ds(COS + m * SUB, SUB), :] for m in range(quads)]
    sin = [tab_ref[pl.ds(SIN + m * SUB, SUB), :] for m in range(quads)]
    flows = []
    seas = []
    for c in range(3):
        o = (c - 1) * side
        s4 = nbr[o + 2, 4:8, :] + nbr[o + 1, 8:12, :] + nbr[o + 3, 0:4, :]
        count = jnp.maximum(s4[2:3], 1.0)
        mean_x = s4[0:1] / count
        mean_y = s4[1:2] / count
        flows.append(CURRENT_TOP * jnp.tanh(mean_x))
        if c == 1:
            flow_y = CURRENT_TOP * jnp.tanh(mean_y)
        sea_c = info[c, 0:1, :]
        damp_c = info[c, 1:2, :]
        seas.append(sea_c)
        wx = info[c, 2:3, :] - mean_x
        wy = info[c, 3:4, :] - mean_y
        for m in range(quads):
            dtab[c, pl.ds(m * SUB, SUB), :] = cos[m] * wx + sin[m] * wy
        for q in range(padded // SUB):
            f2 = tab_ref[pl.ds(F2 + q * SUB, SUB), :]
            rtab[c, pl.ds(q * SUB, SUB), :] = sea_c / (1.0 + f2 * damp_c)
    wide = (SUB, LANES)
    sign = side.astype(F32)
    face_near = jnp.broadcast_to(-sign * (0.5 * (flows[0] + flows[1])), wide)
    face_far = jnp.broadcast_to(sign * (0.5 * (flows[1] + flows[2])), wide)
    flow_y = jnp.broadcast_to(flow_y, wide)
    face_n = 0.5 * (flow_y + pltpu.roll(flow_y, LANES - 1, 1))
    face_s = 0.5 * (flow_y + pltpu.roll(flow_y, 1, 1))
    sea_w = jnp.broadcast_to(sea, wide)
    lane = lax.broadcasted_iota(jnp.int32, wide, 1)
    has_n = lane < LANES - 1
    has_s = lane > 0
    away = [sign * cos[m] for m in range(quads)]
    gain = [[dtab[c, pl.ds(m * SUB, SUB), :] for m in range(quads)] for c in range(3)]

    def forced(energy, c, m, fg, rec):
        return energy * (jnp.maximum(gain[c][m] * fg + (1.0 - WIND_GAIN), 1.0) * rec)

    def drift_rows(acc):
        dx = acc[0] * cos[0]
        dy = acc[0] * sin[0]
        for m in range(1, quads):
            dx = dx + acc[m] * cos[m]
            dy = dy + acc[m] * sin[m]
        dx = jnp.sum(dx, axis=0, keepdims=True)
        dy = jnp.sum(dy, axis=0, keepdims=True)
        return jnp.where(which == 0, dx, jnp.where(which == 1, dy, 0.0))

    def own_level(l, acc):
        fg = tab_ref[pl.ds(FG + l, 1), :]
        gs = tab_ref[pl.ds(GS + l, 1), :]
        wt = tab_ref[pl.ds(WT + l, 1), :]
        rec = rtab[1, pl.ds(l, 1), :]
        rec_near = rtab[0, pl.ds(l, 1), :]
        out = []
        for m in range(quads):
            r = pl.ds(pl.multiple_of(l * NDIR + m * SUB, SUB), SUB)
            e = forced(ctr[r, :], 1, m, fg, rec)
            other = forced(near[r, :], 0, m, fg, rec_near)
            speed = gs * sin[m]
            a = jnp.where(has_n, speed + face_n, 0.0)
            b = jnp.where(has_s, speed + face_s, 0.0)
            c = face_near - gs * away[m]
            flux_n = a * jnp.where(a > 0.0, e, pltpu.roll(e, LANES - 1, 1))
            flux_s = b * jnp.where(b > 0.0, pltpu.roll(e, 1, 1), e)
            u = sea_w * (e - flux_n + flux_s - c * jnp.where(c > 0.0, e, other))
            base[0, r, :] = e
            base[1, r, :] = u
            out.append(acc[m] + wt * u)
        return tuple(out)

    near_copy.wait_recv()
    acc = lax.fori_loop(0, levels, own_level, (zero,) * quads, unroll=6)
    drift[3] = drift_rows(acc)
    partial_copy = pltpu.make_async_remote_copy(
        src_ref=drift.at[3],
        dst_ref=drift.at[2],
        send_sem=drift_send.at[1],
        recv_sem=drift_recv.at[1],
        device_id=at(side),
        device_id_type=MESH,
    )
    partial_copy.start()

    def far_level(l, acc):
        fg = tab_ref[pl.ds(FG + l, 1), :]
        gs = tab_ref[pl.ds(GS + l, 1), :]
        wt = tab_ref[pl.ds(WT + l, 1), :]
        rec = rtab[2, pl.ds(l, 1), :]
        out = []
        for m in range(quads):
            r = pl.ds(pl.multiple_of(l * NDIR + m * SUB, SUB), SUB)
            other = forced(far[r, :], 2, m, fg, rec)
            a = gs * away[m] + face_far
            flux = a * jnp.where(a > 0.0, base[0, r, :], other)
            upd_ref[r, :] = base[1, r, :] - sea_w * flux
            out.append(acc[m] + wt * flux)
        return tuple(out)

    acc = (zero,) * quads
    for k in range(chunks):
        far_copies[k].wait_recv()
        acc = lax.fori_loop(k * per, (k + 1) * per, far_level, acc, unroll=per)

    shared = drift_rows(acc)
    drift[1] = drift[3] - sea * shared
    full_copy = pltpu.make_async_remote_copy(
        src_ref=drift.at[1],
        dst_ref=drift.at[0],
        send_sem=drift_send.at[0],
        recv_sem=drift_recv.at[0],
        device_id=at(-side),
        device_id_type=MESH,
    )
    full_copy.start()
    partial_copy.wait_recv()
    last[...] = drift[2] + seas[2] * shared
    for copy in part_copies + info_copies + nbr_copies + far_copies + [near_copy, partial_copy]:
        copy.wait_send()
    full_copy.wait()
    drift_ref[0] = drift[0]
    drift_ref[1] = drift[1]
    drift_ref[2] = last[...]


def finish(upd_ref, drift, where_ref, upd_hbm, cell_hbm, cell_ref, sem):
    store = pltpu.make_async_copy(upd_ref, upd_hbm, sem.at[0])
    store.start()
    slot = where_ref[0:1, :]
    row = where_ref[1:2, :]
    cells = row.shape[1]
    one_hot = jnp.where(
        lax.broadcasted_iota(jnp.int32, (LANES, cells), 0) == row, 1.0, 0.0
    ).astype(BF16)
    band = jnp.zeros((2 * SUB, LANES), F32)
    place = lax.broadcasted_iota(jnp.int32, (2 * SUB, LANES), 0)
    for c in range(3):
        for v in range(2):
            band = jnp.where(place == 4 * c + v, drift[c, v : v + 1, :], band)
    picked = sum3(jnp.dot(split3(band), one_hot, preferred_element_type=F32))
    for v in range(2):
        out = jnp.where(slot == 2, picked[8 + v : 9 + v], 0.0)
        out = jnp.where(slot == 1, picked[4 + v : 5 + v], out)
        cell_ref[v : v + 1, :] = jnp.where(slot == 0, picked[v : v + 1], out)
    cell_store = pltpu.make_async_copy(cell_ref, cell_hbm, sem.at[1])
    cell_store.start()
    cell_store.wait()
    store.wait()


def body(n_grp, n_dev, spectrum, sea_mask, wind, currents, coupling):
    bins, _, width = spectrum.shape
    levels = bins // NDIR
    cells = currents.shape[2]
    table, padded = bin_tables(levels)
    chunks, head_chunks = 9, 5
    vmem = pl.BlockSpec(memory_space=pltpu.VMEM)
    hbm = pl.BlockSpec(memory_space=pltpu.HBM)
    dma = pltpu.SemaphoreType.DMA
    updated, drift, where = pl.pallas_call(
        functools.partial(kernel, n_grp, n_dev, levels, padded, chunks, head_chunks),
        out_shape=(
            jax.ShapeDtypeStruct((bins, width), F32),
            jax.ShapeDtypeStruct((3, SUB, width), F32),
            jax.ShapeDtypeStruct((2, cells), jnp.int32),
        ),
        in_specs=[hbm] * 6,
        out_specs=(vmem, vmem, vmem),
        scratch_shapes=[
            pltpu.VMEM((bins, width), F32),
            pltpu.VMEM((1, cells), jnp.int32),
            pltpu.VMEM((1, width), jnp.int32),
            pltpu.VMEM((2, width), F32),
            pltpu.VMEM((2, cells), F32),
            pltpu.VMEM(table.shape, F32),
            pltpu.VMEM((bins, width), F32),
            pltpu.VMEM((bins, width), F32),
            pltpu.VMEM((2, bins, width), F32),
            pltpu.VMEM((n_grp, 2 * SUB, width), F32),
            pltpu.VMEM((5, 2 * SUB, width), F32),
            pltpu.VMEM((3, SUB, width), F32),
            pltpu.VMEM((4, SUB, width), F32),
            pltpu.VMEM((SUB, width), F32),
            pltpu.VMEM((3, padded, width), F32),
            pltpu.VMEM((3, NDIR, width), F32),
            dma((6,)),
            dma((chunks + 1,)),
            dma((chunks + 1,)),
            dma((n_grp,)),
            dma((n_grp,)),
            dma((4,)),
            dma((4,)),
            dma((2,)),
            dma((2,)),
            dma((2,)),
            dma((2,)),
        ],
        compiler_params=pltpu.CompilerParams(
            collective_id=0, has_side_effects=True, vmem_limit_bytes=32 * 1024 * 1024
        ),
        name="wave_step",
    )(
        *[
            pltpu.with_memory_space_constraint(x, pltpu.HBM)
            for x in (
                spectrum.reshape(bins, width),
                sea_mask,
                wind.reshape(2, width),
                currents.reshape(2, cells),
                coupling,
                table,
            )
        ]
    )
    updated, cell_drift = pl.pallas_call(
        finish,
        out_shape=(
            jax.ShapeDtypeStruct((bins, width), F32),
            jax.ShapeDtypeStruct((2, cells), F32),
        ),
        in_specs=[vmem, vmem, vmem],
        out_specs=(hbm, hbm),
        scratch_shapes=[pltpu.VMEM((2, cells), F32), dma((2,))],
        compiler_params=pltpu.CompilerParams(vmem_limit_bytes=16 * 1024 * 1024),
        name="finish",
    )(updated, drift, where)
    return updated.reshape(bins, 1, width), cell_drift.reshape(1, 2, cells)


def solution(mesh):
    return jax.shard_map(
        functools.partial(body, mesh.shape["grp"], mesh.shape["dev"]),
        mesh=mesh,
        in_specs=(
            P(None, "dev", None),
            P("dev", None),
            P(None, "dev", None),
            P("grp", None, "dev"),
            P("grp", "dev"),
        ),
        out_specs=(P(None, "dev", None), P("grp", None, "dev")),
        check_vma=False,
    )
```

```python
import functools
import math

import jax
import jax.numpy as jnp
import numpy as np
from jax import lax
from jax.experimental import pallas as pl
from jax.experimental.pallas import tpu as pltpu
from jax.sharding import PartitionSpec as P

MESH = pl.DeviceIdType.MESH
F32 = jnp.float32
BF16 = jnp.bfloat16

NDIR = 32
FIRST_FREQ = 0.04
GROWTH = 1.1
SPEED_TOP = 0.45
CURRENT_TOP = 0.2
WIND_GAIN = 0.03
WHITECAP = 0.3
STEEP_SCALE = 0.4
STOKES_GAIN = 3.0
LANES = 128
SUB = 8
GROWTH_F = WIND_GAIN * 0.64


def bin_tables(levels):
    padded = -(-levels // SUB) * SUB
    heading = np.arange(NDIR) * (2.0 * math.pi / NDIR)
    freq = FIRST_FREQ * GROWTH ** np.arange(padded)
    rows = np.concatenate(
        [
            np.cos(heading),
            np.sin(heading),
            GROWTH_F * freq,
            freq**2,
            SPEED_TOP * FIRST_FREQ / freq,
            STOKES_GAIN * 0.1 * freq**4,
        ]
    )
    table = np.broadcast_to(rows[:, None], (rows.shape[0], LANES))
    return jnp.asarray(table.astype(np.float32)), padded


def split3(x):
    hi = x.astype(BF16)
    rest = x - hi.astype(F32)
    mid = rest.astype(BF16)
    low = (rest - mid.astype(F32)).astype(BF16)
    return jnp.concatenate([hi, mid, low], axis=0)


def sum3(x):
    n = x.shape[0] // 3
    return x[:n] + x[n : 2 * n] + x[2 * n :]


def kernel(
    n_grp,
    n_dev,
    levels,
    padded,
    chunks,
    spec_hbm,
    mask_hbm,
    wind_hbm,
    cur_hbm,
    coup_hbm,
    tab_hbm,
    upd_ref,
    drift_ref,
    where_ref,
    ctr,
    coup_ref,
    mask_ref,
    wind_ref,
    cur_ref,
    tab_ref,
    near,
    far,
    base,
    part,
    link,
    sums,
    drift,
    last,
    rtab,
    load_sem,
    halo_send,
    halo_recv,
    part_send,
    part_recv,
    link_send,
    link_recv,
    sums_send,
    sums_recv,
    drift_send,
    drift_recv,
):
    g = lax.axis_index("grp")
    d = lax.axis_index("dev")
    side = 2 * lax.rem(d, 2) - 1

    bins = levels * NDIR
    per = levels // chunks
    rows = per * NDIR
    quads = NDIR // SUB
    COS, SIN, FG = 0, NDIR, 2 * NDIR
    F2, GS, WT = FG + padded, FG + 2 * padded, FG + 3 * padded

    def at(step):
        return {"grp": g, "dev": lax.rem(d + step + n_dev, n_dev)}

    def group(step):
        return {"grp": lax.rem(g + step, n_grp), "dev": d}

    loads = [
        pltpu.make_async_copy(src, dst, load_sem.at[i])
        for i, (src, dst) in enumerate(
            (
                (coup_hbm, coup_ref),
                (cur_hbm, cur_ref),
                (spec_hbm, ctr),
                (tab_hbm, tab_ref),
                (mask_hbm, mask_ref),
                (wind_hbm, wind_ref),
            )
        )
    ]
    for load in loads:
        load.start()
    barrier = pltpu.get_barrier_semaphore()
    for k in range(1, n_grp):
        pl.semaphore_signal(barrier, inc=1, device_id=group(k), device_id_type=MESH)
    for step in (-side, side):
        pl.semaphore_signal(barrier, inc=1, device_id=at(step), device_id_type=MESH)

    loads[0].wait()
    loads[1].wait()
    coup = coup_ref[...]
    slot = ((coup >> 7) - d + n_dev + 1) & (n_dev - 1)
    row = coup & (LANES - 1)
    cells = coup.shape[1]
    one_hot = jnp.where(
        lax.broadcasted_iota(jnp.int32, (LANES, cells), 0) == row, 1.0, 0.0
    ).astype(BF16)
    kind = lax.broadcasted_iota(jnp.int32, (2 * SUB, cells), 0)
    comp = kind & 3
    value = jnp.where(
        comp == 0, cur_ref[0:1, :], jnp.where(comp == 1, cur_ref[1:2, :], jnp.where(comp == 2, 1.0, 0.0))
    )
    value = jnp.where(jnp.logical_and((kind >> 2) == slot, g > 0), value, 0.0)
    cell_sums = sum3(
        lax.dot_general(
            split3(value), one_hot, (((1,), (1,)), ((), ())), preferred_element_type=F32
        )
    )
    link[1, 0 : 2 * SUB, :] = cell_sums
    part[g] = jnp.zeros((SUB, LANES), F32)
    where_ref[0:1, :] = jnp.where(g > 0, 1 + (slot - 1) * side, 3)
    where_ref[1:2, :] = row

    for load in loads[2:]:
        load.wait()

    def add_level(l, acc):
        r = pl.multiple_of(l * NDIR, NDIR)
        e = ctr[pl.ds(r, SUB), :]
        for m in range(1, quads):
            e = e + ctr[pl.ds(r + m * SUB, SUB), :]
        return (
            acc[0] + e * tab_ref[pl.ds(FG + l, 1), :],
            acc[1] + e * tab_ref[pl.ds(F2 + l, 1), :],
        )

    zero = jnp.zeros((SUB, LANES), F32)
    total, moment = lax.fori_loop(0, levels, add_level, (zero, zero), unroll=4)
    sea = mask_ref[...].astype(F32)
    total = jnp.sum(total, axis=0, keepdims=True) * (0.1 / GROWTH_F) * sea
    moment = jnp.sum(moment, axis=0, keepdims=True) * 0.1 * sea
    is_sea = sea > 0.5
    mean_freq = jnp.where(is_sea, moment / jnp.where(is_sea, total, 1.0), 1.0)
    steepness = STEEP_SCALE * total * mean_freq**4
    damp = WHITECAP * (steepness / mean_freq) ** 2
    which = lax.broadcasted_iota(jnp.int32, (SUB, LANES), 0)
    link[1, 2 * SUB :, :] = jnp.where(
        which == 0,
        sea,
        jnp.where(
            which == 1,
            damp,
            jnp.where(which == 2, wind_ref[0:1, :], jnp.where(which == 3, wind_ref[1:2, :], 0.0)),
        ),
    )

    pl.semaphore_wait(barrier, n_grp - 1 + 2)

    def to_sides(buf, send_sem, recv_sem):
        copies = []
        for i, step in ((1, side), (0, -side)):
            copy = pltpu.make_async_remote_copy(
                src_ref=buf.at[1],
                dst_ref=buf.at[2 * i],
                send_sem=send_sem.at[i],
                recv_sem=recv_sem.at[i],
                device_id=at(step),
                device_id_type=MESH,
            )
            copy.start()
            copies.append(copy)
        return copies

    link_copies = to_sides(link, link_send, link_recv)

    far_copies = []

    def send_far(k):
        copy = pltpu.make_async_remote_copy(
            src_ref=ctr.at[pl.ds(k * rows, rows), :],
            dst_ref=far.at[pl.ds(k * rows, rows), :],
            send_sem=halo_send.at[k],
            recv_sem=halo_recv.at[k],
            device_id=at(side),
            device_id_type=MESH,
        )
        copy.start()
        far_copies.append(copy)

    send_far(0)
    near_copy = pltpu.make_async_remote_copy(
        src_ref=ctr,
        dst_ref=near,
        send_sem=halo_send.at[chunks],
        recv_sem=halo_recv.at[chunks],
        device_id=at(-side),
        device_id_type=MESH,
    )
    near_copy.start()
    for k in range(1, chunks):
        send_far(k)

    for copy in link_copies:
        copy.wait_recv()
    part[g, 0:4, :] = (
        cell_sums[4:8]
        + jnp.where(side > 0, link[0, 8:12, :], link[0, 0:4, :])
        + jnp.where(side > 0, link[2, 0:4, :], link[2, 8:12, :])
    )
    part_copies = []
    for k in range(1, n_grp):
        copy = pltpu.make_async_remote_copy(
            src_ref=part.at[g],
            dst_ref=part.at[g],
            send_sem=part_send.at[k],
            recv_sem=part_recv.at[g],
            device_id=group(k),
            device_id_type=MESH,
        )
        copy.start()
        part_copies.append(copy)
    for k in range(1, n_grp):
        src = lax.rem(g - k + n_grp, n_grp)
        pltpu.make_async_remote_copy(
            src_ref=part.at[src],
            dst_ref=part.at[src],
            send_sem=part_send.at[k],
            recv_sem=part_recv.at[src],
            device_id=group(k),
            device_id_type=MESH,
        ).wait_recv()
    both = part[1]
    for k in range(2, n_grp):
        both = both + part[k]
    sums[1] = both
    sums_copies = to_sides(sums, sums_send, sums_recv)

    cos = [tab_ref[pl.ds(COS + m * SUB, SUB), :] for m in range(quads)]
    sin = [tab_ref[pl.ds(SIN + m * SUB, SUB), :] for m in range(quads)]
    gain = {}

    def column(c, s4):
        count = jnp.maximum(s4[2:3], 1.0)
        mean_x = s4[0:1] / count
        mean_y = s4[1:2] / count
        row = 2 * SUB
        sea_c = link[c, row : row + 1, :]
        damp_c = link[c, row + 1 : row + 2, :]
        wx = link[c, row + 2 : row + 3, :] - mean_x
        wy = link[c, row + 3 : row + 4, :] - mean_y
        gain[c] = [cos[m] * wx + sin[m] * wy for m in range(quads)]
        for q in range(padded // SUB):
            f2 = tab_ref[pl.ds(F2 + q * SUB, SUB), :]
            rtab[c, pl.ds(q * SUB, SUB), :] = sea_c / (1.0 + f2 * damp_c)
        return CURRENT_TOP * jnp.tanh(mean_x), CURRENT_TOP * jnp.tanh(mean_y), sea_c

    flow_x, flow_y, _ = column(1, both)
    sums_copies[1].wait_recv()
    flow_near, _, _ = column(0, sums[0])
    wide = (SUB, LANES)
    sign = side.astype(F32)
    face_near = jnp.broadcast_to(-sign * (0.5 * (flow_near + flow_x)), wide)
    flow_y = jnp.broadcast_to(flow_y, wide)
    face_n = 0.5 * (flow_y + pltpu.roll(flow_y, LANES - 1, 1))
    face_s = 0.5 * (flow_y + pltpu.roll(flow_y, 1, 1))
    sea_w = jnp.broadcast_to(sea, wide)
    lane = lax.broadcasted_iota(jnp.int32, wide, 1)
    has_n = lane < LANES - 1
    has_s = lane > 0
    away = [sign * cos[m] for m in range(quads)]

    def forced(energy, c, m, fg, rec):
        return energy * (jnp.maximum(gain[c][m] * fg + (1.0 - WIND_GAIN), 1.0) * rec)

    def drift_rows(acc):
        dx = acc[0] * cos[0]
        dy = acc[0] * sin[0]
        for m in range(1, quads):
            dx = dx + acc[m] * cos[m]
            dy = dy + acc[m] * sin[m]
        dx = jnp.sum(dx, axis=0, keepdims=True)
        dy = jnp.sum(dy, axis=0, keepdims=True)
        return jnp.where(which == 0, dx, jnp.where(which == 1, dy, 0.0))

    def own_level(l, acc):
        fg = tab_ref[pl.ds(FG + l, 1), :]
        gs = tab_ref[pl.ds(GS + l, 1), :]
        wt = tab_ref[pl.ds(WT + l, 1), :]
        rec = rtab[1, pl.ds(l, 1), :]
        rec_near = rtab[0, pl.ds(l, 1), :]
        out = []
        for m in range(quads):
            r = pl.ds(pl.multiple_of(l * NDIR + m * SUB, SUB), SUB)
            e = forced(ctr[r, :], 1, m, fg, rec)
            other = forced(near[r, :], 0, m, fg, rec_near)
            speed = gs * sin[m]
            a = jnp.where(has_n, speed + face_n, 0.0)
            b = jnp.where(has_s, speed + face_s, 0.0)
            c = face_near - gs * away[m]
            flux_n = a * jnp.where(a > 0.0, e, pltpu.roll(e, LANES - 1, 1))
            flux_s = b * jnp.where(b > 0.0, pltpu.roll(e, 1, 1), e)
            u = sea_w * (e - flux_n + flux_s - c * jnp.where(c > 0.0, e, other))
            base[0, r, :] = e
            base[1, r, :] = u
            out.append(acc[m] + wt * u)
        return tuple(out)

    near_copy.wait_recv()
    acc = lax.fori_loop(0, levels, own_level, (zero,) * quads, unroll=6)
    drift[3] = drift_rows(acc)
    partial_copy = pltpu.make_async_remote_copy(
        src_ref=drift.at[3],
        dst_ref=drift.at[2],
        send_sem=drift_send.at[1],
        recv_sem=drift_recv.at[1],
        device_id=at(side),
        device_id_type=MESH,
    )
    partial_copy.start()

    sums_copies[0].wait_recv()
    flow_far, _, sea_far = column(2, sums[2])
    face_far = jnp.broadcast_to(sign * (0.5 * (flow_x + flow_far)), wide)

    def far_level(l, acc):
        fg = tab_ref[pl.ds(FG + l, 1), :]
        gs = tab_ref[pl.ds(GS + l, 1), :]
        wt = tab_ref[pl.ds(WT + l, 1), :]
        rec = rtab[2, pl.ds(l, 1), :]
        out = []
        for m in range(quads):
            r = pl.ds(pl.multiple_of(l * NDIR + m * SUB, SUB), SUB)
            other = forced(far[r, :], 2, m, fg, rec)
            a = gs * away[m] + face_far
            flux = a * jnp.where(a > 0.0, base[0, r, :], other)
            upd_ref[r, :] = base[1, r, :] - sea_w * flux
            out.append(acc[m] + wt * flux)
        return tuple(out)

    acc = (zero,) * quads
    for k in range(chunks):
        far_copies[k].wait_recv()
        acc = lax.fori_loop(k * per, (k + 1) * per, far_level, acc, unroll=per)

    shared = drift_rows(acc)
    drift[1] = drift[3] - sea * shared
    full_copy = pltpu.make_async_remote_copy(
        src_ref=drift.at[1],
        dst_ref=drift.at[0],
        send_sem=drift_send.at[0],
        recv_sem=drift_recv.at[0],
        device_id=at(-side),
        device_id_type=MESH,
    )
    full_copy.start()
    partial_copy.wait_recv()
    last[...] = drift[2] + sea_far * shared
    for copy in part_copies + link_copies + sums_copies + far_copies + [near_copy, partial_copy]:
        copy.wait_send()
    full_copy.wait()
    drift_ref[0] = drift[0]
    drift_ref[1] = drift[1]
    drift_ref[2] = last[...]


def finish(upd_ref, drift, where_ref, upd_hbm, cell_hbm, cell_ref, sem):
    store = pltpu.make_async_copy(upd_ref, upd_hbm, sem.at[0])
    store.start()
    slot = where_ref[0:1, :]
    row = where_ref[1:2, :]
    cells = row.shape[1]
    one_hot = jnp.where(
        lax.broadcasted_iota(jnp.int32, (LANES, cells), 0) == row, 1.0, 0.0
    ).astype(BF16)
    band = jnp.zeros((2 * SUB, LANES), F32)
    place = lax.broadcasted_iota(jnp.int32, (2 * SUB, LANES), 0)
    for c in range(3):
        for v in range(2):
            band = jnp.where(place == 4 * c + v, drift[c, v : v + 1, :], band)
    picked = sum3(jnp.dot(split3(band), one_hot, preferred_element_type=F32))
    for v in range(2):
        out = jnp.where(slot == 2, picked[8 + v : 9 + v], 0.0)
        out = jnp.where(slot == 1, picked[4 + v : 5 + v], out)
        cell_ref[v : v + 1, :] = jnp.where(slot == 0, picked[v : v + 1], out)
    cell_store = pltpu.make_async_copy(cell_ref, cell_hbm, sem.at[1])
    cell_store.start()
    cell_store.wait()
    store.wait()


def body(n_grp, n_dev, spectrum, sea_mask, wind, currents, coupling):
    bins, _, width = spectrum.shape
    levels = bins // NDIR
    cells = currents.shape[2]
    table, padded = bin_tables(levels)
    chunks = 6
    vmem = pl.BlockSpec(memory_space=pltpu.VMEM)
    hbm = pl.BlockSpec(memory_space=pltpu.HBM)
    dma = pltpu.SemaphoreType.DMA
    updated, drift, where = pl.pallas_call(
        functools.partial(kernel, n_grp, n_dev, levels, padded, chunks),
        out_shape=(
            jax.ShapeDtypeStruct((bins, width), F32),
            jax.ShapeDtypeStruct((3, SUB, width), F32),
            jax.ShapeDtypeStruct((2, cells), jnp.int32),
        ),
        in_specs=[hbm] * 6,
        out_specs=(vmem, vmem, vmem),
        scratch_shapes=[
            pltpu.VMEM((bins, width), F32),
            pltpu.VMEM((1, cells), jnp.int32),
            pltpu.VMEM((1, width), jnp.int32),
            pltpu.VMEM((2, width), F32),
            pltpu.VMEM((2, cells), F32),
            pltpu.VMEM(table.shape, F32),
            pltpu.VMEM((bins, width), F32),
            pltpu.VMEM((bins, width), F32),
            pltpu.VMEM((2, bins, width), F32),
            pltpu.VMEM((n_grp, SUB, width), F32),
            pltpu.VMEM((3, 3 * SUB, width), F32),
            pltpu.VMEM((3, SUB, width), F32),
            pltpu.VMEM((4, SUB, width), F32),
            pltpu.VMEM((SUB, width), F32),
            pltpu.VMEM((3, padded, width), F32),
            dma((6,)),
            dma((chunks + 1,)),
            dma((chunks + 1,)),
            dma((n_grp,)),
            dma((n_grp,)),
            dma((2,)),
            dma((2,)),
            dma((2,)),
            dma((2,)),
            dma((2,)),
            dma((2,)),
        ],
        compiler_params=pltpu.CompilerParams(
            collective_id=0, has_side_effects=True, vmem_limit_bytes=32 * 1024 * 1024
        ),
        name="wave_step",
    )(
        *[
            pltpu.with_memory_space_constraint(x, pltpu.HBM)
            for x in (
                spectrum.reshape(bins, width),
                sea_mask,
                wind.reshape(2, width),
                currents.reshape(2, cells),
                coupling,
                table,
            )
        ]
    )
    updated, cell_drift = pl.pallas_call(
        finish,
        out_shape=(
            jax.ShapeDtypeStruct((bins, width), F32),
            jax.ShapeDtypeStruct((2, cells), F32),
        ),
        in_specs=[vmem, vmem, vmem],
        out_specs=(hbm, hbm),
        scratch_shapes=[pltpu.VMEM((2, cells), F32), dma((2,))],
        compiler_params=pltpu.CompilerParams(vmem_limit_bytes=16 * 1024 * 1024),
        name="finish",
    )(updated, drift, where)
    return updated.reshape(bins, 1, width), cell_drift.reshape(1, 2, cells)


def solution(mesh):
    return jax.shard_map(
        functools.partial(body, mesh.shape["grp"], mesh.shape["dev"]),
        mesh=mesh,
        in_specs=(
            P(None, "dev", None),
            P("dev", None),
            P(None, "dev", None),
            P("grp", None, "dev"),
            P("grp", "dev"),
        ),
        out_specs=(P(None, "dev", None), P("grp", None, "dev")),
        check_vma=False,
    )
```

```python
import functools
import math

import jax
import jax.numpy as jnp
import numpy as np
from jax import lax
from jax.experimental import pallas as pl
from jax.experimental.pallas import tpu as pltpu
from jax.sharding import PartitionSpec as P

MESH = pl.DeviceIdType.MESH
F32 = jnp.float32
BF16 = jnp.bfloat16

NDIR = 32
FIRST_FREQ = 0.04
GROWTH = 1.1
SPEED_TOP = 0.45
CURRENT_TOP = 0.2
WIND_GAIN = 0.03
WHITECAP = 0.3
STEEP_SCALE = 0.4
STOKES_GAIN = 3.0
LANES = 128
SUB = 8
GROWTH_F = WIND_GAIN * 0.64


def bin_tables(levels):
    padded = -(-levels // SUB) * SUB
    heading = np.arange(NDIR) * (2.0 * math.pi / NDIR)
    freq = FIRST_FREQ * GROWTH ** np.arange(padded)
    rows = np.concatenate(
        [
            np.cos(heading),
            np.sin(heading),
            GROWTH_F * freq,
            freq**2,
            SPEED_TOP * FIRST_FREQ / freq,
            STOKES_GAIN * 0.1 * freq**4,
        ]
    )
    table = np.broadcast_to(rows[:, None], (rows.shape[0], LANES))
    return jnp.asarray(table.astype(np.float32)), padded


def split3(x):
    hi = x.astype(BF16)
    rest = x - hi.astype(F32)
    mid = rest.astype(BF16)
    low = (rest - mid.astype(F32)).astype(BF16)
    return jnp.concatenate([hi, mid, low], axis=0)


def sum3(x):
    n = x.shape[0] // 3
    return x[:n] + x[n : 2 * n] + x[2 * n :]


def kernel(
    n_grp,
    n_dev,
    levels,
    padded,
    chunks,
    head_chunks,
    spec_hbm,
    mask_hbm,
    wind_hbm,
    cur_hbm,
    coup_hbm,
    tab_hbm,
    upd_ref,
    drift_ref,
    where_ref,
    ctr,
    coup_ref,
    mask_ref,
    wind_ref,
    cur_ref,
    tab_ref,
    near,
    far,
    base,
    part,
    link,
    sums,
    drift,
    last,
    rtab,
    load_sem,
    halo_send,
    halo_recv,
    part_send,
    part_recv,
    link_send,
    link_recv,
    sums_send,
    sums_recv,
    drift_send,
    drift_recv,
):
    g = lax.axis_index("grp")
    d = lax.axis_index("dev")
    side = 2 * lax.rem(d, 2) - 1

    bins = levels * NDIR
    per = levels // chunks
    rows = per * NDIR
    quads = NDIR // SUB
    COS, SIN, FG = 0, NDIR, 2 * NDIR
    F2, GS, WT = FG + padded, FG + 2 * padded, FG + 3 * padded

    def at(step):
        return {"grp": g, "dev": lax.rem(d + step + n_dev, n_dev)}

    def group(step):
        return {"grp": lax.rem(g + step, n_grp), "dev": d}

    loads = [
        pltpu.make_async_copy(src, dst, load_sem.at[i])
        for i, (src, dst) in enumerate(
            (
                (coup_hbm, coup_ref),
                (cur_hbm, cur_ref),
                (spec_hbm, ctr),
                (tab_hbm, tab_ref),
                (mask_hbm, mask_ref),
                (wind_hbm, wind_ref),
            )
        )
    ]
    for load in loads:
        load.start()
    barrier = pltpu.get_barrier_semaphore()
    for k in range(1, n_grp):
        pl.semaphore_signal(barrier, inc=1, device_id=group(k), device_id_type=MESH)
    for step in (-side, side):
        pl.semaphore_signal(barrier, inc=1, device_id=at(step), device_id_type=MESH)

    loads[0].wait()
    loads[1].wait()
    coup = coup_ref[...]
    slot = ((coup >> 7) - d + n_dev + 1) & (n_dev - 1)
    row = coup & (LANES - 1)
    cells = coup.shape[1]
    one_hot = jnp.where(
        lax.broadcasted_iota(jnp.int32, (LANES, cells), 0) == row, 1.0, 0.0
    ).astype(BF16)
    kind = lax.broadcasted_iota(jnp.int32, (2 * SUB, cells), 0)
    comp = kind & 3
    value = jnp.where(
        comp == 0, cur_ref[0:1, :], jnp.where(comp == 1, cur_ref[1:2, :], jnp.where(comp == 2, 1.0, 0.0))
    )
    value = jnp.where(jnp.logical_and((kind >> 2) == slot, g > 0), value, 0.0)
    cell_sums = sum3(
        lax.dot_general(
            split3(value), one_hot, (((1,), (1,)), ((), ())), preferred_element_type=F32
        )
    )
    link[1, 0 : 2 * SUB, :] = cell_sums
    part[1, g] = jnp.zeros((SUB, LANES), F32)
    sums[1] = jnp.zeros((SUB, LANES), F32)
    where_ref[0:1, :] = jnp.where(g > 0, 1 + (slot - 1) * side, 3)
    where_ref[1:2, :] = row

    for load in loads[2:]:
        load.wait()

    def add_level(l, acc):
        r = pl.multiple_of(l * NDIR, NDIR)
        e = ctr[pl.ds(r, SUB), :]
        for m in range(1, quads):
            e = e + ctr[pl.ds(r + m * SUB, SUB), :]
        return (
            acc[0] + e * tab_ref[pl.ds(FG + l, 1), :],
            acc[1] + e * tab_ref[pl.ds(F2 + l, 1), :],
        )

    zero = jnp.zeros((SUB, LANES), F32)
    total, moment = lax.fori_loop(0, levels, add_level, (zero, zero), unroll=4)
    sea = mask_ref[...].astype(F32)
    total = jnp.sum(total, axis=0, keepdims=True) * (0.1 / GROWTH_F) * sea
    moment = jnp.sum(moment, axis=0, keepdims=True) * 0.1 * sea
    is_sea = sea > 0.5
    mean_freq = jnp.where(is_sea, moment / jnp.where(is_sea, total, 1.0), 1.0)
    steepness = STEEP_SCALE * total * mean_freq**4
    damp = WHITECAP * (steepness / mean_freq) ** 2
    which = lax.broadcasted_iota(jnp.int32, (SUB, LANES), 0)
    link[1, 2 * SUB :, :] = jnp.where(
        which == 0,
        sea,
        jnp.where(
            which == 1,
            damp,
            jnp.where(which == 2, wind_ref[0:1, :], jnp.where(which == 3, wind_ref[1:2, :], 0.0)),
        ),
    )

    pl.semaphore_wait(barrier, n_grp - 1 + 2)

    def to_sides(buf, send_sem, recv_sem):
        copies = []
        for i, step in ((1, side), (0, -side)):
            copy = pltpu.make_async_remote_copy(
                src_ref=buf.at[1],
                dst_ref=buf.at[2 * i],
                send_sem=send_sem.at[i],
                recv_sem=recv_sem.at[i],
                device_id=at(step),
                device_id_type=MESH,
            )
            copy.start()
            copies.append(copy)
        return copies

    link_copies = to_sides(link, link_send, link_recv)

    far_copies = []

    def send_far(k):
        copy = pltpu.make_async_remote_copy(
            src_ref=ctr.at[pl.ds(k * rows, rows), :],
            dst_ref=far.at[pl.ds(k * rows, rows), :],
            send_sem=halo_send.at[k],
            recv_sem=halo_recv.at[k],
            device_id=at(side),
            device_id_type=MESH,
        )
        copy.start()
        far_copies.append(copy)

    def pick(buf, east, west):
        return jnp.where(side > 0, buf[east : east + 4], buf[west : west + 4])

    def to_groups(n):
        copies = []
        for k in range(1, n_grp):
            copy = pltpu.make_async_remote_copy(
                src_ref=part.at[n, g],
                dst_ref=part.at[n, g],
                send_sem=part_send.at[n, k],
                recv_sem=part_recv.at[n, g],
                device_id=group(k),
                device_id_type=MESH,
            )
            copy.start()
            copies.append(copy)
        return copies

    def over_groups(n):
        for k in range(1, n_grp):
            src = lax.rem(g - k + n_grp, n_grp)
            pltpu.make_async_remote_copy(
                src_ref=part.at[n, src],
                dst_ref=part.at[n, src],
                send_sem=part_send.at[n, k],
                recv_sem=part_recv.at[n, src],
                device_id=group(k),
                device_id_type=MESH,
            ).wait_recv()
        both = part[n, 1]
        for k in range(2, n_grp):
            both = both + part[n, k]
        return both

    send_far(0)
    near_copy = pltpu.make_async_remote_copy(
        src_ref=ctr,
        dst_ref=near,
        send_sem=halo_send.at[chunks],
        recv_sem=halo_recv.at[chunks],
        device_id=at(-side),
        device_id_type=MESH,
    )
    near_copy.start()
    for k in range(1, head_chunks):
        send_far(k)

    link_copies[1].wait_recv()
    part[0, g, 0:4, :] = cell_sums[4:8] + pick(link[0], 8, 0)
    part[0, g, 4:8, :] = pick(cell_sums, 8, 0)
    part_copies = to_groups(0)
    link_copies[0].wait_recv()
    part[1, g, 0:4, :] = pick(link[2], 0, 8)
    part_copies += to_groups(1)
    chip = over_groups(0)
    sums[3] = chip
    chip_copy = pltpu.make_async_remote_copy(
        src_ref=sums.at[3],
        dst_ref=sums.at[2],
        send_sem=sums_send.at[1],
        recv_sem=sums_recv.at[1],
        device_id=at(side),
        device_id_type=MESH,
    )
    chip_copy.start()
    for k in range(head_chunks, chunks):
        send_far(k)
    own = chip[0:4] + over_groups(1)[0:4]
    sums[1, 0:4, :] = own
    own_copy = pltpu.make_async_remote_copy(
        src_ref=sums.at[1],
        dst_ref=sums.at[0],
        send_sem=sums_send.at[0],
        recv_sem=sums_recv.at[0],
        device_id=at(-side),
        device_id_type=MESH,
    )
    own_copy.start()

    cos = [tab_ref[pl.ds(COS + m * SUB, SUB), :] for m in range(quads)]
    sin = [tab_ref[pl.ds(SIN + m * SUB, SUB), :] for m in range(quads)]
    gain = {}

    def column(c, s4):
        count = jnp.maximum(s4[2:3], 1.0)
        mean_x = s4[0:1] / count
        mean_y = s4[1:2] / count
        row = 2 * SUB
        sea_c = link[c, row : row + 1, :]
        damp_c = link[c, row + 1 : row + 2, :]
        wx = link[c, row + 2 : row + 3, :] - mean_x
        wy = link[c, row + 3 : row + 4, :] - mean_y
        gain[c] = [cos[m] * wx + sin[m] * wy for m in range(quads)]
        for q in range(padded // SUB):
            f2 = tab_ref[pl.ds(F2 + q * SUB, SUB), :]
            rtab[c, pl.ds(q * SUB, SUB), :] = sea_c / (1.0 + f2 * damp_c)
        return CURRENT_TOP * jnp.tanh(mean_x), CURRENT_TOP * jnp.tanh(mean_y), sea_c

    flow_x, flow_y, _ = column(1, own)
    own_copy.wait_recv()
    flow_near, _, _ = column(0, sums[0])
    wide = (SUB, LANES)
    sign = side.astype(F32)
    face_near = jnp.broadcast_to(-sign * (0.5 * (flow_near + flow_x)), wide)
    flow_y = jnp.broadcast_to(flow_y, wide)
    face_n = 0.5 * (flow_y + pltpu.roll(flow_y, LANES - 1, 1))
    face_s = 0.5 * (flow_y + pltpu.roll(flow_y, 1, 1))
    sea_w = jnp.broadcast_to(sea, wide)
    lane = lax.broadcasted_iota(jnp.int32, wide, 1)
    has_n = lane < LANES - 1
    has_s = lane > 0
    away = [sign * cos[m] for m in range(quads)]

    def forced(energy, c, m, fg, rec):
        return energy * (jnp.maximum(gain[c][m] * fg + (1.0 - WIND_GAIN), 1.0) * rec)

    def drift_rows(acc):
        dx = acc[0] * cos[0]
        dy = acc[0] * sin[0]
        for m in range(1, quads):
            dx = dx + acc[m] * cos[m]
            dy = dy + acc[m] * sin[m]
        dx = jnp.sum(dx, axis=0, keepdims=True)
        dy = jnp.sum(dy, axis=0, keepdims=True)
        return jnp.where(which == 0, dx, jnp.where(which == 1, dy, 0.0))

    def own_level(l, acc):
        fg = tab_ref[pl.ds(FG + l, 1), :]
        gs = tab_ref[pl.ds(GS + l, 1), :]
        wt = tab_ref[pl.ds(WT + l, 1), :]
        rec = rtab[1, pl.ds(l, 1), :]
        rec_near = rtab[0, pl.ds(l, 1), :]
        out = []
        for m in range(quads):
            r = pl.ds(pl.multiple_of(l * NDIR + m * SUB, SUB), SUB)
            e = forced(ctr[r, :], 1, m, fg, rec)
            other = forced(near[r, :], 0, m, fg, rec_near)
            speed = gs * sin[m]
            a = jnp.where(has_n, speed + face_n, 0.0)
            b = jnp.where(has_s, speed + face_s, 0.0)
            c = face_near - gs * away[m]
            flux_n = a * jnp.where(a > 0.0, e, pltpu.roll(e, LANES - 1, 1))
            flux_s = b * jnp.where(b > 0.0, pltpu.roll(e, 1, 1), e)
            u = sea_w * (e - flux_n + flux_s - c * jnp.where(c > 0.0, e, other))
            base[0, r, :] = e
            base[1, r, :] = u
            out.append(acc[m] + wt * u)
        return tuple(out)

    near_copy.wait_recv()
    acc = lax.fori_loop(0, levels, own_level, (zero,) * quads, unroll=6)
    drift[3] = drift_rows(acc)
    partial_copy = pltpu.make_async_remote_copy(
        src_ref=drift.at[3],
        dst_ref=drift.at[2],
        send_sem=drift_send.at[1],
        recv_sem=drift_recv.at[1],
        device_id=at(side),
        device_id_type=MESH,
    )
    partial_copy.start()

    chip_copy.wait_recv()
    flow_far, _, sea_far = column(2, sums[2, 0:4, :] + chip[4:8])
    face_far = jnp.broadcast_to(sign * (0.5 * (flow_x + flow_far)), wide)

    def far_level(l, acc):
        fg = tab_ref[pl.ds(FG + l, 1), :]
        gs = tab_ref[pl.ds(GS + l, 1), :]
        wt = tab_ref[pl.ds(WT + l, 1), :]
        rec = rtab[2, pl.ds(l, 1), :]
        out = []
        for m in range(quads):
            r = pl.ds(pl.multiple_of(l * NDIR + m * SUB, SUB), SUB)
            other = forced(far[r, :], 2, m, fg, rec)
            a = gs * away[m] + face_far
            flux = a * jnp.where(a > 0.0, base[0, r, :], other)
            upd_ref[r, :] = base[1, r, :] - sea_w * flux
            out.append(acc[m] + wt * flux)
        return tuple(out)

    acc = (zero,) * quads
    for k in range(chunks):
        far_copies[k].wait_recv()
        acc = lax.fori_loop(k * per, (k + 1) * per, far_level, acc, unroll=per)

    shared = drift_rows(acc)
    drift[1] = drift[3] - sea * shared
    full_copy = pltpu.make_async_remote_copy(
        src_ref=drift.at[1],
        dst_ref=drift.at[0],
        send_sem=drift_send.at[0],
        recv_sem=drift_recv.at[0],
        device_id=at(-side),
        device_id_type=MESH,
    )
    full_copy.start()
    partial_copy.wait_recv()
    last[...] = drift[2] + sea_far * shared
    for copy in part_copies + link_copies + far_copies + [near_copy, chip_copy, own_copy, partial_copy]:
        copy.wait_send()
    full_copy.wait()
    drift_ref[0] = drift[0]
    drift_ref[1] = drift[1]
    drift_ref[2] = last[...]


def finish(upd_ref, drift, where_ref, upd_hbm, cell_hbm, cell_ref, sem):
    store = pltpu.make_async_copy(upd_ref, upd_hbm, sem.at[0])
    store.start()
    slot = where_ref[0:1, :]
    row = where_ref[1:2, :]
    cells = row.shape[1]
    one_hot = jnp.where(
        lax.broadcasted_iota(jnp.int32, (LANES, cells), 0) == row, 1.0, 0.0
    ).astype(BF16)
    band = jnp.zeros((2 * SUB, LANES), F32)
    place = lax.broadcasted_iota(jnp.int32, (2 * SUB, LANES), 0)
    for c in range(3):
        for v in range(2):
            band = jnp.where(place == 4 * c + v, drift[c, v : v + 1, :], band)
    picked = sum3(jnp.dot(split3(band), one_hot, preferred_element_type=F32))
    for v in range(2):
        out = jnp.where(slot == 2, picked[8 + v : 9 + v], 0.0)
        out = jnp.where(slot == 1, picked[4 + v : 5 + v], out)
        cell_ref[v : v + 1, :] = jnp.where(slot == 0, picked[v : v + 1], out)
    cell_store = pltpu.make_async_copy(cell_ref, cell_hbm, sem.at[1])
    cell_store.start()
    cell_store.wait()
    store.wait()


def body(n_grp, n_dev, spectrum, sea_mask, wind, currents, coupling):
    bins, _, width = spectrum.shape
    levels = bins // NDIR
    cells = currents.shape[2]
    table, padded = bin_tables(levels)
    chunks, head_chunks = 6, 4
    vmem = pl.BlockSpec(memory_space=pltpu.VMEM)
    hbm = pl.BlockSpec(memory_space=pltpu.HBM)
    dma = pltpu.SemaphoreType.DMA
    updated, drift, where = pl.pallas_call(
        functools.partial(kernel, n_grp, n_dev, levels, padded, chunks, head_chunks),
        out_shape=(
            jax.ShapeDtypeStruct((bins, width), F32),
            jax.ShapeDtypeStruct((3, SUB, width), F32),
            jax.ShapeDtypeStruct((2, cells), jnp.int32),
        ),
        in_specs=[hbm] * 6,
        out_specs=(vmem, vmem, vmem),
        scratch_shapes=[
            pltpu.VMEM((bins, width), F32),
            pltpu.VMEM((1, cells), jnp.int32),
            pltpu.VMEM((1, width), jnp.int32),
            pltpu.VMEM((2, width), F32),
            pltpu.VMEM((2, cells), F32),
            pltpu.VMEM(table.shape, F32),
            pltpu.VMEM((bins, width), F32),
            pltpu.VMEM((bins, width), F32),
            pltpu.VMEM((2, bins, width), F32),
            pltpu.VMEM((2, n_grp, SUB, width), F32),
            pltpu.VMEM((3, 3 * SUB, width), F32),
            pltpu.VMEM((4, SUB, width), F32),
            pltpu.VMEM((4, SUB, width), F32),
            pltpu.VMEM((SUB, width), F32),
            pltpu.VMEM((3, padded, width), F32),
            dma((6,)),
            dma((chunks + 1,)),
            dma((chunks + 1,)),
            dma((2, n_grp)),
            dma((2, n_grp)),
            dma((2,)),
            dma((2,)),
            dma((2,)),
            dma((2,)),
            dma((2,)),
            dma((2,)),
        ],
        compiler_params=pltpu.CompilerParams(
            collective_id=0, has_side_effects=True, vmem_limit_bytes=32 * 1024 * 1024
        ),
        name="wave_step",
    )(
        *[
            pltpu.with_memory_space_constraint(x, pltpu.HBM)
            for x in (
                spectrum.reshape(bins, width),
                sea_mask,
                wind.reshape(2, width),
                currents.reshape(2, cells),
                coupling,
                table,
            )
        ]
    )
    updated, cell_drift = pl.pallas_call(
        finish,
        out_shape=(
            jax.ShapeDtypeStruct((bins, width), F32),
            jax.ShapeDtypeStruct((2, cells), F32),
        ),
        in_specs=[vmem, vmem, vmem],
        out_specs=(hbm, hbm),
        scratch_shapes=[pltpu.VMEM((2, cells), F32), dma((2,))],
        compiler_params=pltpu.CompilerParams(vmem_limit_bytes=16 * 1024 * 1024),
        name="finish",
    )(updated, drift, where)
    return updated.reshape(bins, 1, width), cell_drift.reshape(1, 2, cells)


def solution(mesh):
    return jax.shard_map(
        functools.partial(body, mesh.shape["grp"], mesh.shape["dev"]),
        mesh=mesh,
        in_specs=(
            P(None, "dev", None),
            P("dev", None),
            P(None, "dev", None),
            P("grp", None, "dev"),
            P("grp", "dev"),
        ),
        out_specs=(P(None, "dev", None), P("grp", None, "dev")),
        check_vma=False,
    )
```

```python
import functools
import math

import jax
import jax.numpy as jnp
import numpy as np
from jax import lax
from jax.experimental import pallas as pl
from jax.experimental.pallas import tpu as pltpu
from jax.sharding import PartitionSpec as P

MESH = pl.DeviceIdType.MESH
F32 = jnp.float32
BF16 = jnp.bfloat16

NDIR = 32
FIRST_FREQ = 0.04
GROWTH = 1.1
SPEED_TOP = 0.45
CURRENT_TOP = 0.2
WIND_GAIN = 0.03
WHITECAP = 0.3
STEEP_SCALE = 0.4
STOKES_GAIN = 3.0
LANES = 128
SUB = 8
GROWTH_F = WIND_GAIN * 0.64


def bin_tables(levels):
    padded = -(-levels // SUB) * SUB
    heading = np.arange(NDIR) * (2.0 * math.pi / NDIR)
    freq = FIRST_FREQ * GROWTH ** np.arange(padded)
    rows = np.concatenate(
        [
            np.cos(heading),
            np.sin(heading),
            GROWTH_F * freq,
            freq**2,
            SPEED_TOP * FIRST_FREQ / freq,
            STOKES_GAIN * 0.1 * freq**4,
        ]
    )
    table = np.broadcast_to(rows[:, None], (rows.shape[0], LANES))
    return jnp.asarray(table.astype(np.float32)), padded


def split3(x):
    hi = x.astype(BF16)
    rest = x - hi.astype(F32)
    mid = rest.astype(BF16)
    low = (rest - mid.astype(F32)).astype(BF16)
    return jnp.concatenate([hi, mid, low], axis=0)


def sum3(x):
    n = x.shape[0] // 3
    return x[:n] + x[n : 2 * n] + x[2 * n :]


def kernel(
    n_grp,
    n_dev,
    levels,
    padded,
    shared_levels,
    spec_hbm,
    mask_hbm,
    wind_hbm,
    cur_hbm,
    coup_hbm,
    tab_hbm,
    upd_ref,
    drift_ref,
    where_ref,
    ctr,
    coup_ref,
    mask_ref,
    wind_ref,
    cur_ref,
    tab_ref,
    near,
    far,
    base,
    part,
    link,
    sums,
    drift,
    last,
    rtab,
    load_sem,
    halo_send,
    halo_recv,
    pass_send,
    pass_recv,
    part_send,
    part_recv,
    link_send,
    link_recv,
    sums_send,
    sums_recv,
    drift_send,
    drift_recv,
):
    g = lax.axis_index("grp")
    d = lax.axis_index("dev")
    side = 2 * lax.rem(d, 2) - 1

    bins = levels * NDIR
    quads = NDIR // SUB
    COS, SIN, FG = 0, NDIR, 2 * NDIR
    F2, GS, WT = FG + padded, FG + 2 * padded, FG + 3 * padded

    def at(step):
        return {"grp": g, "dev": lax.rem(d + step + n_dev, n_dev)}

    def group(step):
        return {"grp": lax.rem(g + step, n_grp), "dev": d}

    loads = [
        pltpu.make_async_copy(src, dst, load_sem.at[i])
        for i, (src, dst) in enumerate(
            (
                (coup_hbm, coup_ref),
                (cur_hbm, cur_ref),
                (spec_hbm, ctr),
                (tab_hbm, tab_ref),
                (mask_hbm, mask_ref),
                (wind_hbm, wind_ref),
            )
        )
    ]
    for load in loads:
        load.start()
    barrier = pltpu.get_barrier_semaphore()
    for k in range(1, n_grp):
        pl.semaphore_signal(barrier, inc=1, device_id=group(k), device_id_type=MESH)
    for step in (-side, side):
        pl.semaphore_signal(barrier, inc=1, device_id=at(step), device_id_type=MESH)

    loads[0].wait()
    loads[1].wait()
    coup = coup_ref[...]
    slot = ((coup >> 7) - d + n_dev + 1) & (n_dev - 1)
    row = coup & (LANES - 1)
    cells = coup.shape[1]
    one_hot = jnp.where(
        lax.broadcasted_iota(jnp.int32, (LANES, cells), 0) == row, 1.0, 0.0
    ).astype(BF16)
    kind = lax.broadcasted_iota(jnp.int32, (2 * SUB, cells), 0)
    comp = kind & 3
    value = jnp.where(
        comp == 0, cur_ref[0:1, :], jnp.where(comp == 1, cur_ref[1:2, :], jnp.where(comp == 2, 1.0, 0.0))
    )
    value = jnp.where(jnp.logical_and((kind >> 2) == slot, g > 0), value, 0.0)
    cell_sums = sum3(
        lax.dot_general(
            split3(value), one_hot, (((1,), (1,)), ((), ())), preferred_element_type=F32
        )
    )
    link[1, 0 : 2 * SUB, :] = cell_sums
    part[1, g] = jnp.zeros((SUB, LANES), F32)
    sums[1] = jnp.zeros((SUB, LANES), F32)
    where_ref[0:1, :] = jnp.where(g > 0, 1 + (slot - 1) * side, 3)
    where_ref[1:2, :] = row

    for load in loads[2:]:
        load.wait()

    def add_level(l, acc):
        r = pl.multiple_of(l * NDIR, NDIR)
        e = ctr[pl.ds(r, SUB), :]
        for m in range(1, quads):
            e = e + ctr[pl.ds(r + m * SUB, SUB), :]
        return (
            acc[0] + e * tab_ref[pl.ds(FG + l, 1), :],
            acc[1] + e * tab_ref[pl.ds(F2 + l, 1), :],
        )

    zero = jnp.zeros((SUB, LANES), F32)
    total, moment = lax.fori_loop(0, levels, add_level, (zero, zero), unroll=4)
    sea = mask_ref[...].astype(F32)
    total = jnp.sum(total, axis=0, keepdims=True) * (0.1 / GROWTH_F) * sea
    moment = jnp.sum(moment, axis=0, keepdims=True) * 0.1 * sea
    is_sea = sea > 0.5
    mean_freq = jnp.where(is_sea, moment / jnp.where(is_sea, total, 1.0), 1.0)
    steepness = STEEP_SCALE * total * mean_freq**4
    damp = WHITECAP * (steepness / mean_freq) ** 2
    which = lax.broadcasted_iota(jnp.int32, (SUB, LANES), 0)
    link[1, 2 * SUB :, :] = jnp.where(
        which == 0,
        sea,
        jnp.where(
            which == 1,
            damp,
            jnp.where(which == 2, wind_ref[0:1, :], jnp.where(which == 3, wind_ref[1:2, :], 0.0)),
        ),
    )

    pl.semaphore_wait(barrier, n_grp - 1 + 2)

    def to_sides(buf, send_sem, recv_sem):
        copies = []
        for i, step in ((1, side), (0, -side)):
            copy = pltpu.make_async_remote_copy(
                src_ref=buf.at[1],
                dst_ref=buf.at[2 * i],
                send_sem=send_sem.at[i],
                recv_sem=recv_sem.at[i],
                device_id=at(step),
                device_id_type=MESH,
            )
            copy.start()
            copies.append(copy)
        return copies

    link_copies = to_sides(link, link_send, link_recv)

    half = shared_levels // 2
    parity = lax.rem(g, 2)
    mine, theirs = parity * shared_levels, (1 - parity) * shared_levels
    first, middle = 2 * shared_levels, 28
    spans = ((mine, half), (mine + half, half), (first, middle - first), (middle, levels - middle))

    def span(start, count):
        return pl.ds(pl.multiple_of(start * NDIR, NDIR), count * NDIR)

    far_copies = []

    def send_far(k):
        there = span(*spans[k])
        copy = pltpu.make_async_remote_copy(
            src_ref=ctr.at[there, :],
            dst_ref=far.at[there, :],
            send_sem=halo_send.at[k],
            recv_sem=halo_recv.at[k],
            device_id=at(side),
            device_id_type=MESH,
        )
        copy.start()
        far_copies.append(copy)

    def pick(buf, east, west):
        return jnp.where(side > 0, buf[east : east + 4], buf[west : west + 4])

    def to_groups(n):
        copies = []
        for k in range(1, n_grp):
            copy = pltpu.make_async_remote_copy(
                src_ref=part.at[n, g],
                dst_ref=part.at[n, g],
                send_sem=part_send.at[n, k],
                recv_sem=part_recv.at[n, g],
                device_id=group(k),
                device_id_type=MESH,
            )
            copy.start()
            copies.append(copy)
        return copies

    def over_groups(n):
        for k in range(1, n_grp):
            src = lax.rem(g - k + n_grp, n_grp)
            pltpu.make_async_remote_copy(
                src_ref=part.at[n, src],
                dst_ref=part.at[n, src],
                send_sem=part_send.at[n, k],
                recv_sem=part_recv.at[n, src],
                device_id=group(k),
                device_id_type=MESH,
            ).wait_recv()
        both = part[n, 1]
        for k in range(2, n_grp):
            both = both + part[n, k]
        return both

    send_far(0)
    near_copy = pltpu.make_async_remote_copy(
        src_ref=ctr,
        dst_ref=near,
        send_sem=halo_send.at[4],
        recv_sem=halo_recv.at[4],
        device_id=at(-side),
        device_id_type=MESH,
    )
    near_copy.start()
    send_far(1)
    send_far(2)

    def damping(c, sea_c, damp_c):
        for q in range(padded // SUB):
            f2 = tab_ref[pl.ds(F2 + q * SUB, SUB), :]
            rtab[c, pl.ds(q * SUB, SUB), :] = sea_c / (1.0 + f2 * damp_c)

    link_copies[1].wait_recv()
    part[0, g, 0:4, :] = cell_sums[4:8] + pick(link[0], 8, 0)
    part[0, g, 4:8, :] = pick(cell_sums, 8, 0)
    part_copies = to_groups(0)
    link_copies[0].wait_recv()
    part[1, g, 0:4, :] = pick(link[2], 0, 8)
    part_copies += to_groups(1)
    damping(1, sea, damp)
    for c in (0, 2):
        damping(c, link[c, 2 * SUB : 2 * SUB + 1, :], link[c, 2 * SUB + 1 : 2 * SUB + 2, :])
    chip = over_groups(0)
    sums[3] = chip
    chip_copy = pltpu.make_async_remote_copy(
        src_ref=sums.at[3],
        dst_ref=sums.at[2],
        send_sem=sums_send.at[1],
        recv_sem=sums_recv.at[1],
        device_id=at(side),
        device_id_type=MESH,
    )
    chip_copy.start()
    send_far(3)
    pass_copies = []
    for i, step in ((0, 1), (1, n_grp - 1)):
        far_copies[i].wait_recv()
        there = span(*spans[i])
        copy = pltpu.make_async_remote_copy(
            src_ref=far.at[there, :],
            dst_ref=far.at[there, :],
            send_sem=pass_send.at[i],
            recv_sem=pass_recv.at[i],
            device_id=group(step),
            device_id_type=MESH,
        )
        copy.start()
        pass_copies.append(copy)
    own = chip[0:4] + over_groups(1)[0:4]
    sums[1, 0:4, :] = own
    own_copy = pltpu.make_async_remote_copy(
        src_ref=sums.at[1],
        dst_ref=sums.at[0],
        send_sem=sums_send.at[0],
        recv_sem=sums_recv.at[0],
        device_id=at(-side),
        device_id_type=MESH,
    )
    own_copy.start()

    cos = [tab_ref[pl.ds(COS + m * SUB, SUB), :] for m in range(quads)]
    sin = [tab_ref[pl.ds(SIN + m * SUB, SUB), :] for m in range(quads)]
    gain = {}

    def column(c, s4):
        count = jnp.maximum(s4[2:3], 1.0)
        mean_x = s4[0:1] / count
        mean_y = s4[1:2] / count
        row = 2 * SUB
        sea_c = link[c, row : row + 1, :]
        wx = link[c, row + 2 : row + 3, :] - mean_x
        wy = link[c, row + 3 : row + 4, :] - mean_y
        gain[c] = [cos[m] * wx + sin[m] * wy for m in range(quads)]
        return CURRENT_TOP * jnp.tanh(mean_x), CURRENT_TOP * jnp.tanh(mean_y), sea_c

    flow_x, flow_y, _ = column(1, own)
    own_copy.wait_recv()
    flow_near, _, _ = column(0, sums[0])
    wide = (SUB, LANES)
    sign = side.astype(F32)
    face_near = jnp.broadcast_to(-sign * (0.5 * (flow_near + flow_x)), wide)
    flow_y = jnp.broadcast_to(flow_y, wide)
    face_n = 0.5 * (flow_y + pltpu.roll(flow_y, LANES - 1, 1))
    face_s = 0.5 * (flow_y + pltpu.roll(flow_y, 1, 1))
    sea_w = jnp.broadcast_to(sea, wide)
    lane = lax.broadcasted_iota(jnp.int32, wide, 1)
    has_n = lane < LANES - 1
    has_s = lane > 0
    away = [sign * cos[m] for m in range(quads)]

    def forced(energy, c, m, fg, rec):
        return energy * (jnp.maximum(gain[c][m] * fg + (1.0 - WIND_GAIN), 1.0) * rec)

    def drift_rows(acc):
        dx = acc[0] * cos[0]
        dy = acc[0] * sin[0]
        for m in range(1, quads):
            dx = dx + acc[m] * cos[m]
            dy = dy + acc[m] * sin[m]
        dx = jnp.sum(dx, axis=0, keepdims=True)
        dy = jnp.sum(dy, axis=0, keepdims=True)
        return jnp.where(which == 0, dx, jnp.where(which == 1, dy, 0.0))

    def own_level(l, acc):
        fg = tab_ref[pl.ds(FG + l, 1), :]
        gs = tab_ref[pl.ds(GS + l, 1), :]
        wt = tab_ref[pl.ds(WT + l, 1), :]
        rec = rtab[1, pl.ds(l, 1), :]
        rec_near = rtab[0, pl.ds(l, 1), :]
        out = []
        for m in range(quads):
            r = pl.ds(pl.multiple_of(l * NDIR + m * SUB, SUB), SUB)
            e = forced(ctr[r, :], 1, m, fg, rec)
            other = forced(near[r, :], 0, m, fg, rec_near)
            speed = gs * sin[m]
            a = jnp.where(has_n, speed + face_n, 0.0)
            b = jnp.where(has_s, speed + face_s, 0.0)
            c = face_near - gs * away[m]
            flux_n = a * jnp.where(a > 0.0, e, pltpu.roll(e, LANES - 1, 1))
            flux_s = b * jnp.where(b > 0.0, pltpu.roll(e, 1, 1), e)
            u = sea_w * (e - flux_n + flux_s - c * jnp.where(c > 0.0, e, other))
            base[0, r, :] = e
            base[1, r, :] = u
            out.append(acc[m] + wt * u)
        return tuple(out)

    near_copy.wait_recv()
    acc = lax.fori_loop(0, levels, own_level, (zero,) * quads, unroll=6)
    drift[3] = drift_rows(acc)
    partial_copy = pltpu.make_async_remote_copy(
        src_ref=drift.at[3],
        dst_ref=drift.at[2],
        send_sem=drift_send.at[1],
        recv_sem=drift_recv.at[1],
        device_id=at(side),
        device_id_type=MESH,
    )
    partial_copy.start()

    chip_copy.wait_recv()
    flow_far, _, sea_far = column(2, sums[2, 0:4, :] + chip[4:8])
    face_far = jnp.broadcast_to(sign * (0.5 * (flow_x + flow_far)), wide)

    def far_level(l, acc):
        fg = tab_ref[pl.ds(FG + l, 1), :]
        gs = tab_ref[pl.ds(GS + l, 1), :]
        wt = tab_ref[pl.ds(WT + l, 1), :]
        rec = rtab[2, pl.ds(l, 1), :]
        out = []
        for m in range(quads):
            r = pl.ds(pl.multiple_of(l * NDIR + m * SUB, SUB), SUB)
            other = forced(far[r, :], 2, m, fg, rec)
            a = gs * away[m] + face_far
            flux = a * jnp.where(a > 0.0, base[0, r, :], other)
            upd_ref[r, :] = base[1, r, :] - sea_w * flux
            out.append(acc[m] + wt * flux)
        return tuple(out)

    acc = (zero,) * quads

    def far_levels(start, count, acc):
        return lax.fori_loop(0, count, lambda i, acc: far_level(start + i, acc), acc, unroll=4)

    acc = far_levels(mine, shared_levels, acc)
    for k in (2, 3):
        far_copies[k].wait_recv()
        acc = far_levels(*spans[k], acc)
    for i in range(2):
        here = span(theirs + i * half, half)
        pltpu.make_async_remote_copy(
            src_ref=far.at[here, :],
            dst_ref=far.at[here, :],
            send_sem=pass_send.at[i],
            recv_sem=pass_recv.at[i],
            device_id=group(1 + i * (n_grp - 2)),
            device_id_type=MESH,
        ).wait_recv()
    acc = far_levels(theirs, shared_levels, acc)

    shared = drift_rows(acc)
    drift[1] = drift[3] - sea * shared
    full_copy = pltpu.make_async_remote_copy(
        src_ref=drift.at[1],
        dst_ref=drift.at[0],
        send_sem=drift_send.at[0],
        recv_sem=drift_recv.at[0],
        device_id=at(-side),
        device_id_type=MESH,
    )
    full_copy.start()
    partial_copy.wait_recv()
    last[...] = drift[2] + sea_far * shared
    for copy in part_copies + link_copies + far_copies + pass_copies + [near_copy, chip_copy, own_copy, partial_copy]:
        copy.wait_send()
    full_copy.wait()
    drift_ref[0] = drift[0]
    drift_ref[1] = drift[1]
    drift_ref[2] = last[...]


def finish(upd_ref, drift, where_ref, upd_hbm, cell_hbm, cell_ref, sem):
    store = pltpu.make_async_copy(upd_ref, upd_hbm, sem.at[0])
    store.start()
    slot = where_ref[0:1, :]
    row = where_ref[1:2, :]
    cells = row.shape[1]
    one_hot = jnp.where(
        lax.broadcasted_iota(jnp.int32, (LANES, cells), 0) == row, 1.0, 0.0
    ).astype(BF16)
    band = jnp.zeros((2 * SUB, LANES), F32)
    place = lax.broadcasted_iota(jnp.int32, (2 * SUB, LANES), 0)
    for c in range(3):
        for v in range(2):
            band = jnp.where(place == 4 * c + v, drift[c, v : v + 1, :], band)
    picked = sum3(jnp.dot(split3(band), one_hot, preferred_element_type=F32))
    for v in range(2):
        out = jnp.where(slot == 2, picked[8 + v : 9 + v], 0.0)
        out = jnp.where(slot == 1, picked[4 + v : 5 + v], out)
        cell_ref[v : v + 1, :] = jnp.where(slot == 0, picked[v : v + 1], out)
    cell_store = pltpu.make_async_copy(cell_ref, cell_hbm, sem.at[1])
    cell_store.start()
    cell_store.wait()
    store.wait()


def body(n_grp, n_dev, spectrum, sea_mask, wind, currents, coupling):
    bins, _, width = spectrum.shape
    levels = bins // NDIR
    cells = currents.shape[2]
    table, padded = bin_tables(levels)
    shared_levels = 8
    vmem = pl.BlockSpec(memory_space=pltpu.VMEM)
    hbm = pl.BlockSpec(memory_space=pltpu.HBM)
    dma = pltpu.SemaphoreType.DMA
    updated, drift, where = pl.pallas_call(
        functools.partial(kernel, n_grp, n_dev, levels, padded, shared_levels),
        out_shape=(
            jax.ShapeDtypeStruct((bins, width), F32),
            jax.ShapeDtypeStruct((3, SUB, width), F32),
            jax.ShapeDtypeStruct((2, cells), jnp.int32),
        ),
        in_specs=[hbm] * 6,
        out_specs=(vmem, vmem, vmem),
        scratch_shapes=[
            pltpu.VMEM((bins, width), F32),
            pltpu.VMEM((1, cells), jnp.int32),
            pltpu.VMEM((1, width), jnp.int32),
            pltpu.VMEM((2, width), F32),
            pltpu.VMEM((2, cells), F32),
            pltpu.VMEM(table.shape, F32),
            pltpu.VMEM((bins, width), F32),
            pltpu.VMEM((bins, width), F32),
            pltpu.VMEM((2, bins, width), F32),
            pltpu.VMEM((2, n_grp, SUB, width), F32),
            pltpu.VMEM((3, 3 * SUB, width), F32),
            pltpu.VMEM((4, SUB, width), F32),
            pltpu.VMEM((4, SUB, width), F32),
            pltpu.VMEM((SUB, width), F32),
            pltpu.VMEM((3, padded, width), F32),
            dma((6,)),
            dma((5,)),
            dma((5,)),
            dma((2,)),
            dma((2,)),
            dma((2, n_grp)),
            dma((2, n_grp)),
            dma((2,)),
            dma((2,)),
            dma((2,)),
            dma((2,)),
            dma((2,)),
            dma((2,)),
        ],
        compiler_params=pltpu.CompilerParams(
            collective_id=0, has_side_effects=True, vmem_limit_bytes=32 * 1024 * 1024
        ),
        name="wave_step",
    )(
        *[
            pltpu.with_memory_space_constraint(x, pltpu.HBM)
            for x in (
                spectrum.reshape(bins, width),
                sea_mask,
                wind.reshape(2, width),
                currents.reshape(2, cells),
                coupling,
                table,
            )
        ]
    )
    updated, cell_drift = pl.pallas_call(
        finish,
        out_shape=(
            jax.ShapeDtypeStruct((bins, width), F32),
            jax.ShapeDtypeStruct((2, cells), F32),
        ),
        in_specs=[vmem, vmem, vmem],
        out_specs=(hbm, hbm),
        scratch_shapes=[pltpu.VMEM((2, cells), F32), dma((2,))],
        compiler_params=pltpu.CompilerParams(vmem_limit_bytes=16 * 1024 * 1024),
        name="finish",
    )(updated, drift, where)
    return updated.reshape(bins, 1, width), cell_drift.reshape(1, 2, cells)


def solution(mesh):
    return jax.shard_map(
        functools.partial(body, mesh.shape["grp"], mesh.shape["dev"]),
        mesh=mesh,
        in_specs=(
            P(None, "dev", None),
            P("dev", None),
            P(None, "dev", None),
            P("grp", None, "dev"),
            P("grp", "dev"),
        ),
        out_specs=(P(None, "dev", None), P("grp", None, "dev")),
        check_vma=False,
    )
```

```python
import functools
import math

import jax
import jax.numpy as jnp
import numpy as np
from jax import lax
from jax.experimental import pallas as pl
from jax.experimental.pallas import tpu as pltpu
from jax.sharding import PartitionSpec as P

MESH = pl.DeviceIdType.MESH
F32 = jnp.float32
BF16 = jnp.bfloat16

NDIR = 32
FIRST_FREQ = 0.04
GROWTH = 1.1
SPEED_TOP = 0.45
CURRENT_TOP = 0.2
WIND_GAIN = 0.03
WHITECAP = 0.3
STEEP_SCALE = 0.4
STOKES_GAIN = 3.0
LANES = 128
SUB = 8
GROWTH_F = WIND_GAIN * 0.64


def bin_tables(levels):
    padded = -(-levels // SUB) * SUB
    heading = np.arange(NDIR) * (2.0 * math.pi / NDIR)
    freq = FIRST_FREQ * GROWTH ** np.arange(padded)
    rows = np.concatenate(
        [
            np.cos(heading),
            np.sin(heading),
            GROWTH_F * freq,
            freq**2,
            SPEED_TOP * FIRST_FREQ / freq,
            STOKES_GAIN * 0.1 * freq**4,
        ]
    )
    table = np.broadcast_to(rows[:, None], (rows.shape[0], LANES))
    return jnp.asarray(table.astype(np.float32)), padded


def split3(x):
    hi = x.astype(BF16)
    rest = x - hi.astype(F32)
    mid = rest.astype(BF16)
    low = (rest - mid.astype(F32)).astype(BF16)
    return jnp.concatenate([hi, mid, low], axis=0)


def sum3(x):
    n = x.shape[0] // 3
    return x[:n] + x[n : 2 * n] + x[2 * n :]


def kernel(
    n_grp,
    n_dev,
    levels,
    padded,
    shared_levels,
    spec_hbm,
    mask_hbm,
    wind_hbm,
    cur_hbm,
    coup_hbm,
    tab_hbm,
    upd_ref,
    drift_ref,
    where_ref,
    ctr,
    coup_ref,
    mask_ref,
    wind_ref,
    cur_ref,
    tab_ref,
    near,
    far,
    base,
    speed,
    part,
    link,
    sums,
    drift,
    last,
    rtab,
    load_sem,
    halo_send,
    halo_recv,
    pass_send,
    pass_recv,
    part_send,
    part_recv,
    share_send,
    link_send,
    link_recv,
    sums_send,
    sums_recv,
    drift_send,
    drift_recv,
):
    g = lax.axis_index("grp")
    d = lax.axis_index("dev")
    side = 2 * lax.rem(d, 2) - 1

    bins = levels * NDIR
    quads = NDIR // SUB
    COS, SIN, FG = 0, NDIR, 2 * NDIR
    F2, GS, WT = FG + padded, FG + 2 * padded, FG + 3 * padded

    def at(step):
        return {"grp": g, "dev": lax.rem(d + step + n_dev, n_dev)}

    def group(step):
        return {"grp": lax.rem(g + step, n_grp), "dev": d}

    loads = [
        pltpu.make_async_copy(src, dst, load_sem.at[i])
        for i, (src, dst) in enumerate(
            (
                (coup_hbm, coup_ref),
                (cur_hbm, cur_ref),
                (spec_hbm, ctr),
                (tab_hbm, tab_ref),
                (mask_hbm, mask_ref),
                (wind_hbm, wind_ref),
            )
        )
    ]
    for load in loads:
        load.start()
    barrier = pltpu.get_barrier_semaphore()
    for peer in [at(side), at(-side)] + [group(k) for k in range(1, n_grp)]:
        pl.semaphore_signal(barrier, inc=1, device_id=peer, device_id_type=MESH)

    def across(step):
        return {"grp": lax.rem(g + step, n_grp), "dev": lax.rem(d + side + n_dev, n_dev)}

    @pl.when(side < 0)
    def _():
        for k in range(1, n_grp):
            pl.semaphore_signal(barrier, inc=1, device_id=across(k), device_id_type=MESH)

    loads[0].wait()
    loads[1].wait()
    coup = coup_ref[...]
    slot = ((coup >> 7) - d + n_dev + 1) & (n_dev - 1)
    row = coup & (LANES - 1)
    cells = coup.shape[1]
    one_hot = jnp.where(
        lax.broadcasted_iota(jnp.int32, (LANES, cells), 0) == row, 1.0, 0.0
    ).astype(BF16)
    kind = lax.broadcasted_iota(jnp.int32, (2 * SUB, cells), 0)
    comp = kind & 3
    value = jnp.where(
        comp == 0, cur_ref[0:1, :], jnp.where(comp == 1, cur_ref[1:2, :], jnp.where(comp == 2, 1.0, 0.0))
    )
    value = jnp.where(jnp.logical_and((kind >> 2) == slot, g > 0), value, 0.0)
    cell_sums = sum3(
        lax.dot_general(
            split3(value), one_hot, (((1,), (1,)), ((), ())), preferred_element_type=F32
        )
    )
    link[1, 0:4, :] = jnp.where(side > 0, cell_sums[8:12], cell_sums[0:4])
    link[3, 0:4, :] = jnp.where(side > 0, cell_sums[0:4], cell_sums[8:12])
    part[1, g] = jnp.zeros((SUB, LANES), F32)
    sums[1] = jnp.zeros((SUB, LANES), F32)
    where_ref[0:1, :] = jnp.where(g > 0, 1 + (slot - 1) * side, 3)
    where_ref[1:2, :] = row

    for load in loads[2:]:
        load.wait()

    def add_level(l, acc):
        r = pl.multiple_of(l * NDIR, NDIR)
        e = ctr[pl.ds(r, SUB), :]
        for m in range(1, quads):
            e = e + ctr[pl.ds(r + m * SUB, SUB), :]
        return (
            acc[0] + e * tab_ref[pl.ds(FG + l, 1), :],
            acc[1] + e * tab_ref[pl.ds(F2 + l, 1), :],
        )

    zero = jnp.zeros((SUB, LANES), F32)
    total, moment = lax.fori_loop(0, levels, add_level, (zero, zero), unroll=4)
    sea = mask_ref[...].astype(F32)
    total = jnp.sum(total, axis=0, keepdims=True) * (0.1 / GROWTH_F) * sea
    moment = jnp.sum(moment, axis=0, keepdims=True) * 0.1 * sea
    is_sea = sea > 0.5
    mean_freq = jnp.where(is_sea, moment / jnp.where(is_sea, total, 1.0), 1.0)
    steepness = STEEP_SCALE * total * mean_freq**4
    damp = WHITECAP * (steepness / mean_freq) ** 2
    which = lax.broadcasted_iota(jnp.int32, (SUB, LANES), 0)
    for i in (1, 3):
        for n, term in enumerate((sea, damp, wind_ref[0:1, :], wind_ref[1:2, :])):
            link[i, 4 + n : 5 + n, :] = term

    def damping(c, sea_c, damp_c):
        for q in range(padded // SUB):
            f2 = tab_ref[pl.ds(F2 + q * SUB, SUB), :]
            rtab[c, pl.ds(q * SUB, SUB), :] = sea_c / (1.0 + f2 * damp_c)

    damping(1, sea, damp)
    wide = (SUB, LANES)
    sign = side.astype(F32)
    cos = [tab_ref[pl.ds(COS + m * SUB, SUB), :] for m in range(quads)]
    sin = [tab_ref[pl.ds(SIN + m * SUB, SUB), :] for m in range(quads)]
    lane = lax.broadcasted_iota(jnp.int32, wide, 1)
    has_n = lane < LANES - 1
    has_s = lane > 0
    away = [sign * cos[m] for m in range(quads)]

    def speed_level(l, carry):
        gs = tab_ref[pl.ds(GS + l, 1), :]
        rec = rtab[1, pl.ds(l, 1), :]
        for m in range(quads):
            r = pl.ds(pl.multiple_of(l * NDIR + m * SUB, SUB), SUB)
            y = gs * sin[m]
            speed[0, r, :] = jnp.where(has_n, y, 0.0)
            speed[1, r, :] = jnp.where(has_s, y, 0.0)
            speed[2, r, :] = gs * away[m]
            base[0, r, :] = ctr[r, :] * rec
        return carry

    lax.fori_loop(0, levels, speed_level, 0, unroll=4)

    pl.semaphore_wait(barrier, n_grp + 1 + jnp.where(side > 0, n_grp - 1, 0))

    link_copies = []
    for i, step in ((1, side), (0, -side)):
        copy = pltpu.make_async_remote_copy(
            src_ref=link.at[3 - 2 * i],
            dst_ref=link.at[2 * i],
            send_sem=link_send.at[i],
            recv_sem=link_recv.at[i],
            device_id=at(step),
            device_id_type=MESH,
        )
        copy.start()
        link_copies.append(copy)

    def share_copy(k):
        return pltpu.make_async_remote_copy(
            src_ref=link.at[1],
            dst_ref=part.at[1, g],
            send_sem=share_send.at[k],
            recv_sem=part_recv.at[1, g],
            device_id=across(k),
            device_id_type=MESH,
        )

    @pl.when(side > 0)
    def _():
        for k in range(1, n_grp):
            share_copy(k).start()


    half = shared_levels // 2
    parity = lax.rem(g, 2)
    mine, theirs = parity * shared_levels, (1 - parity) * shared_levels
    first, middle = 2 * shared_levels, 32
    spans = ((mine, half), (mine + half, half), (first, middle - first), (middle, levels - middle))

    def span(start, count):
        return pl.ds(pl.multiple_of(start * NDIR, NDIR), count * NDIR)

    far_copies = []

    def send_far(k):
        there = span(*spans[k])
        copy = pltpu.make_async_remote_copy(
            src_ref=ctr.at[there, :],
            dst_ref=far.at[there, :],
            send_sem=halo_send.at[k],
            recv_sem=halo_recv.at[k],
            device_id=at(side),
            device_id_type=MESH,
        )
        copy.start()
        far_copies.append(copy)

    def group_copy(n, k):
        return pltpu.make_async_remote_copy(
            src_ref=part.at[n, g],
            dst_ref=part.at[n, g],
            send_sem=part_send.at[n, k],
            recv_sem=part_recv.at[n, g],
            device_id=group(k),
            device_id_type=MESH,
        )

    def over_groups(n):
        for k in range(1, n_grp):
            src = lax.rem(g - k + n_grp, n_grp)
            pltpu.make_async_remote_copy(
                src_ref=part.at[n, src],
                dst_ref=part.at[n, src],
                send_sem=part_send.at[n, k],
                recv_sem=part_recv.at[n, src],
                device_id=group(k),
                device_id_type=MESH,
            ).wait_recv()
        both = part[n, 1]
        for k in range(2, n_grp):
            both = both + part[n, k]
        return both

    send_far(0)
    near_copy = pltpu.make_async_remote_copy(
        src_ref=ctr,
        dst_ref=near,
        send_sem=halo_send.at[4],
        recv_sem=halo_recv.at[4],
        device_id=at(-side),
        device_id_type=MESH,
    )
    near_copy.start()
    send_far(1)
    send_far(2)

    link_copies[1].wait_recv()
    part[0, g, 0:4, :] = cell_sums[4:8] + link[0, 0:4, :]
    part[0, g, 4:8, :] = link[1, 0:4, :]
    for k in range(1, n_grp):
        group_copy(0, k).start()
    link_copies[0].wait_recv()
    part[1, g, 0:4, :] = link[2, 0:4, :]

    @pl.when(side > 0)
    def _():
        for k in range(1, n_grp):
            group_copy(1, k).start()

    for c in (0, 2):
        damping(c, link[c, 4:5, :], link[c, 5:6, :])
    near_copy.wait_recv()

    def near_level(l, carry):
        rec = rtab[0, pl.ds(l, 1), :]
        for m in range(quads):
            r = pl.ds(pl.multiple_of(l * NDIR + m * SUB, SUB), SUB)
            base[1, r, :] = near[r, :] * rec
        return carry

    lax.fori_loop(0, levels, near_level, 0, unroll=6)
    chip = over_groups(0)
    sums[3] = chip
    chip_copy = pltpu.make_async_remote_copy(
        src_ref=sums.at[3],
        dst_ref=sums.at[2],
        send_sem=sums_send.at[1],
        recv_sem=sums_recv.at[1],
        device_id=at(side),
        device_id_type=MESH,
    )
    chip_copy.start()
    send_far(3)
    pass_copies = []
    for i, step in ((0, 1), (1, n_grp - 1)):
        far_copies[i].wait_recv()
        there = span(*spans[i])
        copy = pltpu.make_async_remote_copy(
            src_ref=far.at[there, :],
            dst_ref=far.at[there, :],
            send_sem=pass_send.at[i],
            recv_sem=pass_recv.at[i],
            device_id=group(step),
            device_id_type=MESH,
        )
        copy.start()
        pass_copies.append(copy)
    own = chip[0:4] + over_groups(1)[0:4]
    sums[1, 0:4, :] = own
    own_copy = pltpu.make_async_remote_copy(
        src_ref=sums.at[1],
        dst_ref=sums.at[0],
        send_sem=sums_send.at[0],
        recv_sem=sums_recv.at[0],
        device_id=at(-side),
        device_id_type=MESH,
    )
    own_copy.start()

    gain = {}

    def column(c, s4):
        count = jnp.maximum(s4[2:3], 1.0)
        mean_x = s4[0:1] / count
        mean_y = s4[1:2] / count
        sea_c = link[c, 4:5, :]
        wx = link[c, 6:7, :] - mean_x
        wy = link[c, 7:8, :] - mean_y
        gain[c] = [cos[m] * wx + sin[m] * wy for m in range(quads)]
        return CURRENT_TOP * jnp.tanh(mean_x), CURRENT_TOP * jnp.tanh(mean_y), sea_c

    flow_x, flow_y, _ = column(1, own)
    own_copy.wait_recv()
    flow_near, _, _ = column(0, sums[0])
    face_near = jnp.broadcast_to(-sign * (0.5 * (flow_near + flow_x)), wide)
    flow_y = jnp.broadcast_to(flow_y, wide)
    face_n = jnp.where(has_n, 0.5 * (flow_y + pltpu.roll(flow_y, LANES - 1, 1)), 0.0)
    face_s = jnp.where(has_s, 0.5 * (flow_y + pltpu.roll(flow_y, 1, 1)), 0.0)
    sea_w = jnp.broadcast_to(sea, wide)

    def forced(damped, c, m, fg):
        return damped * jnp.maximum(gain[c][m] * fg + (1.0 - WIND_GAIN), 1.0)

    def drift_rows(acc):
        dx = acc[0] * cos[0]
        dy = acc[0] * sin[0]
        for m in range(1, quads):
            dx = dx + acc[m] * cos[m]
            dy = dy + acc[m] * sin[m]
        dx = jnp.sum(dx, axis=0, keepdims=True)
        dy = jnp.sum(dy, axis=0, keepdims=True)
        return jnp.where(which == 0, dx, jnp.where(which == 1, dy, 0.0))

    def own_level(l, acc):
        fg = tab_ref[pl.ds(FG + l, 1), :]
        wt = tab_ref[pl.ds(WT + l, 1), :]
        out = []
        for m in range(quads):
            r = pl.ds(pl.multiple_of(l * NDIR + m * SUB, SUB), SUB)
            e = forced(base[0, r, :], 1, m, fg)
            other = forced(base[1, r, :], 0, m, fg)
            a = speed[0, r, :] + face_n
            b = speed[1, r, :] + face_s
            c = face_near - speed[2, r, :]
            flux_n = a * jnp.where(a > 0.0, e, pltpu.roll(e, LANES - 1, 1))
            flux_s = b * jnp.where(b > 0.0, pltpu.roll(e, 1, 1), e)
            u = sea_w * (e - flux_n + flux_s - c * jnp.where(c > 0.0, e, other))
            base[0, r, :] = e
            base[1, r, :] = u
            out.append(acc[m] + wt * u)
        return tuple(out)

    acc = lax.fori_loop(0, levels, own_level, (zero,) * quads, unroll=6)
    drift[3] = drift_rows(acc)
    partial_copy = pltpu.make_async_remote_copy(
        src_ref=drift.at[3],
        dst_ref=drift.at[2],
        send_sem=drift_send.at[1],
        recv_sem=drift_recv.at[1],
        device_id=at(side),
        device_id_type=MESH,
    )
    partial_copy.start()

    chip_copy.wait_recv()
    flow_far, _, sea_far = column(2, sums[2, 0:4, :] + chip[4:8])
    face_far = jnp.broadcast_to(sign * (0.5 * (flow_x + flow_far)), wide)

    def far_level(l, acc):
        fg = tab_ref[pl.ds(FG + l, 1), :]
        wt = tab_ref[pl.ds(WT + l, 1), :]
        rec = rtab[2, pl.ds(l, 1), :]
        out = []
        for m in range(quads):
            r = pl.ds(pl.multiple_of(l * NDIR + m * SUB, SUB), SUB)
            other = forced(far[r, :] * rec, 2, m, fg)
            a = speed[2, r, :] + face_far
            flux = a * jnp.where(a > 0.0, base[0, r, :], other)
            upd_ref[r, :] = base[1, r, :] - sea_w * flux
            out.append(acc[m] + wt * flux)
        return tuple(out)

    acc = (zero,) * quads

    def far_levels(start, count, acc):
        return lax.fori_loop(0, count, lambda i, acc: far_level(start + i, acc), acc, unroll=4)

    acc = far_levels(mine, shared_levels, acc)
    for k in (2, 3):
        far_copies[k].wait_recv()
        acc = far_levels(*spans[k], acc)
    for i in range(2):
        here = span(theirs + i * half, half)
        pltpu.make_async_remote_copy(
            src_ref=far.at[here, :],
            dst_ref=far.at[here, :],
            send_sem=pass_send.at[i],
            recv_sem=pass_recv.at[i],
            device_id=group(1 + i * (n_grp - 2)),
            device_id_type=MESH,
        ).wait_recv()
    acc = far_levels(theirs, shared_levels, acc)

    shared = drift_rows(acc)
    drift[1] = drift[3] - sea * shared
    full_copy = pltpu.make_async_remote_copy(
        src_ref=drift.at[1],
        dst_ref=drift.at[0],
        send_sem=drift_send.at[0],
        recv_sem=drift_recv.at[0],
        device_id=at(-side),
        device_id_type=MESH,
    )
    full_copy.start()
    partial_copy.wait_recv()
    last[...] = drift[2] + sea_far * shared
    for k in range(1, n_grp):
        group_copy(0, k).wait_send()

    @pl.when(side > 0)
    def _():
        for k in range(1, n_grp):
            group_copy(1, k).wait_send()
            share_copy(k).wait_send()

    for copy in link_copies + far_copies + pass_copies + [near_copy, chip_copy, own_copy, partial_copy]:
        copy.wait_send()
    full_copy.wait()
    drift_ref[0] = drift[0]
    drift_ref[1] = drift[1]
    drift_ref[2] = last[...]


def finish(upd_ref, drift, where_ref, upd_hbm, cell_hbm, cell_ref, sem):
    store = pltpu.make_async_copy(upd_ref, upd_hbm, sem.at[0])
    store.start()
    cells = where_ref.shape[1]
    for j in range(cells // LANES):
        here = pl.ds(j * LANES, LANES)
        role = where_ref[0:1, here]
        row = jnp.broadcast_to(where_ref[1:2, here], (SUB, LANES))
        out = jnp.zeros((SUB, LANES), F32)
        for c in range(3):
            out = jnp.where(role == c, jnp.take_along_axis(drift[c], row, axis=1), out)
        cell_ref[:, here] = out[0:2]
    cell_store = pltpu.make_async_copy(cell_ref, cell_hbm, sem.at[1])
    cell_store.start()
    cell_store.wait()
    store.wait()


def body(n_grp, n_dev, spectrum, sea_mask, wind, currents, coupling):
    bins, _, width = spectrum.shape
    levels = bins // NDIR
    cells = currents.shape[2]
    table, padded = bin_tables(levels)
    shared_levels = 8
    vmem = pl.BlockSpec(memory_space=pltpu.VMEM)
    hbm = pl.BlockSpec(memory_space=pltpu.HBM)
    dma = pltpu.SemaphoreType.DMA
    updated, drift, where = pl.pallas_call(
        functools.partial(kernel, n_grp, n_dev, levels, padded, shared_levels),
        out_shape=(
            jax.ShapeDtypeStruct((bins, width), F32),
            jax.ShapeDtypeStruct((3, SUB, width), F32),
            jax.ShapeDtypeStruct((2, cells), jnp.int32),
        ),
        in_specs=[hbm] * 6,
        out_specs=(vmem, vmem, vmem),
        scratch_shapes=[
            pltpu.VMEM((bins, width), F32),
            pltpu.VMEM((1, cells), jnp.int32),
            pltpu.VMEM((1, width), jnp.int32),
            pltpu.VMEM((2, width), F32),
            pltpu.VMEM((2, cells), F32),
            pltpu.VMEM(table.shape, F32),
            pltpu.VMEM((bins, width), F32),
            pltpu.VMEM((bins, width), F32),
            pltpu.VMEM((2, bins, width), F32),
            pltpu.VMEM((3, bins, width), F32),
            pltpu.VMEM((2, n_grp, SUB, width), F32),
            pltpu.VMEM((4, SUB, width), F32),
            pltpu.VMEM((4, SUB, width), F32),
            pltpu.VMEM((4, SUB, width), F32),
            pltpu.VMEM((SUB, width), F32),
            pltpu.VMEM((3, padded, width), F32),
            dma((6,)),
            dma((5,)),
            dma((5,)),
            dma((2,)),
            dma((2,)),
            dma((2, n_grp)),
            dma((2, n_grp)),
            dma((n_grp,)),
            dma((2,)),
            dma((2,)),
            dma((2,)),
            dma((2,)),
            dma((2,)),
            dma((2,)),
        ],
        compiler_params=pltpu.CompilerParams(
            collective_id=0, has_side_effects=True, vmem_limit_bytes=32 * 1024 * 1024
        ),
        name="wave_step",
    )(
        *[
            pltpu.with_memory_space_constraint(x, pltpu.HBM)
            for x in (
                spectrum.reshape(bins, width),
                sea_mask,
                wind.reshape(2, width),
                currents.reshape(2, cells),
                coupling,
                table,
            )
        ]
    )
    updated, cell_drift = pl.pallas_call(
        finish,
        out_shape=(
            jax.ShapeDtypeStruct((bins, width), F32),
            jax.ShapeDtypeStruct((2, cells), F32),
        ),
        in_specs=[vmem, vmem, vmem],
        out_specs=(hbm, hbm),
        scratch_shapes=[pltpu.VMEM((2, cells), F32), dma((2,))],
        compiler_params=pltpu.CompilerParams(vmem_limit_bytes=16 * 1024 * 1024),
        name="finish",
    )(updated, drift, where)
    return updated.reshape(bins, 1, width), cell_drift.reshape(1, 2, cells)


def solution(mesh):
    return jax.shard_map(
        functools.partial(body, mesh.shape["grp"], mesh.shape["dev"]),
        mesh=mesh,
        in_specs=(
            P(None, "dev", None),
            P("dev", None),
            P(None, "dev", None),
            P("grp", None, "dev"),
            P("grp", "dev"),
        ),
        out_specs=(P(None, "dev", None), P("grp", None, "dev")),
        check_vma=False,
    )
```

```python
import functools
import math

import jax
import jax.numpy as jnp
import numpy as np
from jax import lax
from jax.experimental import pallas as pl
from jax.experimental.pallas import tpu as pltpu
from jax.sharding import PartitionSpec as P

MESH = pl.DeviceIdType.MESH
F32 = jnp.float32
BF16 = jnp.bfloat16

NDIR = 32
FIRST_FREQ = 0.04
GROWTH = 1.1
SPEED_TOP = 0.45
CURRENT_TOP = 0.2
WIND_GAIN = 0.03
WHITECAP = 0.3
STEEP_SCALE = 0.4
STOKES_GAIN = 3.0
LANES = 128
SUB = 8
GROWTH_F = WIND_GAIN * 0.64


def bin_tables(levels):
    padded = -(-levels // SUB) * SUB
    heading = np.arange(NDIR) * (2.0 * math.pi / NDIR)
    freq = FIRST_FREQ * GROWTH ** np.arange(padded)
    rows = np.concatenate(
        [
            np.cos(heading),
            np.sin(heading),
            GROWTH_F * freq,
            freq**2,
            SPEED_TOP * FIRST_FREQ / freq,
            STOKES_GAIN * 0.1 * freq**4,
        ]
    )
    table = np.broadcast_to(rows[:, None], (rows.shape[0], LANES))
    return jnp.asarray(table.astype(np.float32)), padded


def split3(x):
    hi = x.astype(BF16)
    rest = x - hi.astype(F32)
    mid = rest.astype(BF16)
    low = (rest - mid.astype(F32)).astype(BF16)
    return jnp.concatenate([hi, mid, low], axis=0)


def sum3(x):
    n = x.shape[0] // 3
    return x[:n] + x[n : 2 * n] + x[2 * n :]


def kernel(
    n_grp,
    n_dev,
    levels,
    padded,
    shared_levels,
    spec_hbm,
    mask_hbm,
    wind_hbm,
    cur_hbm,
    coup_hbm,
    tab_hbm,
    upd_ref,
    drift_ref,
    where_ref,
    ctr,
    coup_ref,
    mask_ref,
    wind_ref,
    cur_ref,
    tab_ref,
    near,
    far,
    base,
    speed,
    part,
    link,
    sums,
    drift,
    last,
    rtab,
    load_sem,
    halo_send,
    halo_recv,
    pass_send,
    pass_recv,
    part_send,
    part_recv,
    share_send,
    link_send,
    link_recv,
    sums_send,
    sums_recv,
    drift_send,
    drift_recv,
):
    g = lax.axis_index("grp")
    d = lax.axis_index("dev")
    side = 2 * lax.rem(d, 2) - 1

    bins = levels * NDIR
    quads = NDIR // SUB
    COS, SIN, FG = 0, NDIR, 2 * NDIR
    F2, GS, WT = FG + padded, FG + 2 * padded, FG + 3 * padded

    def at(step):
        return {"grp": g, "dev": lax.rem(d + step + n_dev, n_dev)}

    def group(step):
        return {"grp": lax.rem(g + step, n_grp), "dev": d}

    loads = [
        pltpu.make_async_copy(src, dst, load_sem.at[i])
        for i, (src, dst) in enumerate(
            (
                (coup_hbm, coup_ref),
                (cur_hbm, cur_ref),
                (spec_hbm, ctr),
                (tab_hbm, tab_ref),
                (mask_hbm, mask_ref),
                (wind_hbm, wind_ref),
            )
        )
    ]
    for load in loads:
        load.start()
    barrier = pltpu.get_barrier_semaphore()
    for peer in [at(side), at(-side)] + [group(k) for k in range(1, n_grp)]:
        pl.semaphore_signal(barrier, inc=1, device_id=peer, device_id_type=MESH)

    def across(step):
        return {"grp": lax.rem(g + step, n_grp), "dev": lax.rem(d + side + n_dev, n_dev)}

    @pl.when(side < 0)
    def _():
        for k in range(1, n_grp):
            pl.semaphore_signal(barrier, inc=1, device_id=across(k), device_id_type=MESH)

    loads[0].wait()
    loads[1].wait()
    coup = coup_ref[...]
    slot = ((coup >> 7) - d + n_dev + 1) & (n_dev - 1)
    row = coup & (LANES - 1)
    cells = coup.shape[1]
    one_hot = jnp.where(
        lax.broadcasted_iota(jnp.int32, (LANES, cells), 0) == row, 1.0, 0.0
    ).astype(BF16)
    kind = lax.broadcasted_iota(jnp.int32, (2 * SUB, cells), 0)
    comp = kind & 3
    value = jnp.where(
        comp == 0, cur_ref[0:1, :], jnp.where(comp == 1, cur_ref[1:2, :], jnp.where(comp == 2, 1.0, 0.0))
    )
    value = jnp.where(jnp.logical_and((kind >> 2) == slot, g > 0), value, 0.0)
    cell_sums = sum3(
        lax.dot_general(
            split3(value), one_hot, (((1,), (1,)), ((), ())), preferred_element_type=F32
        )
    )
    link[1, 0:4, :] = jnp.where(side > 0, cell_sums[8:12], cell_sums[0:4])
    link[3, 0:4, :] = jnp.where(side > 0, cell_sums[0:4], cell_sums[8:12])
    part[1, g] = jnp.zeros((SUB, LANES), F32)
    sums[1] = jnp.zeros((SUB, LANES), F32)
    where_ref[0:1, :] = jnp.where(g > 0, 1 + (slot - 1) * side, 3)
    where_ref[1:2, :] = row

    for load in loads[2:]:
        load.wait()

    def add_level(l, acc):
        r = pl.multiple_of(l * NDIR, NDIR)
        e = ctr[pl.ds(r, SUB), :]
        for m in range(1, quads):
            e = e + ctr[pl.ds(r + m * SUB, SUB), :]
        return (
            acc[0] + e * tab_ref[pl.ds(FG + l, 1), :],
            acc[1] + e * tab_ref[pl.ds(F2 + l, 1), :],
        )

    zero = jnp.zeros((SUB, LANES), F32)
    total, moment = lax.fori_loop(0, levels, add_level, (zero, zero), unroll=4)
    sea = mask_ref[...].astype(F32)
    total = jnp.sum(total, axis=0, keepdims=True) * (0.1 / GROWTH_F) * sea
    moment = jnp.sum(moment, axis=0, keepdims=True) * 0.1 * sea
    is_sea = sea > 0.5
    mean_freq = jnp.where(is_sea, moment / jnp.where(is_sea, total, 1.0), 1.0)
    steepness = STEEP_SCALE * total * mean_freq**4
    damp = WHITECAP * (steepness / mean_freq) ** 2
    which = lax.broadcasted_iota(jnp.int32, (SUB, LANES), 0)
    for i in (1, 3):
        for n, term in enumerate((sea, damp, wind_ref[0:1, :], wind_ref[1:2, :])):
            link[i, 4 + n : 5 + n, :] = term

    def damping(c, sea_c, damp_c):
        for q in range(padded // SUB):
            f2 = tab_ref[pl.ds(F2 + q * SUB, SUB), :]
            rtab[c, pl.ds(q * SUB, SUB), :] = sea_c / (1.0 + f2 * damp_c)

    damping(1, sea, damp)
    wide = (SUB, LANES)
    sign = side.astype(F32)
    cos = [tab_ref[pl.ds(COS + m * SUB, SUB), :] for m in range(quads)]
    sin = [tab_ref[pl.ds(SIN + m * SUB, SUB), :] for m in range(quads)]
    lane = lax.broadcasted_iota(jnp.int32, wide, 1)
    has_n = lane < LANES - 1
    has_s = lane > 0
    away = [sign * cos[m] for m in range(quads)]

    def speed_level(l, carry):
        gs = tab_ref[pl.ds(GS + l, 1), :]
        rec = rtab[1, pl.ds(l, 1), :]
        for m in range(quads):
            r = pl.ds(pl.multiple_of(l * NDIR + m * SUB, SUB), SUB)
            y = gs * sin[m]
            speed[0, r, :] = jnp.where(has_n, y, 0.0)
            speed[1, r, :] = jnp.where(has_s, y, 0.0)
            speed[2, r, :] = gs * away[m]
            base[0, r, :] = ctr[r, :] * rec
        return carry

    lax.fori_loop(0, levels, speed_level, 0, unroll=4)

    pl.semaphore_wait(barrier, n_grp + 1 + jnp.where(side > 0, n_grp - 1, 0))

    link_copies = []
    for i, step in ((1, side), (0, -side)):
        copy = pltpu.make_async_remote_copy(
            src_ref=link.at[3 - 2 * i],
            dst_ref=link.at[2 * i],
            send_sem=link_send.at[i],
            recv_sem=link_recv.at[i],
            device_id=at(step),
            device_id_type=MESH,
        )
        copy.start()
        link_copies.append(copy)

    def share_copy(k):
        return pltpu.make_async_remote_copy(
            src_ref=link.at[1],
            dst_ref=part.at[1, g],
            send_sem=share_send.at[k],
            recv_sem=part_recv.at[1, g],
            device_id=across(k),
            device_id_type=MESH,
        )

    @pl.when(jnp.logical_and(side > 0, g > 0))
    def _():
        for k in range(1, n_grp):
            share_copy(k).start()


    half = shared_levels // 2
    parity = lax.rem(g, 2)
    mine, theirs = parity * shared_levels, (1 - parity) * shared_levels
    first, middle = 2 * shared_levels, 32
    spans = ((mine, half), (mine + half, half), (first, middle - first), (middle, levels - middle))

    def span(start, count):
        return pl.ds(pl.multiple_of(start * NDIR, NDIR), count * NDIR)

    far_copies = []

    def send_far(k):
        there = span(*spans[k])
        copy = pltpu.make_async_remote_copy(
            src_ref=ctr.at[there, :],
            dst_ref=far.at[there, :],
            send_sem=halo_send.at[k],
            recv_sem=halo_recv.at[k],
            device_id=at(side),
            device_id_type=MESH,
        )
        copy.start()
        far_copies.append(copy)

    def group_copy(n, k):
        return pltpu.make_async_remote_copy(
            src_ref=part.at[n, g],
            dst_ref=part.at[n, g],
            send_sem=part_send.at[n, k],
            recv_sem=part_recv.at[n, g],
            device_id=group(k),
            device_id_type=MESH,
        )

    def over_groups(n):
        for src in range(1, n_grp):

            @pl.when(g != src)
            def _(src=src):
                pltpu.make_async_remote_copy(
                    src_ref=part.at[n, src],
                    dst_ref=part.at[n, src],
                    send_sem=part_send.at[n, 1],
                    recv_sem=part_recv.at[n, src],
                    device_id=group(1),
                    device_id_type=MESH,
                ).wait_recv()

        both = part[n, 1]
        for k in range(2, n_grp):
            both = both + part[n, k]
        return both

    send_far(0)
    near_copy = pltpu.make_async_remote_copy(
        src_ref=ctr,
        dst_ref=near,
        send_sem=halo_send.at[4],
        recv_sem=halo_recv.at[4],
        device_id=at(-side),
        device_id_type=MESH,
    )
    near_copy.start()
    send_far(1)
    send_far(2)

    link_copies[1].wait_recv()
    part[0, g, 0:4, :] = cell_sums[4:8] + link[0, 0:4, :]
    part[0, g, 4:8, :] = link[1, 0:4, :]

    @pl.when(g > 0)
    def _():
        for k in range(1, n_grp):
            group_copy(0, k).start()

    link_copies[0].wait_recv()
    part[1, g, 0:4, :] = link[2, 0:4, :]

    @pl.when(jnp.logical_and(side > 0, g > 0))
    def _():
        for k in range(1, n_grp):
            group_copy(1, k).start()

    for c in (0, 2):
        damping(c, link[c, 4:5, :], link[c, 5:6, :])
    near_copy.wait_recv()

    def near_level(l, carry):
        rec = rtab[0, pl.ds(l, 1), :]
        for m in range(quads):
            r = pl.ds(pl.multiple_of(l * NDIR + m * SUB, SUB), SUB)
            base[1, r, :] = near[r, :] * rec
        return carry

    lax.fori_loop(0, levels, near_level, 0, unroll=6)
    chip = over_groups(0)
    sums[3] = chip
    chip_copy = pltpu.make_async_remote_copy(
        src_ref=sums.at[3],
        dst_ref=sums.at[2],
        send_sem=sums_send.at[1],
        recv_sem=sums_recv.at[1],
        device_id=at(side),
        device_id_type=MESH,
    )
    chip_copy.start()
    send_far(3)
    pass_copies = []
    for i, step in ((0, 1), (1, n_grp - 1)):
        far_copies[i].wait_recv()
        there = span(*spans[i])
        copy = pltpu.make_async_remote_copy(
            src_ref=far.at[there, :],
            dst_ref=far.at[there, :],
            send_sem=pass_send.at[i],
            recv_sem=pass_recv.at[i],
            device_id=group(step),
            device_id_type=MESH,
        )
        copy.start()
        pass_copies.append(copy)
    own = chip[0:4] + over_groups(1)[0:4]
    sums[1, 0:4, :] = own
    own_copy = pltpu.make_async_remote_copy(
        src_ref=sums.at[1],
        dst_ref=sums.at[0],
        send_sem=sums_send.at[0],
        recv_sem=sums_recv.at[0],
        device_id=at(-side),
        device_id_type=MESH,
    )
    own_copy.start()

    gain = {}

    def column(c, s4):
        count = jnp.maximum(s4[2:3], 1.0)
        mean_x = s4[0:1] / count
        mean_y = s4[1:2] / count
        sea_c = link[c, 4:5, :]
        wx = link[c, 6:7, :] - mean_x
        wy = link[c, 7:8, :] - mean_y
        gain[c] = [cos[m] * wx + sin[m] * wy for m in range(quads)]
        return CURRENT_TOP * jnp.tanh(mean_x), CURRENT_TOP * jnp.tanh(mean_y), sea_c

    flow_x, flow_y, _ = column(1, own)
    own_copy.wait_recv()
    flow_near, _, _ = column(0, sums[0])
    face_near = jnp.broadcast_to(-sign * (0.5 * (flow_near + flow_x)), wide)
    flow_y = jnp.broadcast_to(flow_y, wide)
    face_n = jnp.where(has_n, 0.5 * (flow_y + pltpu.roll(flow_y, LANES - 1, 1)), 0.0)
    face_s = jnp.where(has_s, 0.5 * (flow_y + pltpu.roll(flow_y, 1, 1)), 0.0)
    sea_w = jnp.broadcast_to(sea, wide)

    def forced(damped, c, m, fg):
        return damped * jnp.maximum(gain[c][m] * fg + (1.0 - WIND_GAIN), 1.0)

    def drift_rows(acc):
        dx = acc[0] * cos[0]
        dy = acc[0] * sin[0]
        for m in range(1, quads):
            dx = dx + acc[m] * cos[m]
            dy = dy + acc[m] * sin[m]
        dx = jnp.sum(dx, axis=0, keepdims=True)
        dy = jnp.sum(dy, axis=0, keepdims=True)
        return jnp.where(which == 0, dx, jnp.where(which == 1, dy, 0.0))

    def own_level(l, acc):
        fg = tab_ref[pl.ds(FG + l, 1), :]
        wt = tab_ref[pl.ds(WT + l, 1), :]
        out = []
        for m in range(quads):
            r = pl.ds(pl.multiple_of(l * NDIR + m * SUB, SUB), SUB)
            e = forced(base[0, r, :], 1, m, fg)
            other = forced(base[1, r, :], 0, m, fg)
            a = speed[0, r, :] + face_n
            b = speed[1, r, :] + face_s
            c = face_near - speed[2, r, :]
            flux_n = a * jnp.where(a > 0.0, e, pltpu.roll(e, LANES - 1, 1))
            flux_s = b * jnp.where(b > 0.0, pltpu.roll(e, 1, 1), e)
            u = sea_w * (e - flux_n + flux_s - c * jnp.where(c > 0.0, e, other))
            base[0, r, :] = e
            base[1, r, :] = u
            out.append(acc[m] + wt * u)
        return tuple(out)

    acc = lax.fori_loop(0, levels, own_level, (zero,) * quads, unroll=6)
    drift[3] = drift_rows(acc)
    partial_copy = pltpu.make_async_remote_copy(
        src_ref=drift.at[3],
        dst_ref=drift.at[2],
        send_sem=drift_send.at[1],
        recv_sem=drift_recv.at[1],
        device_id=at(side),
        device_id_type=MESH,
    )
    partial_copy.start()

    chip_copy.wait_recv()
    flow_far, _, sea_far = column(2, sums[2, 0:4, :] + chip[4:8])
    face_far = jnp.broadcast_to(sign * (0.5 * (flow_x + flow_far)), wide)

    def far_level(l, acc):
        fg = tab_ref[pl.ds(FG + l, 1), :]
        wt = tab_ref[pl.ds(WT + l, 1), :]
        rec = rtab[2, pl.ds(l, 1), :]
        out = []
        for m in range(quads):
            r = pl.ds(pl.multiple_of(l * NDIR + m * SUB, SUB), SUB)
            other = forced(far[r, :] * rec, 2, m, fg)
            a = speed[2, r, :] + face_far
            flux = a * jnp.where(a > 0.0, base[0, r, :], other)
            upd_ref[r, :] = base[1, r, :] - sea_w * flux
            out.append(acc[m] + wt * flux)
        return tuple(out)

    acc = (zero,) * quads

    def far_levels(start, count, acc):
        return lax.fori_loop(0, count, lambda i, acc: far_level(start + i, acc), acc, unroll=4)

    acc = far_levels(mine, shared_levels, acc)
    for k in (2, 3):
        far_copies[k].wait_recv()
        acc = far_levels(*spans[k], acc)
    for i in range(2):
        here = span(theirs + i * half, half)
        pltpu.make_async_remote_copy(
            src_ref=far.at[here, :],
            dst_ref=far.at[here, :],
            send_sem=pass_send.at[i],
            recv_sem=pass_recv.at[i],
            device_id=group(1 + i * (n_grp - 2)),
            device_id_type=MESH,
        ).wait_recv()
    acc = far_levels(theirs, shared_levels, acc)

    shared = drift_rows(acc)
    drift[1] = drift[3] - sea * shared
    full_copy = pltpu.make_async_remote_copy(
        src_ref=drift.at[1],
        dst_ref=drift.at[0],
        send_sem=drift_send.at[0],
        recv_sem=drift_recv.at[0],
        device_id=at(-side),
        device_id_type=MESH,
    )
    full_copy.start()
    partial_copy.wait_recv()
    last[...] = drift[2] + sea_far * shared
    @pl.when(g > 0)
    def _():
        for k in range(1, n_grp):
            group_copy(0, k).wait_send()

    @pl.when(jnp.logical_and(side > 0, g > 0))
    def _():
        for k in range(1, n_grp):
            group_copy(1, k).wait_send()
            share_copy(k).wait_send()

    for copy in link_copies + far_copies + pass_copies + [near_copy, chip_copy, own_copy, partial_copy]:
        copy.wait_send()
    full_copy.wait()
    drift_ref[0] = drift[0]
    drift_ref[1] = drift[1]
    drift_ref[2] = last[...]


def finish(upd_ref, drift, where_ref, upd_hbm, cell_hbm, cell_ref, sem):
    store = pltpu.make_async_copy(upd_ref, upd_hbm, sem.at[0])
    store.start()
    cells = where_ref.shape[1]
    for j in range(cells // LANES):
        here = pl.ds(j * LANES, LANES)
        role = where_ref[0:1, here]
        row = jnp.broadcast_to(where_ref[1:2, here], (SUB, LANES))
        out = jnp.zeros((SUB, LANES), F32)
        for c in range(3):
            out = jnp.where(role == c, jnp.take_along_axis(drift[c], row, axis=1), out)
        cell_ref[:, here] = out[0:2]
    cell_store = pltpu.make_async_copy(cell_ref, cell_hbm, sem.at[1])
    cell_store.start()
    cell_store.wait()
    store.wait()


def body(n_grp, n_dev, spectrum, sea_mask, wind, currents, coupling):
    bins, _, width = spectrum.shape
    levels = bins // NDIR
    cells = currents.shape[2]
    table, padded = bin_tables(levels)
    shared_levels = 8
    vmem = pl.BlockSpec(memory_space=pltpu.VMEM)
    hbm = pl.BlockSpec(memory_space=pltpu.HBM)
    dma = pltpu.SemaphoreType.DMA
    updated, drift, where = pl.pallas_call(
        functools.partial(kernel, n_grp, n_dev, levels, padded, shared_levels),
        out_shape=(
            jax.ShapeDtypeStruct((bins, width), F32),
            jax.ShapeDtypeStruct((3, SUB, width), F32),
            jax.ShapeDtypeStruct((2, cells), jnp.int32),
        ),
        in_specs=[hbm] * 6,
        out_specs=(vmem, vmem, vmem),
        scratch_shapes=[
            pltpu.VMEM((bins, width), F32),
            pltpu.VMEM((1, cells), jnp.int32),
            pltpu.VMEM((1, width), jnp.int32),
            pltpu.VMEM((2, width), F32),
            pltpu.VMEM((2, cells), F32),
            pltpu.VMEM(table.shape, F32),
            pltpu.VMEM((bins, width), F32),
            pltpu.VMEM((bins, width), F32),
            pltpu.VMEM((2, bins, width), F32),
            pltpu.VMEM((3, bins, width), F32),
            pltpu.VMEM((2, n_grp, SUB, width), F32),
            pltpu.VMEM((4, SUB, width), F32),
            pltpu.VMEM((4, SUB, width), F32),
            pltpu.VMEM((4, SUB, width), F32),
            pltpu.VMEM((SUB, width), F32),
            pltpu.VMEM((3, padded, width), F32),
            dma((6,)),
            dma((5,)),
            dma((5,)),
            dma((2,)),
            dma((2,)),
            dma((2, n_grp)),
            dma((2, n_grp)),
            dma((n_grp,)),
            dma((2,)),
            dma((2,)),
            dma((2,)),
            dma((2,)),
            dma((2,)),
            dma((2,)),
        ],
        compiler_params=pltpu.CompilerParams(
            collective_id=0, has_side_effects=True, vmem_limit_bytes=32 * 1024 * 1024
        ),
        name="wave_step",
    )(
        *[
            pltpu.with_memory_space_constraint(x, pltpu.HBM)
            for x in (
                spectrum.reshape(bins, width),
                sea_mask,
                wind.reshape(2, width),
                currents.reshape(2, cells),
                coupling,
                table,
            )
        ]
    )
    updated, cell_drift = pl.pallas_call(
        finish,
        out_shape=(
            jax.ShapeDtypeStruct((bins, width), F32),
            jax.ShapeDtypeStruct((2, cells), F32),
        ),
        in_specs=[vmem, vmem, vmem],
        out_specs=(hbm, hbm),
        scratch_shapes=[pltpu.VMEM((2, cells), F32), dma((2,))],
        compiler_params=pltpu.CompilerParams(vmem_limit_bytes=16 * 1024 * 1024),
        name="finish",
    )(updated, drift, where)
    return updated.reshape(bins, 1, width), cell_drift.reshape(1, 2, cells)


def solution(mesh):
    return jax.shard_map(
        functools.partial(body, mesh.shape["grp"], mesh.shape["dev"]),
        mesh=mesh,
        in_specs=(
            P(None, "dev", None),
            P("dev", None),
            P(None, "dev", None),
            P("grp", None, "dev"),
            P("grp", "dev"),
        ),
        out_specs=(P(None, "dev", None), P("grp", None, "dev")),
        check_vma=False,
    )
```

```python
import functools
import math

import jax
import jax.numpy as jnp
import numpy as np
from jax import lax
from jax.experimental import pallas as pl
from jax.experimental.pallas import tpu as pltpu
from jax.sharding import PartitionSpec as P

MESH = pl.DeviceIdType.MESH
F32 = jnp.float32
BF16 = jnp.bfloat16

NDIR = 32
FIRST_FREQ = 0.04
GROWTH = 1.1
SPEED_TOP = 0.45
CURRENT_TOP = 0.2
WIND_GAIN = 0.03
WHITECAP = 0.3
STEEP_SCALE = 0.4
STOKES_GAIN = 3.0
LANES = 128
SUB = 8
GROWTH_F = WIND_GAIN * 0.64


def bin_tables(levels):
    padded = -(-levels // SUB) * SUB
    heading = np.arange(NDIR) * (2.0 * math.pi / NDIR)
    freq = FIRST_FREQ * GROWTH ** np.arange(padded)
    rows = np.concatenate(
        [
            np.cos(heading),
            np.sin(heading),
            GROWTH_F * freq,
            freq**2,
            SPEED_TOP * FIRST_FREQ / freq,
            STOKES_GAIN * 0.1 * freq**4,
        ]
    )
    table = np.broadcast_to(rows[:, None], (rows.shape[0], LANES))
    return jnp.asarray(table.astype(np.float32)), padded


def split3(x):
    hi = x.astype(BF16)
    rest = x - hi.astype(F32)
    mid = rest.astype(BF16)
    low = (rest - mid.astype(F32)).astype(BF16)
    return jnp.concatenate([hi, mid, low], axis=0)


def sum3(x):
    n = x.shape[0] // 3
    return x[:n] + x[n : 2 * n] + x[2 * n :]


def kernel(
    n_grp,
    n_dev,
    levels,
    padded,
    shared_levels,
    spec_hbm,
    mask_hbm,
    wind_hbm,
    cur_hbm,
    coup_hbm,
    tab_hbm,
    upd_ref,
    drift_ref,
    where_ref,
    ctr,
    coup_ref,
    mask_ref,
    wind_ref,
    cur_ref,
    tab_ref,
    near,
    far,
    base,
    speed,
    part,
    link,
    sums,
    drift,
    last,
    rtab,
    near_flow,
    load_sem,
    halo_send,
    halo_recv,
    pass_send,
    pass_recv,
    part_send,
    part_recv,
    share_send,
    link_send,
    link_recv,
    sums_send,
    sums_recv,
    drift_send,
    drift_recv,
):
    g = lax.axis_index("grp")
    d = lax.axis_index("dev")
    side = 2 * lax.rem(d, 2) - 1

    bins = levels * NDIR
    quads = NDIR // SUB
    COS, SIN, FG = 0, NDIR, 2 * NDIR
    F2, GS, WT = FG + padded, FG + 2 * padded, FG + 3 * padded

    def at(step):
        return {"grp": g, "dev": lax.rem(d + step + n_dev, n_dev)}

    def group(step):
        return {"grp": lax.rem(g + step, n_grp), "dev": d}

    loads = [
        pltpu.make_async_copy(src, dst, load_sem.at[i])
        for i, (src, dst) in enumerate(
            (
                (coup_hbm, coup_ref),
                (cur_hbm, cur_ref),
                (spec_hbm, ctr),
                (tab_hbm, tab_ref),
                (mask_hbm, mask_ref),
                (wind_hbm, wind_ref),
            )
        )
    ]
    for load in loads:
        load.start()
    barrier = pltpu.get_barrier_semaphore()
    for peer in [at(side), at(-side)] + [group(k) for k in range(1, n_grp)]:
        pl.semaphore_signal(barrier, inc=1, device_id=peer, device_id_type=MESH)

    def across(step):
        return {"grp": lax.rem(g + step, n_grp), "dev": lax.rem(d + side + n_dev, n_dev)}

    @pl.when(side < 0)
    def _():
        for k in range(1, n_grp):
            pl.semaphore_signal(barrier, inc=1, device_id=across(k), device_id_type=MESH)

    loads[0].wait()
    loads[1].wait()
    coup = coup_ref[...]
    slot = ((coup >> 7) - d + n_dev + 1) & (n_dev - 1)
    row = coup & (LANES - 1)
    cells = coup.shape[1]
    one_hot = jnp.where(
        lax.broadcasted_iota(jnp.int32, (LANES, cells), 0) == row, 1.0, 0.0
    ).astype(BF16)
    kind = lax.broadcasted_iota(jnp.int32, (2 * SUB, cells), 0)
    comp = kind & 3
    value = jnp.where(
        comp == 0, cur_ref[0:1, :], jnp.where(comp == 1, cur_ref[1:2, :], jnp.where(comp == 2, 1.0, 0.0))
    )
    value = jnp.where(jnp.logical_and((kind >> 2) == slot, g > 0), value, 0.0)
    cell_sums = sum3(
        lax.dot_general(
            split3(value), one_hot, (((1,), (1,)), ((), ())), preferred_element_type=F32
        )
    )
    link[1, 0:4, :] = jnp.where(side > 0, cell_sums[8:12], cell_sums[0:4])
    link[3, 0:4, :] = jnp.where(side > 0, cell_sums[0:4], cell_sums[8:12])
    part[1, g] = jnp.zeros((SUB, LANES), F32)
    sums[1] = jnp.zeros((SUB, LANES), F32)
    where_ref[0:1, :] = jnp.where(g > 0, 1 + (slot - 1) * side, 3)
    where_ref[1:2, :] = row

    for load in loads[2:]:
        load.wait()

    def add_level(l, acc):
        r = pl.multiple_of(l * NDIR, NDIR)
        e = ctr[pl.ds(r, SUB), :]
        for m in range(1, quads):
            e = e + ctr[pl.ds(r + m * SUB, SUB), :]
        return (
            acc[0] + e * tab_ref[pl.ds(FG + l, 1), :],
            acc[1] + e * tab_ref[pl.ds(F2 + l, 1), :],
        )

    zero = jnp.zeros((SUB, LANES), F32)
    total, moment = lax.fori_loop(0, levels, add_level, (zero, zero), unroll=4)
    sea = mask_ref[...].astype(F32)
    total = jnp.sum(total, axis=0, keepdims=True) * (0.1 / GROWTH_F) * sea
    moment = jnp.sum(moment, axis=0, keepdims=True) * 0.1 * sea
    is_sea = sea > 0.5
    mean_freq = jnp.where(is_sea, moment / jnp.where(is_sea, total, 1.0), 1.0)
    steepness = STEEP_SCALE * total * mean_freq**4
    damp = WHITECAP * (steepness / mean_freq) ** 2
    which = lax.broadcasted_iota(jnp.int32, (SUB, LANES), 0)
    for i in (1, 3):
        for n, term in enumerate((sea, damp, wind_ref[0:1, :], wind_ref[1:2, :])):
            link[i, 4 + n : 5 + n, :] = term

    def damping(c, sea_c, damp_c):
        for q in range(padded // SUB):
            f2 = tab_ref[pl.ds(F2 + q * SUB, SUB), :]
            rtab[c, pl.ds(q * SUB, SUB), :] = sea_c / (1.0 + f2 * damp_c)

    damping(1, sea, damp)
    wide = (SUB, LANES)
    sign = side.astype(F32)
    cos = [tab_ref[pl.ds(COS + m * SUB, SUB), :] for m in range(quads)]
    sin = [tab_ref[pl.ds(SIN + m * SUB, SUB), :] for m in range(quads)]
    lane = lax.broadcasted_iota(jnp.int32, wide, 1)
    has_n = lane < LANES - 1
    has_s = lane > 0
    away = [sign * cos[m] for m in range(quads)]

    def speed_level(l, carry):
        gs = tab_ref[pl.ds(GS + l, 1), :]
        rec = rtab[1, pl.ds(l, 1), :]
        for m in range(quads):
            r = pl.ds(pl.multiple_of(l * NDIR + m * SUB, SUB), SUB)
            y = gs * sin[m]
            speed[0, r, :] = jnp.where(has_n, y, 0.0)
            speed[1, r, :] = jnp.where(has_s, y, 0.0)
            speed[2, r, :] = gs * away[m]
            base[0, r, :] = ctr[r, :] * rec
        return carry

    lax.fori_loop(0, levels, speed_level, 0, unroll=4)

    pl.semaphore_wait(barrier, n_grp + 1 + jnp.where(side > 0, n_grp - 1, 0))

    link_copies = []
    for i, step in ((1, side), (0, -side)):
        copy = pltpu.make_async_remote_copy(
            src_ref=link.at[3 - 2 * i],
            dst_ref=link.at[2 * i],
            send_sem=link_send.at[i],
            recv_sem=link_recv.at[i],
            device_id=at(step),
            device_id_type=MESH,
        )
        copy.start()
        link_copies.append(copy)

    def share_copy(k):
        return pltpu.make_async_remote_copy(
            src_ref=link.at[1],
            dst_ref=part.at[1, g],
            send_sem=share_send.at[k],
            recv_sem=part_recv.at[1, g],
            device_id=across(k),
            device_id_type=MESH,
        )

    @pl.when(jnp.logical_and(side > 0, g > 0))
    def _():
        for k in range(1, n_grp):
            share_copy(k).start()


    half = shared_levels // 2
    parity = lax.rem(g, 2)
    mine, theirs = parity * shared_levels, (1 - parity) * shared_levels
    first, middle = 2 * shared_levels, 32
    spans = ((mine, half), (mine + half, half), (first, middle - first), (middle, levels - middle))

    def span(start, count):
        return pl.ds(pl.multiple_of(start * NDIR, NDIR), count * NDIR)

    far_copies = []

    def send_far(k):
        there = span(*spans[k])
        copy = pltpu.make_async_remote_copy(
            src_ref=ctr.at[there, :],
            dst_ref=far.at[there, :],
            send_sem=halo_send.at[k],
            recv_sem=halo_recv.at[k],
            device_id=at(side),
            device_id_type=MESH,
        )
        copy.start()
        far_copies.append(copy)

    def group_copy(n, k):
        return pltpu.make_async_remote_copy(
            src_ref=part.at[n, g],
            dst_ref=part.at[n, g],
            send_sem=part_send.at[n, k],
            recv_sem=part_recv.at[n, g],
            device_id=group(k),
            device_id_type=MESH,
        )

    def over_groups(n):
        for src in range(1, n_grp):

            @pl.when(g != src)
            def _(src=src):
                pltpu.make_async_remote_copy(
                    src_ref=part.at[n, src],
                    dst_ref=part.at[n, src],
                    send_sem=part_send.at[n, 1],
                    recv_sem=part_recv.at[n, src],
                    device_id=group(1),
                    device_id_type=MESH,
                ).wait_recv()

        both = part[n, 1]
        for k in range(2, n_grp):
            both = both + part[n, k]
        return both

    send_far(0)
    near_copy = pltpu.make_async_remote_copy(
        src_ref=ctr,
        dst_ref=near,
        send_sem=halo_send.at[4],
        recv_sem=halo_recv.at[4],
        device_id=at(-side),
        device_id_type=MESH,
    )
    near_copy.start()
    send_far(1)
    send_far(2)

    link_copies[1].wait_recv()
    part[0, g, 0:4, :] = cell_sums[4:8] + link[0, 0:4, :]
    part[0, g, 4:8, :] = link[1, 0:4, :]

    @pl.when(g > 0)
    def _():
        for k in range(1, n_grp):
            group_copy(0, k).start()

    link_copies[0].wait_recv()
    part[1, g, 0:4, :] = link[2, 0:4, :]

    @pl.when(jnp.logical_and(side > 0, g > 0))
    def _():
        for k in range(1, n_grp):
            group_copy(1, k).start()

    for c in (0, 2):
        damping(c, link[c, 4:5, :], link[c, 5:6, :])
    near_copy.wait_recv()

    def near_level(l, carry):
        rec = rtab[0, pl.ds(l, 1), :]
        for m in range(quads):
            r = pl.ds(pl.multiple_of(l * NDIR + m * SUB, SUB), SUB)
            base[1, r, :] = near[r, :] * rec
        return carry

    lax.fori_loop(0, levels, near_level, 0, unroll=6)
    chip = over_groups(0)
    sums[3] = chip
    chip_copy = pltpu.make_async_remote_copy(
        src_ref=sums.at[3],
        dst_ref=sums.at[2],
        send_sem=sums_send.at[1],
        recv_sem=sums_recv.at[1],
        device_id=at(side),
        device_id_type=MESH,
    )
    chip_copy.start()
    send_far(3)
    pass_copies = []
    for i, step in ((0, 1), (1, n_grp - 1)):
        far_copies[i].wait_recv()
        there = span(*spans[i])
        copy = pltpu.make_async_remote_copy(
            src_ref=far.at[there, :],
            dst_ref=far.at[there, :],
            send_sem=pass_send.at[i],
            recv_sem=pass_recv.at[i],
            device_id=group(step),
            device_id_type=MESH,
        )
        copy.start()
        pass_copies.append(copy)
    gain = {}

    def column(c, s4):
        count = jnp.maximum(s4[2:3], 1.0)
        mean_x = s4[0:1] / count
        mean_y = s4[1:2] / count
        sea_c = link[c, 4:5, :]
        wx = link[c, 6:7, :] - mean_x
        wy = link[c, 7:8, :] - mean_y
        gain[c] = [cos[m] * wx + sin[m] * wy for m in range(quads)]
        return CURRENT_TOP * jnp.tanh(mean_x), CURRENT_TOP * jnp.tanh(mean_y), sea_c

    def near_forced():
        pltpu.make_async_remote_copy(
            src_ref=sums.at[1],
            dst_ref=sums.at[0],
            send_sem=sums_send.at[0],
            recv_sem=sums_recv.at[0],
            device_id=at(-side),
            device_id_type=MESH,
        ).wait_recv()
        near_flow[...] = jnp.broadcast_to(column(0, sums[0])[0], wide)

        def level(l, carry):
            fg = tab_ref[pl.ds(FG + l, 1), :]
            for m in range(quads):
                r = pl.ds(pl.multiple_of(l * NDIR + m * SUB, SUB), SUB)
                base[1, r, :] = base[1, r, :] * jnp.maximum(
                    gain[0][m] * fg + (1.0 - WIND_GAIN), 1.0
                )
            return carry

        lax.fori_loop(0, levels, level, 0, unroll=6)

    pl.when(side > 0)(near_forced)
    own = chip[0:4] + over_groups(1)[0:4]
    sums[1, 0:4, :] = own
    own_copy = pltpu.make_async_remote_copy(
        src_ref=sums.at[1],
        dst_ref=sums.at[0],
        send_sem=sums_send.at[0],
        recv_sem=sums_recv.at[0],
        device_id=at(-side),
        device_id_type=MESH,
    )
    own_copy.start()

    flow_x, flow_y, _ = column(1, own)
    pl.when(side < 0)(near_forced)
    face_near = jnp.broadcast_to(-sign * (0.5 * (near_flow[...] + flow_x)), wide)
    flow_y = jnp.broadcast_to(flow_y, wide)
    face_n = jnp.where(has_n, 0.5 * (flow_y + pltpu.roll(flow_y, LANES - 1, 1)), 0.0)
    face_s = jnp.where(has_s, 0.5 * (flow_y + pltpu.roll(flow_y, 1, 1)), 0.0)
    sea_w = jnp.broadcast_to(sea, wide)

    def forced(damped, c, m, fg):
        return damped * jnp.maximum(gain[c][m] * fg + (1.0 - WIND_GAIN), 1.0)

    def drift_rows(acc):
        dx = acc[0] * cos[0]
        dy = acc[0] * sin[0]
        for m in range(1, quads):
            dx = dx + acc[m] * cos[m]
            dy = dy + acc[m] * sin[m]
        dx = jnp.sum(dx, axis=0, keepdims=True)
        dy = jnp.sum(dy, axis=0, keepdims=True)
        return jnp.where(which == 0, dx, jnp.where(which == 1, dy, 0.0))

    def own_level(l, acc):
        fg = tab_ref[pl.ds(FG + l, 1), :]
        wt = tab_ref[pl.ds(WT + l, 1), :]
        out = []
        for m in range(quads):
            r = pl.ds(pl.multiple_of(l * NDIR + m * SUB, SUB), SUB)
            e = forced(base[0, r, :], 1, m, fg)
            other = base[1, r, :]
            a = speed[0, r, :] + face_n
            b = speed[1, r, :] + face_s
            c = face_near - speed[2, r, :]
            flux_n = a * jnp.where(a > 0.0, e, pltpu.roll(e, LANES - 1, 1))
            flux_s = b * jnp.where(b > 0.0, pltpu.roll(e, 1, 1), e)
            u = sea_w * (e - flux_n + flux_s - c * jnp.where(c > 0.0, e, other))
            base[0, r, :] = e
            base[1, r, :] = u
            out.append(acc[m] + wt * u)
        return tuple(out)

    acc = lax.fori_loop(0, levels, own_level, (zero,) * quads, unroll=6)
    drift[3] = drift_rows(acc)
    partial_copy = pltpu.make_async_remote_copy(
        src_ref=drift.at[3],
        dst_ref=drift.at[2],
        send_sem=drift_send.at[1],
        recv_sem=drift_recv.at[1],
        device_id=at(side),
        device_id_type=MESH,
    )
    partial_copy.start()

    chip_copy.wait_recv()
    flow_far, _, sea_far = column(2, sums[2, 0:4, :] + chip[4:8])
    face_far = jnp.broadcast_to(sign * (0.5 * (flow_x + flow_far)), wide)

    def far_level(l, acc):
        fg = tab_ref[pl.ds(FG + l, 1), :]
        wt = tab_ref[pl.ds(WT + l, 1), :]
        rec = rtab[2, pl.ds(l, 1), :]
        out = []
        for m in range(quads):
            r = pl.ds(pl.multiple_of(l * NDIR + m * SUB, SUB), SUB)
            other = forced(far[r, :] * rec, 2, m, fg)
            a = speed[2, r, :] + face_far
            flux = a * jnp.where(a > 0.0, base[0, r, :], other)
            upd_ref[r, :] = base[1, r, :] - sea_w * flux
            out.append(acc[m] + wt * flux)
        return tuple(out)

    acc = (zero,) * quads

    def far_levels(start, count, acc):
        return lax.fori_loop(0, count, lambda i, acc: far_level(start + i, acc), acc, unroll=4)

    acc = far_levels(mine, shared_levels, acc)
    for k in (2, 3):
        far_copies[k].wait_recv()
        acc = far_levels(*spans[k], acc)
    for i in range(2):
        here = span(theirs + i * half, half)
        pltpu.make_async_remote_copy(
            src_ref=far.at[here, :],
            dst_ref=far.at[here, :],
            send_sem=pass_send.at[i],
            recv_sem=pass_recv.at[i],
            device_id=group(1 + i * (n_grp - 2)),
            device_id_type=MESH,
        ).wait_recv()
    acc = far_levels(theirs, shared_levels, acc)

    shared = drift_rows(acc)
    drift[1] = drift[3] - sea * shared
    full_copy = pltpu.make_async_remote_copy(
        src_ref=drift.at[1],
        dst_ref=drift.at[0],
        send_sem=drift_send.at[0],
        recv_sem=drift_recv.at[0],
        device_id=at(-side),
        device_id_type=MESH,
    )
    full_copy.start()
    partial_copy.wait_recv()
    last[...] = drift[2] + sea_far * shared
    @pl.when(g > 0)
    def _():
        for k in range(1, n_grp):
            group_copy(0, k).wait_send()

    @pl.when(jnp.logical_and(side > 0, g > 0))
    def _():
        for k in range(1, n_grp):
            group_copy(1, k).wait_send()
            share_copy(k).wait_send()

    for copy in link_copies + far_copies + pass_copies + [near_copy, chip_copy, own_copy, partial_copy]:
        copy.wait_send()
    full_copy.wait()
    drift_ref[0] = drift[0]
    drift_ref[1] = drift[1]
    drift_ref[2] = last[...]


def finish(upd_ref, drift, where_ref, upd_hbm, cell_hbm, cell_ref, sem):
    store = pltpu.make_async_copy(upd_ref, upd_hbm, sem.at[0])
    store.start()
    cells = where_ref.shape[1]
    for j in range(cells // LANES):
        here = pl.ds(j * LANES, LANES)
        role = where_ref[0:1, here]
        row = jnp.broadcast_to(where_ref[1:2, here], (SUB, LANES))
        out = jnp.zeros((SUB, LANES), F32)
        for c in range(3):
            out = jnp.where(role == c, jnp.take_along_axis(drift[c], row, axis=1), out)
        cell_ref[:, here] = out[0:2]
    cell_store = pltpu.make_async_copy(cell_ref, cell_hbm, sem.at[1])
    cell_store.start()
    cell_store.wait()
    store.wait()


def body(n_grp, n_dev, spectrum, sea_mask, wind, currents, coupling):
    bins, _, width = spectrum.shape
    levels = bins // NDIR
    cells = currents.shape[2]
    table, padded = bin_tables(levels)
    shared_levels = 8
    vmem = pl.BlockSpec(memory_space=pltpu.VMEM)
    hbm = pl.BlockSpec(memory_space=pltpu.HBM)
    dma = pltpu.SemaphoreType.DMA
    updated, drift, where = pl.pallas_call(
        functools.partial(kernel, n_grp, n_dev, levels, padded, shared_levels),
        out_shape=(
            jax.ShapeDtypeStruct((bins, width), F32),
            jax.ShapeDtypeStruct((3, SUB, width), F32),
            jax.ShapeDtypeStruct((2, cells), jnp.int32),
        ),
        in_specs=[hbm] * 6,
        out_specs=(vmem, vmem, vmem),
        scratch_shapes=[
            pltpu.VMEM((bins, width), F32),
            pltpu.VMEM((1, cells), jnp.int32),
            pltpu.VMEM((1, width), jnp.int32),
            pltpu.VMEM((2, width), F32),
            pltpu.VMEM((2, cells), F32),
            pltpu.VMEM(table.shape, F32),
            pltpu.VMEM((bins, width), F32),
            pltpu.VMEM((bins, width), F32),
            pltpu.VMEM((2, bins, width), F32),
            pltpu.VMEM((3, bins, width), F32),
            pltpu.VMEM((2, n_grp, SUB, width), F32),
            pltpu.VMEM((4, SUB, width), F32),
            pltpu.VMEM((4, SUB, width), F32),
            pltpu.VMEM((4, SUB, width), F32),
            pltpu.VMEM((SUB, width), F32),
            pltpu.VMEM((3, padded, width), F32),
            pltpu.VMEM((SUB, width), F32),
            dma((6,)),
            dma((5,)),
            dma((5,)),
            dma((2,)),
            dma((2,)),
            dma((2, n_grp)),
            dma((2, n_grp)),
            dma((n_grp,)),
            dma((2,)),
            dma((2,)),
            dma((2,)),
            dma((2,)),
            dma((2,)),
            dma((2,)),
        ],
        compiler_params=pltpu.CompilerParams(
            collective_id=0, has_side_effects=True, vmem_limit_bytes=32 * 1024 * 1024
        ),
        name="wave_step",
    )(
        *[
            pltpu.with_memory_space_constraint(x, pltpu.HBM)
            for x in (
                spectrum.reshape(bins, width),
                sea_mask,
                wind.reshape(2, width),
                currents.reshape(2, cells),
                coupling,
                table,
            )
        ]
    )
    updated, cell_drift = pl.pallas_call(
        finish,
        out_shape=(
            jax.ShapeDtypeStruct((bins, width), F32),
            jax.ShapeDtypeStruct((2, cells), F32),
        ),
        in_specs=[vmem, vmem, vmem],
        out_specs=(hbm, hbm),
        scratch_shapes=[pltpu.VMEM((2, cells), F32), dma((2,))],
        compiler_params=pltpu.CompilerParams(vmem_limit_bytes=16 * 1024 * 1024),
        name="finish",
    )(updated, drift, where)
    return updated.reshape(bins, 1, width), cell_drift.reshape(1, 2, cells)


def solution(mesh):
    return jax.shard_map(
        functools.partial(body, mesh.shape["grp"], mesh.shape["dev"]),
        mesh=mesh,
        in_specs=(
            P(None, "dev", None),
            P("dev", None),
            P(None, "dev", None),
            P("grp", None, "dev"),
            P("grp", "dev"),
        ),
        out_specs=(P(None, "dev", None), P("grp", None, "dev")),
        check_vma=False,
    )
```

```python
import functools
import math

import jax
import jax.numpy as jnp
import numpy as np
from jax import lax
from jax.experimental import pallas as pl
from jax.experimental.pallas import tpu as pltpu
from jax.sharding import PartitionSpec as P

MESH = pl.DeviceIdType.MESH
F32 = jnp.float32
BF16 = jnp.bfloat16

NDIR = 32
FIRST_FREQ = 0.04
GROWTH = 1.1
SPEED_TOP = 0.45
CURRENT_TOP = 0.2
WIND_GAIN = 0.03
WHITECAP = 0.3
STEEP_SCALE = 0.4
STOKES_GAIN = 3.0
LANES = 128
SUB = 8
GROWTH_F = WIND_GAIN * 0.64


def bin_tables(levels):
    padded = -(-levels // SUB) * SUB
    heading = np.arange(NDIR) * (2.0 * math.pi / NDIR)
    freq = FIRST_FREQ * GROWTH ** np.arange(padded)
    rows = np.concatenate(
        [
            np.cos(heading),
            np.sin(heading),
            GROWTH_F * freq,
            freq**2,
            SPEED_TOP * FIRST_FREQ / freq,
            STOKES_GAIN * 0.1 * freq**4,
        ]
    )
    table = np.broadcast_to(rows[:, None], (rows.shape[0], LANES))
    return jnp.asarray(table.astype(np.float32)), padded


def split3(x):
    hi = x.astype(BF16)
    rest = x - hi.astype(F32)
    mid = rest.astype(BF16)
    low = (rest - mid.astype(F32)).astype(BF16)
    return jnp.concatenate([hi, mid, low], axis=0)


def sum3(x):
    n = x.shape[0] // 3
    return x[:n] + x[n : 2 * n] + x[2 * n :]


def kernel(
    n_grp,
    n_dev,
    levels,
    padded,
    shared_levels,
    spec_hbm,
    mask_hbm,
    wind_hbm,
    cur_hbm,
    coup_hbm,
    tab_hbm,
    upd_ref,
    drift_ref,
    where_ref,
    ctr,
    coup_ref,
    mask_ref,
    wind_ref,
    cur_ref,
    tab_ref,
    near,
    far,
    base,
    speed,
    part,
    link,
    sums,
    drift,
    last,
    rtab,
    near_flow,
    load_sem,
    halo_send,
    halo_recv,
    pass_send,
    pass_recv,
    part_send,
    part_recv,
    share_send,
    link_send,
    link_recv,
    sums_send,
    sums_recv,
    drift_send,
    drift_recv,
):
    g = lax.axis_index("grp")
    d = lax.axis_index("dev")
    side = 2 * lax.rem(d, 2) - 1

    bins = levels * NDIR
    quads = NDIR // SUB
    COS, SIN, FG = 0, NDIR, 2 * NDIR
    F2, GS, WT = FG + padded, FG + 2 * padded, FG + 3 * padded

    def at(step):
        return {"grp": g, "dev": lax.rem(d + step + n_dev, n_dev)}

    def group(step):
        return {"grp": lax.rem(g + step, n_grp), "dev": d}

    loads = [
        pltpu.make_async_copy(src, dst, load_sem.at[i])
        for i, (src, dst) in enumerate(
            (
                (coup_hbm, coup_ref),
                (cur_hbm, cur_ref),
                (spec_hbm, ctr),
                (tab_hbm, tab_ref),
                (mask_hbm, mask_ref),
                (wind_hbm, wind_ref),
            )
        )
    ]
    for load in loads:
        load.start()
    barrier = pltpu.get_barrier_semaphore()
    for peer in [at(side), at(-side)] + [group(k) for k in range(1, n_grp)]:
        pl.semaphore_signal(barrier, inc=1, device_id=peer, device_id_type=MESH)

    def across(step):
        return {"grp": lax.rem(g + step, n_grp), "dev": lax.rem(d + side + n_dev, n_dev)}

    @pl.when(side < 0)
    def _():
        for k in range(1, n_grp):
            pl.semaphore_signal(barrier, inc=1, device_id=across(k), device_id_type=MESH)

    loads[0].wait()
    loads[1].wait()
    coup = coup_ref[...]
    slot = ((coup >> 7) - d + n_dev + 1) & (n_dev - 1)
    row = coup & (LANES - 1)
    cells = coup.shape[1]
    one_hot = jnp.where(
        lax.broadcasted_iota(jnp.int32, (LANES, cells), 0) == row, 1.0, 0.0
    ).astype(BF16)
    kind = lax.broadcasted_iota(jnp.int32, (2 * SUB, cells), 0)
    comp = kind & 3
    value = jnp.where(
        comp == 0, cur_ref[0:1, :], jnp.where(comp == 1, cur_ref[1:2, :], jnp.where(comp == 2, 1.0, 0.0))
    )
    value = jnp.where(jnp.logical_and((kind >> 2) == slot, g > 0), value, 0.0)
    cell_sums = sum3(
        lax.dot_general(
            split3(value), one_hot, (((1,), (1,)), ((), ())), preferred_element_type=F32
        )
    )
    link[1, 0:4, :] = jnp.where(side > 0, cell_sums[8:12], cell_sums[0:4])
    link[3, 0:4, :] = jnp.where(side > 0, cell_sums[0:4], cell_sums[8:12])
    part[1, g] = jnp.zeros((SUB, LANES), F32)
    sums[1] = jnp.zeros((SUB, LANES), F32)
    where_ref[0:1, :] = jnp.where(g > 0, 1 + (slot - 1) * side, 3)
    where_ref[1:2, :] = row

    for load in loads[2:]:
        load.wait()

    def add_level(l, acc):
        r = pl.multiple_of(l * NDIR, NDIR)
        e = ctr[pl.ds(r, SUB), :]
        for m in range(1, quads):
            e = e + ctr[pl.ds(r + m * SUB, SUB), :]
        return (
            acc[0] + e * tab_ref[pl.ds(FG + l, 1), :],
            acc[1] + e * tab_ref[pl.ds(F2 + l, 1), :],
        )

    zero = jnp.zeros((SUB, LANES), F32)
    total, moment = lax.fori_loop(0, levels, add_level, (zero, zero), unroll=4)
    sea = mask_ref[...].astype(F32)
    total = jnp.sum(total, axis=0, keepdims=True) * (0.1 / GROWTH_F) * sea
    moment = jnp.sum(moment, axis=0, keepdims=True) * 0.1 * sea
    is_sea = sea > 0.5
    mean_freq = jnp.where(is_sea, moment / jnp.where(is_sea, total, 1.0), 1.0)
    steepness = STEEP_SCALE * total * mean_freq**4
    damp = WHITECAP * (steepness / mean_freq) ** 2
    which = lax.broadcasted_iota(jnp.int32, (SUB, LANES), 0)
    for i in (1, 3):
        for n, term in enumerate((sea, damp, wind_ref[0:1, :], wind_ref[1:2, :])):
            link[i, 4 + n : 5 + n, :] = term

    def damping(c, sea_c, damp_c):
        for q in range(padded // SUB):
            f2 = tab_ref[pl.ds(F2 + q * SUB, SUB), :]
            rtab[c, pl.ds(q * SUB, SUB), :] = sea_c / (1.0 + f2 * damp_c)

    damping(1, sea, damp)
    wide = (SUB, LANES)
    sign = side.astype(F32)
    cos = [tab_ref[pl.ds(COS + m * SUB, SUB), :] for m in range(quads)]
    sin = [tab_ref[pl.ds(SIN + m * SUB, SUB), :] for m in range(quads)]
    lane = lax.broadcasted_iota(jnp.int32, wide, 1)
    has_n = lane < LANES - 1
    has_s = lane > 0
    away = [sign * cos[m] for m in range(quads)]

    def speed_level(l, carry):
        gs = tab_ref[pl.ds(GS + l, 1), :]
        rec = rtab[1, pl.ds(l, 1), :]
        for m in range(quads):
            r = pl.ds(pl.multiple_of(l * NDIR + m * SUB, SUB), SUB)
            y = gs * sin[m]
            speed[0, r, :] = jnp.where(has_n, y, 0.0)
            speed[1, r, :] = jnp.where(has_s, y, 0.0)
            speed[2, r, :] = gs * away[m]
            base[0, r, :] = ctr[r, :] * rec
        return carry

    lax.fori_loop(0, levels, speed_level, 0, unroll=4)

    pl.semaphore_wait(barrier, n_grp + 1 + jnp.where(side > 0, n_grp - 1, 0))

    link_copies = []
    for i, step in ((1, side), (0, -side)):
        copy = pltpu.make_async_remote_copy(
            src_ref=link.at[3 - 2 * i],
            dst_ref=link.at[2 * i],
            send_sem=link_send.at[i],
            recv_sem=link_recv.at[i],
            device_id=at(step),
            device_id_type=MESH,
        )
        copy.start()
        link_copies.append(copy)

    def share_copy(k):
        return pltpu.make_async_remote_copy(
            src_ref=link.at[1],
            dst_ref=part.at[1, g],
            send_sem=share_send.at[k],
            recv_sem=part_recv.at[1, g],
            device_id=across(k),
            device_id_type=MESH,
        )

    @pl.when(jnp.logical_and(side > 0, g > 0))
    def _():
        for k in range(1, n_grp):
            share_copy(k).start()


    half = shared_levels // 2
    parity = lax.rem(g, 2)
    mine, theirs = parity * shared_levels, (1 - parity) * shared_levels
    first, middle = 2 * shared_levels, 32
    spans = ((mine, half), (mine + half, half), (first, middle - first), (middle, levels - middle))

    def span(start, count):
        return pl.ds(pl.multiple_of(start * NDIR, NDIR), count * NDIR)

    far_copies = []

    def send_far(k):
        there = span(*spans[k])
        copy = pltpu.make_async_remote_copy(
            src_ref=ctr.at[there, :],
            dst_ref=far.at[there, :],
            send_sem=halo_send.at[k],
            recv_sem=halo_recv.at[k],
            device_id=at(side),
            device_id_type=MESH,
        )
        copy.start()
        far_copies.append(copy)

    def group_copy(n, k):
        return pltpu.make_async_remote_copy(
            src_ref=part.at[n, g],
            dst_ref=part.at[n, g],
            send_sem=part_send.at[n, k],
            recv_sem=part_recv.at[n, g],
            device_id=group(k),
            device_id_type=MESH,
        )

    def over_groups(n):
        for src in range(1, n_grp):

            @pl.when(g != src)
            def _(src=src):
                pltpu.make_async_remote_copy(
                    src_ref=part.at[n, src],
                    dst_ref=part.at[n, src],
                    send_sem=part_send.at[n, 1],
                    recv_sem=part_recv.at[n, src],
                    device_id=group(1),
                    device_id_type=MESH,
                ).wait_recv()

        both = part[n, 1]
        for k in range(2, n_grp):
            both = both + part[n, k]
        return both

    send_far(0)
    send_far(1)
    send_far(2)

    link_copies[1].wait_recv()
    part[0, g, 0:4, :] = cell_sums[4:8] + link[0, 0:4, :]
    part[0, g, 4:8, :] = link[1, 0:4, :]

    @pl.when(g > 0)
    def _():
        for k in range(1, n_grp):
            group_copy(0, k).start()

    near_copy = pltpu.make_async_remote_copy(
        src_ref=ctr,
        dst_ref=near,
        send_sem=halo_send.at[4],
        recv_sem=halo_recv.at[4],
        device_id=at(-side),
        device_id_type=MESH,
    )
    near_copy.start()

    link_copies[0].wait_recv()
    part[1, g, 0:4, :] = link[2, 0:4, :]

    @pl.when(jnp.logical_and(side > 0, g > 0))
    def _():
        for k in range(1, n_grp):
            group_copy(1, k).start()

    for c in (0, 2):
        damping(c, link[c, 4:5, :], link[c, 5:6, :])
    near_copy.wait_recv()

    def near_level(l, carry):
        rec = rtab[0, pl.ds(l, 1), :]
        for m in range(quads):
            r = pl.ds(pl.multiple_of(l * NDIR + m * SUB, SUB), SUB)
            base[1, r, :] = near[r, :] * rec
        return carry

    lax.fori_loop(0, levels, near_level, 0, unroll=6)
    chip = over_groups(0)
    sums[3] = chip
    chip_copy = pltpu.make_async_remote_copy(
        src_ref=sums.at[3],
        dst_ref=sums.at[2],
        send_sem=sums_send.at[1],
        recv_sem=sums_recv.at[1],
        device_id=at(side),
        device_id_type=MESH,
    )
    chip_copy.start()
    send_far(3)
    pass_copies = []
    for i, step in ((0, 1), (1, n_grp - 1)):
        far_copies[i].wait_recv()
        there = span(*spans[i])
        copy = pltpu.make_async_remote_copy(
            src_ref=far.at[there, :],
            dst_ref=far.at[there, :],
            send_sem=pass_send.at[i],
            recv_sem=pass_recv.at[i],
            device_id=group(step),
            device_id_type=MESH,
        )
        copy.start()
        pass_copies.append(copy)
    gain = {}

    def column(c, s4):
        count = jnp.maximum(s4[2:3], 1.0)
        mean_x = s4[0:1] / count
        mean_y = s4[1:2] / count
        sea_c = link[c, 4:5, :]
        wx = link[c, 6:7, :] - mean_x
        wy = link[c, 7:8, :] - mean_y
        gain[c] = [cos[m] * wx + sin[m] * wy for m in range(quads)]
        return CURRENT_TOP * jnp.tanh(mean_x), CURRENT_TOP * jnp.tanh(mean_y), sea_c

    def near_forced():
        pltpu.make_async_remote_copy(
            src_ref=sums.at[1],
            dst_ref=sums.at[0],
            send_sem=sums_send.at[0],
            recv_sem=sums_recv.at[0],
            device_id=at(-side),
            device_id_type=MESH,
        ).wait_recv()
        near_flow[...] = jnp.broadcast_to(column(0, sums[0])[0], wide)

        def level(l, carry):
            fg = tab_ref[pl.ds(FG + l, 1), :]
            for m in range(quads):
                r = pl.ds(pl.multiple_of(l * NDIR + m * SUB, SUB), SUB)
                base[1, r, :] = base[1, r, :] * jnp.maximum(
                    gain[0][m] * fg + (1.0 - WIND_GAIN), 1.0
                )
            return carry

        lax.fori_loop(0, levels, level, 0, unroll=6)

    pl.when(side > 0)(near_forced)
    own = chip[0:4] + over_groups(1)[0:4]
    sums[1, 0:4, :] = own
    own_copy = pltpu.make_async_remote_copy(
        src_ref=sums.at[1],
        dst_ref=sums.at[0],
        send_sem=sums_send.at[0],
        recv_sem=sums_recv.at[0],
        device_id=at(-side),
        device_id_type=MESH,
    )
    own_copy.start()

    flow_x, flow_y, _ = column(1, own)
    pl.when(side < 0)(near_forced)
    face_near = jnp.broadcast_to(-sign * (0.5 * (near_flow[...] + flow_x)), wide)
    flow_y = jnp.broadcast_to(flow_y, wide)
    face_n = jnp.where(has_n, 0.5 * (flow_y + pltpu.roll(flow_y, LANES - 1, 1)), 0.0)
    face_s = jnp.where(has_s, 0.5 * (flow_y + pltpu.roll(flow_y, 1, 1)), 0.0)
    sea_w = jnp.broadcast_to(sea, wide)

    def forced(damped, c, m, fg):
        return damped * jnp.maximum(gain[c][m] * fg + (1.0 - WIND_GAIN), 1.0)

    def drift_rows(acc):
        dx = acc[0] * cos[0]
        dy = acc[0] * sin[0]
        for m in range(1, quads):
            dx = dx + acc[m] * cos[m]
            dy = dy + acc[m] * sin[m]
        dx = jnp.sum(dx, axis=0, keepdims=True)
        dy = jnp.sum(dy, axis=0, keepdims=True)
        return jnp.where(which == 0, dx, jnp.where(which == 1, dy, 0.0))

    def own_level(l, acc):
        fg = tab_ref[pl.ds(FG + l, 1), :]
        wt = tab_ref[pl.ds(WT + l, 1), :]
        out = []
        for m in range(quads):
            r = pl.ds(pl.multiple_of(l * NDIR + m * SUB, SUB), SUB)
            e = forced(base[0, r, :], 1, m, fg)
            other = base[1, r, :]
            a = speed[0, r, :] + face_n
            b = speed[1, r, :] + face_s
            c = face_near - speed[2, r, :]
            flux_n = a * jnp.where(a > 0.0, e, pltpu.roll(e, LANES - 1, 1))
            flux_s = b * jnp.where(b > 0.0, pltpu.roll(e, 1, 1), e)
            u = sea_w * (e - flux_n + flux_s - c * jnp.where(c > 0.0, e, other))
            base[0, r, :] = e
            base[1, r, :] = u
            out.append(acc[m] + wt * u)
        return tuple(out)

    acc = lax.fori_loop(0, levels, own_level, (zero,) * quads, unroll=6)
    drift[3] = drift_rows(acc)
    partial_copy = pltpu.make_async_remote_copy(
        src_ref=drift.at[3],
        dst_ref=drift.at[2],
        send_sem=drift_send.at[1],
        recv_sem=drift_recv.at[1],
        device_id=at(side),
        device_id_type=MESH,
    )
    partial_copy.start()

    chip_copy.wait_recv()
    flow_far, _, sea_far = column(2, sums[2, 0:4, :] + chip[4:8])
    face_far = jnp.broadcast_to(sign * (0.5 * (flow_x + flow_far)), wide)

    def far_level(l, acc):
        fg = tab_ref[pl.ds(FG + l, 1), :]
        wt = tab_ref[pl.ds(WT + l, 1), :]
        rec = rtab[2, pl.ds(l, 1), :]
        out = []
        for m in range(quads):
            r = pl.ds(pl.multiple_of(l * NDIR + m * SUB, SUB), SUB)
            other = forced(far[r, :] * rec, 2, m, fg)
            a = speed[2, r, :] + face_far
            flux = a * jnp.where(a > 0.0, base[0, r, :], other)
            upd_ref[r, :] = base[1, r, :] - sea_w * flux
            out.append(acc[m] + wt * flux)
        return tuple(out)

    acc = (zero,) * quads

    def far_levels(start, count, acc):
        return lax.fori_loop(0, count, lambda i, acc: far_level(start + i, acc), acc, unroll=4)

    acc = far_levels(mine, shared_levels, acc)
    for k in (2, 3):
        far_copies[k].wait_recv()
        acc = far_levels(*spans[k], acc)
    for i in range(2):
        here = span(theirs + i * half, half)
        pltpu.make_async_remote_copy(
            src_ref=far.at[here, :],
            dst_ref=far.at[here, :],
            send_sem=pass_send.at[i],
            recv_sem=pass_recv.at[i],
            device_id=group(1 + i * (n_grp - 2)),
            device_id_type=MESH,
        ).wait_recv()
    acc = far_levels(theirs, shared_levels, acc)

    shared = drift_rows(acc)
    drift[1] = drift[3] - sea * shared
    full_copy = pltpu.make_async_remote_copy(
        src_ref=drift.at[1],
        dst_ref=drift.at[0],
        send_sem=drift_send.at[0],
        recv_sem=drift_recv.at[0],
        device_id=at(-side),
        device_id_type=MESH,
    )
    full_copy.start()
    partial_copy.wait_recv()
    last[...] = drift[2] + sea_far * shared
    @pl.when(g > 0)
    def _():
        for k in range(1, n_grp):
            group_copy(0, k).wait_send()

    @pl.when(jnp.logical_and(side > 0, g > 0))
    def _():
        for k in range(1, n_grp):
            group_copy(1, k).wait_send()
            share_copy(k).wait_send()

    for copy in link_copies + far_copies + pass_copies + [near_copy, chip_copy, own_copy, partial_copy]:
        copy.wait_send()
    full_copy.wait()
    drift_ref[0] = drift[0]
    drift_ref[1] = drift[1]
    drift_ref[2] = last[...]


def finish(upd_ref, drift, where_ref, upd_hbm, cell_hbm, cell_ref, sem):
    store = pltpu.make_async_copy(upd_ref, upd_hbm, sem.at[0])
    store.start()
    cells = where_ref.shape[1]
    for j in range(cells // LANES):
        here = pl.ds(j * LANES, LANES)
        role = where_ref[0:1, here]
        row = jnp.broadcast_to(where_ref[1:2, here], (SUB, LANES))
        out = jnp.zeros((SUB, LANES), F32)
        for c in range(3):
            out = jnp.where(role == c, jnp.take_along_axis(drift[c], row, axis=1), out)
        cell_ref[:, here] = out[0:2]
    cell_store = pltpu.make_async_copy(cell_ref, cell_hbm, sem.at[1])
    cell_store.start()
    cell_store.wait()
    store.wait()


def body(n_grp, n_dev, spectrum, sea_mask, wind, currents, coupling):
    bins, _, width = spectrum.shape
    levels = bins // NDIR
    cells = currents.shape[2]
    table, padded = bin_tables(levels)
    shared_levels = 8
    vmem = pl.BlockSpec(memory_space=pltpu.VMEM)
    hbm = pl.BlockSpec(memory_space=pltpu.HBM)
    dma = pltpu.SemaphoreType.DMA
    updated, drift, where = pl.pallas_call(
        functools.partial(kernel, n_grp, n_dev, levels, padded, shared_levels),
        out_shape=(
            jax.ShapeDtypeStruct((bins, width), F32),
            jax.ShapeDtypeStruct((3, SUB, width), F32),
            jax.ShapeDtypeStruct((2, cells), jnp.int32),
        ),
        in_specs=[hbm] * 6,
        out_specs=(vmem, vmem, vmem),
        scratch_shapes=[
            pltpu.VMEM((bins, width), F32),
            pltpu.VMEM((1, cells), jnp.int32),
            pltpu.VMEM((1, width), jnp.int32),
            pltpu.VMEM((2, width), F32),
            pltpu.VMEM((2, cells), F32),
            pltpu.VMEM(table.shape, F32),
            pltpu.VMEM((bins, width), F32),
            pltpu.VMEM((bins, width), F32),
            pltpu.VMEM((2, bins, width), F32),
            pltpu.VMEM((3, bins, width), F32),
            pltpu.VMEM((2, n_grp, SUB, width), F32),
            pltpu.VMEM((4, SUB, width), F32),
            pltpu.VMEM((4, SUB, width), F32),
            pltpu.VMEM((4, SUB, width), F32),
            pltpu.VMEM((SUB, width), F32),
            pltpu.VMEM((3, padded, width), F32),
            pltpu.VMEM((SUB, width), F32),
            dma((6,)),
            dma((5,)),
            dma((5,)),
            dma((2,)),
            dma((2,)),
            dma((2, n_grp)),
            dma((2, n_grp)),
            dma((n_grp,)),
            dma((2,)),
            dma((2,)),
            dma((2,)),
            dma((2,)),
            dma((2,)),
            dma((2,)),
        ],
        compiler_params=pltpu.CompilerParams(
            collective_id=0, has_side_effects=True, vmem_limit_bytes=32 * 1024 * 1024
        ),
        name="wave_step",
    )(
        *[
            pltpu.with_memory_space_constraint(x, pltpu.HBM)
            for x in (
                spectrum.reshape(bins, width),
                sea_mask,
                wind.reshape(2, width),
                currents.reshape(2, cells),
                coupling,
                table,
            )
        ]
    )
    updated, cell_drift = pl.pallas_call(
        finish,
        out_shape=(
            jax.ShapeDtypeStruct((bins, width), F32),
            jax.ShapeDtypeStruct((2, cells), F32),
        ),
        in_specs=[vmem, vmem, vmem],
        out_specs=(hbm, hbm),
        scratch_shapes=[pltpu.VMEM((2, cells), F32), dma((2,))],
        compiler_params=pltpu.CompilerParams(vmem_limit_bytes=16 * 1024 * 1024),
        name="finish",
    )(updated, drift, where)
    return updated.reshape(bins, 1, width), cell_drift.reshape(1, 2, cells)


def solution(mesh):
    return jax.shard_map(
        functools.partial(body, mesh.shape["grp"], mesh.shape["dev"]),
        mesh=mesh,
        in_specs=(
            P(None, "dev", None),
            P("dev", None),
            P(None, "dev", None),
            P("grp", None, "dev"),
            P("grp", "dev"),
        ),
        out_specs=(P(None, "dev", None), P("grp", None, "dev")),
        check_vma=False,
    )
```
